32 devices in a mesh: wa: 8 (over z, x), ta: 4 (over y, core).
Axes of the slice: x: 2, y: 2, z: 4, core: 2. Of those that a mesh axis runs over, the one named last changes fastest.
Arguments:
- tokens: bfloat16 [12544, 512], P('wa', 'ta'), may hold values from -6 to 6
- gain_one: float32 [512], P('ta'), may hold values from 0.5 to 1.5
- shift_one: float32 [512], P('ta'), may hold values from -3 to 3
- w_query: bfloat16 [512, 512], P('wa', 'ta'), may hold values from -1 to 1
- w_key: bfloat16 [512, 512], P('wa', 'ta'), may hold values from -0.25 to 0.25
- w_value: bfloat16 [512, 512], P('wa', 'ta'), may hold values from -0.25 to 0.25
- b_query: float32 [512], P('ta'), may hold values from -3 to 3
- b_value: float32 [512], P('ta'), may hold values from -3 to 3
- w_out: bfloat16 [512, 512], P('ta', 'wa'), may hold values from -0.75 to 0.75
- b_out: float32 [512], P('ta'), may hold values from -3 to 3
- gain_two: float32 [512], P('ta'), may hold values from 0.5 to 1.5
- shift_two: float32 [512], P('ta'), may hold values from -3 to 3
- w_hidden: bfloat16 [512, 2048], P('wa', 'ta'), may hold values from -0.25 to 0.25
- b_hidden: float32 [2048], P('ta'), may hold values from -3 to 3
- w_down: bfloat16 [2048, 512], P('ta', 'wa'), may hold values from -0.125 to 0.125
- b_down: float32 [512], P('ta'), may hold values from -3 to 3
- bias_table: float32 [169, 16], P(None, 'ta'), may hold values from -4 to 4
- rel_index: int32 [49, 49], replicated, may hold values from 0 to 168, as said below
- region: int32 [256, 49], P('wa'), may hold values from 0 to 3, as said below
- win_count: int32 [8], P('wa'), may hold values from 16 to 32, as said below
- cotangent: bfloat16 [12544, 512], P('wa', 'ta'), may hold values from -6 to 6
Outputs:
- y_out: float32 [12544, 512], P('wa', 'ta')
- grad_tokens: float32 [12544, 512], P('wa', 'ta')
- grad_gain_one: float32 [512], P('ta')
- grad_shift_one: float32 [512], P('ta')
- grad_w_query: float32 [512, 512], P('wa', 'ta')
- grad_w_key: float32 [512, 512], P('wa', 'ta')
- grad_w_value: float32 [512, 512], P('wa', 'ta')
- grad_b_query: float32 [512], P('ta')
- grad_b_value: float32 [512], P('ta')
- grad_w_out: float32 [512, 512], P('ta', 'wa')
- grad_b_out: float32 [512], P('ta')
- grad_gain_two: float32 [512], P('ta')
- grad_shift_two: float32 [512], P('ta')
- grad_w_hidden: float32 [512, 2048], P('wa', 'ta')
- grad_b_hidden: float32 [2048], P('ta')
- grad_w_down: float32 [2048, 512], P('ta', 'wa')
- grad_b_down: float32 [512], P('ta')
- grad_table: float32 [169, 16], P(None, 'ta')
The draws below stay inside these ranges and needn't reach their ends.
Inputs may be any that keep to these rules, and one draw needn't show every extreme that they name: `rel_index`: pairs (i, j) of window positions with the same offset of rows and of columns share an entry, and every entry is used. Within a window slot, region is constant on rectangular blocks of positions cut by at most one row and one column. `win_count`: some index of wa has all 32 slots live.
All inputs are finite; a program needn't handle non-finite values.
Results may differ from the reference program's by a relative error of at most 0.012.
Values may be sent and summed in bfloat16 or wider, within the bound.
A program may use at most 128 MiB of HBM per device.

```python
import jax
import jax.numpy as jnp
from jax import lax

C = 512
HEADS = 16
HDIM = 32
HID = 2048
SIDE = 7
WT = 49
TABLE = 169
CAP = 32
WINDOWS = 256
TOKENS = 12544
N_WA = 8


def draw_w_query(key, part):
    base = jnp.clip(jax.random.normal(key, (C, C), jnp.float32), -6.0, 6.0) * C ** (-0.5)
    return base.astype(jnp.bfloat16)


def draw_rel_index(key, part):
    place = jnp.arange(WT, dtype=jnp.int32)
    row_pos = place // SIDE
    col_pos = place % SIDE
    offset = (row_pos[:, None] - row_pos[None, :] + SIDE - 1) * (2 * SIDE - 1)
    offset = offset + (col_pos[:, None] - col_pos[None, :] + SIDE - 1)
    shuffled = jax.random.permutation(key, TABLE).astype(jnp.int32)
    return shuffled[offset].astype(jnp.int32)


def draw_region(key, part):
    cuts = jax.random.randint(key, (WINDOWS, 2), 1, SIDE + 1).astype(jnp.int32)
    place = jnp.arange(WT, dtype=jnp.int32)
    row_pos = place // SIDE
    col_pos = place % SIDE
    upper = (row_pos[None, :] >= cuts[:, 0:1]).astype(jnp.int32)
    right = (col_pos[None, :] >= cuts[:, 1:2]).astype(jnp.int32)
    return (upper * 2 + right).astype(jnp.int32)


def draw_win_count(key, part):
    counts = jax.random.randint(key, (N_WA,), (CAP + 1) // 2, CAP + 1).astype(jnp.int32)
    fullest = jax.random.randint(jax.random.fold_in(key, 3), (), 0, N_WA).astype(jnp.int32)
    return jnp.where(jnp.arange(N_WA, dtype=jnp.int32) == fullest, CAP, counts).astype(jnp.int32)


def steps_of(own_key, shape, pieces, least, top_value):
    level, own = 1.0, jax.random.fold_in(own_key, 6)
    for position, shards_of in pieces:
        steps = jnp.exp(jax.random.uniform(jax.random.fold_in(own, position), (shards_of,), jnp.float32, least / len(pieces), top_value / len(pieces)))
        level = level * jnp.repeat(steps, shape[position] // shards_of).reshape([-1 if axis == position else 1 for axis in range(len(shape))])
    return level


def noise(stream_key, dims, scale, most, shards=(), kind=jnp.bfloat16):
    factor_of = steps_of(stream_key, dims, shards, -0.22, 0.18) if shards else 1.0
    entries = jax.random.normal(stream_key, dims, jnp.float32) * scale * factor_of
    return jnp.minimum(jnp.maximum(entries, -most), most).astype(kind)


def setup_inputs(seed: int = 0) -> dict:
    key_of = jax.random.split(jax.random.key(seed), 22)
    tokens = noise(key_of[0], (TOKENS, C), 1.0, 6.0, ((0, 8), (1, 4)))
    gain_one = jnp.clip(1.0 + 0.1 * jax.random.normal(key_of[1], (C,), jnp.float32), 0.5, 1.5)
    shift_one = noise(key_of[2], (C,), 0.5, 3.0, ((0, 4),), jnp.float32)
    w_query = draw_w_query(jax.random.fold_in(key_of[21], 71), 0)
    w_key = noise(key_of[4], (C, C), C ** -0.5, 0.25, ((0, 8), (1, 4)))
    w_value = noise(key_of[5], (C, C), C ** -0.5, 0.25, ((0, 8), (1, 4)))
    b_query = noise(key_of[6], (C,), 0.5, 3.0, ((0, 4),), jnp.float32)
    b_value = noise(key_of[7], (C,), 0.5, 3.0, ((0, 4),), jnp.float32)
    w_out = noise(key_of[8], (C, C), (C // 8) ** -0.5, 0.75, ((0, 4), (1, 8)))
    b_out = noise(key_of[9], (C,), 0.5, 3.0, ((0, 4),), jnp.float32)
    gain_two = jnp.clip(1.0 + 0.1 * jax.random.normal(key_of[10], (C,), jnp.float32), 0.5, 1.5)
    shift_two = noise(key_of[11], (C,), 0.5, 3.0, ((0, 4),), jnp.float32)
    w_hidden = noise(key_of[12], (C, HID), C ** -0.5, 0.25, ((0, 8), (1, 4)))
    b_hidden = noise(key_of[13], (HID,), 0.5, 3.0, ((0, 4),), jnp.float32)
    w_down = noise(key_of[14], (HID, C), HID ** -0.5, 0.125, ((0, 4), (1, 8)))
    b_down = noise(key_of[15], (C,), 0.5, 3.0, ((0, 4),), jnp.float32)
    bias_table = noise(key_of[16], (TABLE, HEADS), 1.0, 4.0, ((1, 4),), jnp.float32)
    rel_index = draw_rel_index(jax.random.fold_in(key_of[21], 71), 0)
    region = draw_region(jax.random.fold_in(key_of[21], 71), 0)
    win_count = draw_win_count(jax.random.fold_in(key_of[21], 71), 0)
    cotangent = noise(key_of[20], (TOKENS, C), 1.0, 6.0, ((0, 8), (1, 4)))
    return {"tokens": tokens, "gain_one": gain_one, "shift_one": shift_one, "w_query": w_query, "w_key": w_key, "w_value": w_value, "b_query": b_query, "b_value": b_value, "w_out": w_out, "b_out": b_out, "gain_two": gain_two, "shift_two": shift_two, "w_hidden": w_hidden, "b_hidden": b_hidden, "w_down": w_down, "b_down": b_down, "bias_table": bias_table, "rel_index": rel_index, "region": region, "win_count": win_count, "cotangent": cotangent}


eps_norm = 1e-05
mask_value = -100.0

@jax.custom_vjp
def low(v):
    return lax.optimization_barrier(v.astype(jnp.bfloat16)).astype(jnp.float32)

@jax.custom_vjp
def low_back(v):
    return v

def low_keep(v):
    return (low(v), None)

def low_pass(kept, grad):
    return (grad,)

def back_keep(v):
    return (v, None)

def back_low(kept, grad):
    return (low(grad),)
low.defvjp(low_keep, low_pass)
low_back.defvjp(back_keep, back_low)

def product(left, right):
    return jnp.dot(left, right, precision=lax.Precision.HIGHEST, preferred_element_type=jnp.float32)

def layer_norm(value, gain, shift):
    mean = lax.optimization_barrier(jnp.mean(value, axis=-1, keepdims=True))
    spread = lax.optimization_barrier(jnp.mean(value * value, axis=-1, keepdims=True)) - mean * mean
    return (value - mean) * lax.rsqrt(spread + eps_norm) * gain + shift

def forward(tokens, gain_one, shift_one, w_query, w_key, w_value, b_query, b_value, w_out, b_out, gain_two, shift_two, w_hidden, b_hidden, w_down, b_down, bias_table, onehot, allowed):
    windows = tokens.shape[0] // WT
    h_one = low(layer_norm(tokens, gain_one, shift_one))
    query = low_back(low((product(h_one, w_query) + b_query) * HDIM ** (-0.5)))
    keyset = low_back(low(product(h_one, w_key)))
    values = low_back(low(product(h_one, w_value) + b_value))

    def split(t):
        return t.reshape(windows, WT, HEADS, HDIM)
    rel_bias = product(onehot, bias_table).T.reshape(HEADS, WT, WT)
    scores = jnp.einsum('wihd,wjhd->whij', split(query), split(keyset), precision=lax.Precision.HIGHEST)
    scores = low_back(scores + rel_bias[None] + allowed[:, None])
    probs = low(jax.nn.softmax(scores, axis=-1))
    attended = jnp.einsum('whij,wjhd->wihd', probs, split(values), precision=lax.Precision.HIGHEST)
    attended = low_back(low(attended.reshape(windows * WT, C)))
    mixed = tokens + low_back(product(attended, w_out)) + b_out
    h_two = low(layer_norm(mixed, gain_two, shift_two))
    hidden = low_back(product(h_two, w_hidden)) + b_hidden
    act = low(jax.nn.gelu(hidden, approximate=False))
    return mixed + low_back(product(act, w_down)) + b_down

def reference(tokens, gain_one, shift_one, w_query, w_key, w_value, b_query, b_value, w_out, b_out, gain_two, shift_two, w_hidden, b_hidden, w_down, b_down, bias_table, rel_index, region, win_count, cotangent):
    windows = region.shape[0]
    flat = rel_index.reshape(-1).astype(jnp.int32)
    onehot = (flat[:, None] == jnp.arange(TABLE, dtype=jnp.int32)[None, :]).astype(jnp.float32)
    allowed = jnp.where(region[:, :, None] == region[:, None, :], 0.0, mask_value).astype(jnp.float32)
    slot = jnp.arange(windows * WT, dtype=jnp.int32) // WT
    owner = (slot // CAP).astype(jnp.int32)
    live = (slot % CAP < win_count[owner]).astype(jnp.float32)[:, None]
    params = (tokens.astype(jnp.float32), gain_one.astype(jnp.float32), shift_one.astype(jnp.float32), w_query.astype(jnp.float32), w_key.astype(jnp.float32), w_value.astype(jnp.float32), b_query.astype(jnp.float32), b_value.astype(jnp.float32), w_out.astype(jnp.float32), b_out.astype(jnp.float32), gain_two.astype(jnp.float32), shift_two.astype(jnp.float32), w_hidden.astype(jnp.float32), b_hidden.astype(jnp.float32), w_down.astype(jnp.float32), b_down.astype(jnp.float32), bias_table.astype(jnp.float32))

    def closed(*args):
        return forward(*args, onehot, allowed)
    result, pull = jax.vjp(closed, *params)
    grads = pull(cotangent.astype(jnp.float32) * live)
    return (result * live, grads[0], grads[1], grads[2], grads[3], grads[4], grads[5], grads[6], grads[7], grads[8], grads[9], grads[10], grads[11], grads[12], grads[13], grads[14], grads[15], grads[16])
```

```python
import functools

import jax
import jax.numpy as jnp
from jax import lax
from jax.experimental import pallas as pl
from jax.experimental.pallas import tpu as pltpu
from jax.sharding import PartitionSpec as P

C = 512
HDIM = 32
WT = 49
PAD = 64
TABLE = 169
TPAD = 256
NCH = 6
CW = 256
LANES = 128
SROWS = 24
SCALE = HDIM ** (-0.5)
EPS = 1e-05
F32 = jnp.float32
BF16 = jnp.bfloat16
MESH = pl.DeviceIdType.MESH
ANY = pl.BlockSpec(memory_space=pl.ANY)
VM = pl.BlockSpec(memory_space=pltpu.VMEM)


def place():
    a, t = lax.axis_index("wa"), lax.axis_index("ta")
    return a, t, lax.rem(a, 2), lax.div(a, 2), lax.rem(t, 2), lax.div(t, 2)


def greet(peers):
    barrier = pltpu.get_barrier_semaphore()
    for peer in peers:
        pl.semaphore_signal(barrier, inc=1, device_id=peer, device_id_type=MESH)
    pl.semaphore_wait(barrier, len(peers))


def remote(src, dst, send, recv, peer):
    copy = pltpu.make_async_remote_copy(
        src_ref=src, dst_ref=dst, send_sem=send, recv_sem=recv, device_id=peer, device_id_type=MESH
    )
    copy.start()
    return copy


def bring(nt, nz, tok, cot, wp, vec, rb, xg, cg, gw, vg, rg, b0, b1, b2, b3, b4, *sems):
    loc, ta_s, ta_r, z_s, z_r, p_s, p_r, q_s, q_r, k_s, k_r = sems
    a, t, x, z, c, y = place()
    xp = (z * 2 + (1 - x), t)
    yp = (a, (1 - y) * 2 + c)
    cp = (a, y * 2 + (1 - c))
    ty = (1 - y) * 2 + c
    zs = [(lax.rem(z + d, nz) * 2 + x, t) for d in range(1, nz)]
    ts = [(a, lax.rem(t + d, nt)) for d in range(1, nt)]
    own = [(tok.at[t], b0, xg.at[t]), (cot.at[t], b1, cg.at[t]), (wp, b2, gw.at[:, t, z, x])]
    own += [(vec, b3, vg.at[t]), (rb, b4, rg.at[t])]
    ins = [pltpu.make_async_copy(s, m, loc.at[i]) for i, (s, m, _) in enumerate(own)]
    for copy in ins:
        copy.start()
    greet(zs + ts + [xp])
    waits = []
    for ch in range(NCH):
        for d, peer in enumerate(zs):
            waits.append(
                remote(wp.at[ch], gw.at[ch, t, z, x], z_s.at[ch, d], z_r.at[ch, d], peer)
            )
    for d, peer in enumerate(ts):
        other = peer[1]
        for i, (s, g) in enumerate(((tok.at[other], xg), (cot.at[other], cg), (vec, vg), (rb, rg))):
            waits.append(remote(s, g.at[t], ta_s.at[i, d], ta_r.at[i, d], peer))
    outs = []
    for i, (_, m, o) in enumerate(own):
        ins[i].wait()
        outs.append(pltpu.make_async_copy(m, o, loc.at[i]))
        outs[-1].start()
    outs[2].wait()

    def got(ref, sem):
        pltpu.make_async_copy(ref, ref, sem).wait()

    zw = 0
    for ch in range(NCH):
        for d in range(1, nz):
            waits[zw].wait_recv()
            zw += 1
        if ch % 2 == 0:
            ref = gw.at[ch, t, :, x]
            waits.append(remote(ref, ref, p_s.at[ch], p_r.at[ch], xp))
        else:
            ref = gw.at[ch, t, :, x]
            waits.append(remote(ref, ref, p_s.at[ch], p_r.at[ch], yp))
    first = waits[-NCH:]
    second = []
    for ch in range(NCH):
        first[ch].wait_recv()
        if ch % 2 == 0:
            ref = gw.at[ch, t]
            second.append((remote(ref, ref, q_s.at[ch, 0], q_r.at[ch, 0], yp),))
            waits.append(remote(ref, ref, k_s.at[ch, 0], k_r.at[ch, 0], cp))
        else:
            pair = []
            for i, tt in enumerate((t, ty)):
                ref = gw.at[ch, tt, :, x]
                pair.append(remote(ref, ref, q_s.at[ch, i], q_r.at[ch, i], xp))
            second.append(tuple(pair))
    for ch in range(NCH):
        for copy in second[ch]:
            copy.wait_recv()
        if ch % 2 == 1:
            ref = gw.at[ch, t]
            waits.append(remote(ref, ref, k_s.at[ch, 0], k_r.at[ch, 0], cp))
        ref = gw.at[ch, ty]
        waits.append(remote(ref, ref, k_s.at[ch, 1], k_r.at[ch, 1], cp))
    nzc = NCH * (nz - 1)
    for copy in waits[nzc : nzc + 4 * (nt - 1)]:
        copy.wait_recv()
    for copy in waits[nzc + 4 * (nt - 1) + NCH :]:
        copy.wait_recv()
    for copy in waits:
        copy.wait_send()
    for group in second:
        for copy in group:
            copy.wait_send()
    for i, copy in enumerate(outs):
        if i != 2:
            copy.wait()


def bring_call(nt, nz, tok, cot, wp, vec, rb):
    rows = tok.shape[1]
    deep = wp.shape[1]
    sem = pltpu.SemaphoreType.DMA
    return pl.pallas_call(
        functools.partial(bring, nt, nz),
        name="bring",
        out_shape=(
            jax.ShapeDtypeStruct((nt, rows, LANES), BF16),
            jax.ShapeDtypeStruct((nt, rows, LANES), BF16),
            jax.ShapeDtypeStruct((NCH, nt, nz, 2, deep, CW), BF16),
            jax.ShapeDtypeStruct((nt,) + vec.shape, F32),
            jax.ShapeDtypeStruct((nt,) + rb.shape, F32),
        ),
        in_specs=[ANY] * 5,
        out_specs=(ANY,) * 5,
        scratch_shapes=[
            pltpu.VMEM(tok.shape[1:], BF16),
            pltpu.VMEM(tok.shape[1:], BF16),
            pltpu.VMEM(wp.shape, BF16),
            pltpu.VMEM(vec.shape, F32),
            pltpu.VMEM(rb.shape, F32),
            sem((5,)),
            sem((4, nt - 1)),
            sem((4, nt - 1)),
            sem((NCH, nz - 1)),
            sem((NCH, nz - 1)),
            sem((NCH,)),
            sem((NCH,)),
            sem((NCH, 2)),
            sem((NCH, 2)),
            sem((NCH, 2)),
            sem((NCH, 2)),
        ],
        compiler_params=pltpu.CompilerParams(collective_id=0, has_side_effects=True),
    )(tok, cot, wp, vec, rb)


def nn(left, right):
    return jnp.dot(left, right, preferred_element_type=F32)


def nt_dot(left, right):
    return lax.dot_general(left, right, (((1,), (1,)), ((), ())), preferred_element_type=F32)


def tn_dot(left, right):
    return lax.dot_general(left, right, (((0,), (0,)), ((), ())), preferred_element_type=F32)


def norm(value):
    mean = jnp.mean(value, axis=1, keepdims=True)
    spread = jnp.mean(value * value, axis=1, keepdims=True) - mean * mean
    rstd = lax.rsqrt(spread + EPS)
    return (value - mean) * rstd, rstd


def norm_back(scaled, normed, rstd):
    first = jnp.mean(scaled, axis=1, keepdims=True)
    second = jnp.mean(scaled * normed, axis=1, keepdims=True)
    return rstd * (scaled - first - normed * second)


def gelu_pair(u):
    cdf = 0.5 + 0.5 * lax.erf(u * (0.5**0.5))
    pdf = jnp.exp(-0.5 * u * u) * ((2.0 * jnp.pi) ** -0.5)
    return u * cdf, cdf + u * pdf


def rowsum(value):
    return jnp.sum(value, axis=0, keepdims=True)


def work(
    nt, slots, live, x_in, c_in, gw, vec, rb, mask,
    y_out, g_out, dw, small, pairs,
    xs, xp, gy, h1, h1t, h2t, gyt, qs, kvs, probs, att, acc, acc2, n1, r1, n2, r2, low, gkv, gq,
):
    heads = LANES // HDIM
    rows = slots * PAD
    half = 2 * PAD
    nhalf = rows // half

    def wide(i):
        return jnp.concatenate([vec[t, i : i + 1, :] for t in range(nt)], axis=1)

    def put_small(i, value):
        for t in range(nt):
            small[t, i : i + 1, :] = value[:, t * LANES : (t + 1) * LANES]

    def spread(source, target):
        for t in range(nt):
            xs[:, t * LANES : (t + 1) * LANES] = source[t].astype(F32)
        zero = jnp.zeros((PAD - WT, C), F32)
        for w in range(slots):
            target[w * PAD : w * PAD + WT, :] = xs[w * WT : (w + 1) * WT, :]
            target[w * PAD + WT : (w + 1) * PAD, :] = zero

    def gather(source, target):
        for w in range(slots):
            xs[w * WT : (w + 1) * WT, :] = source[w * PAD : w * PAD + WT, :]
        for t in range(nt):
            target[t] = xs[:, t * LANES : (t + 1) * LANES].astype(BF16)

    small[...] = jnp.zeros_like(small)
    pairs[...] = jnp.zeros_like(pairs)
    spread(x_in, xp)
    spread(c_in, gy)
    gain1, shift1 = wide(0), wide(1)
    n_live = live[0]

    def each(body, init=0):
        def step(i, carry):
            return body(i, pl.ds(pl.multiple_of(i * half, half), half), carry)

        return lax.fori_loop(0, nhalf, step, init)

    def start(i, at, carry):
        normed, rstd = norm(xp[at, :])
        n1[at, :] = normed
        r1[at, :] = rstd
        h = normed * gain1 + shift1
        h1[at, :] = h.astype(BF16)
        h1t[:, at] = h.T.astype(BF16)
        slot = lax.div(i * half + lax.broadcasted_iota(jnp.int32, (half, 1), 0), PAD)
        g = jnp.where(slot < n_live, gy[at, :], 0.0)
        gy[at, :] = g
        gyt[:, at] = g.T.astype(BF16)
        return carry

    each(start)
    lane_head = lax.broadcasted_iota(jnp.int32, (PAD, LANES), 1) // HDIM
    ones = [(lane_head == h).astype(F32).astype(BF16) for h in range(heads)]

    def stack(value):
        return jnp.concatenate([value * ones[h] for h in range(heads)], axis=0)

    def pick(value):
        out = value[0:PAD]
        for h in range(1, heads):
            out = jnp.where(lane_head == h, value[h * PAD : (h + 1) * PAD], out)
        return out

    acc[...] = jnp.zeros_like(acc)

    def attend(t, carry):
        q = (nn(h1[...], gw[0, t][:, :LANES]) + vec[t, 2:3, :]) * SCALE
        qs[t] = q.astype(BF16)
        kv = nn(h1[...], gw[1, t])
        kvs[t, :, :LANES] = kv[:, :LANES].astype(BF16)
        kvs[t, :, LANES:] = (kv[:, LANES:] + vec[t, 3:4, :]).astype(BF16)

        def window(w, carry):
            at = pl.ds(pl.multiple_of(w * PAD, PAD), PAD)
            s = nt_dot(kvs[t, at, :LANES], stack(qs[t, at, :])) + rb[t] + mask[w]
            e = jnp.exp(s - jnp.max(s, axis=0, keepdims=True))
            p = e / rowsum(e)
            probs[t, w] = p
            att[t, at, :] = pick(tn_dot(p.astype(BF16), kvs[t, at, LANES:])).astype(BF16)
            return carry

        lax.fori_loop(0, slots, window, 0, unroll=2)
        acc[...] += nt_dot(att[t], gw[0, t][:, LANES:])
        return carry

    lax.fori_loop(0, nt, attend, 0)
    b_out, gain2, shift2 = wide(4), wide(5), wide(6)

    def middle(i, at, carry):
        x1 = xp[at, :] + acc[at, :] + b_out
        xp[at, :] = x1
        normed, rstd = norm(x1)
        n2[at, :] = normed
        r2[at, :] = rstd
        h = normed * gain2 + shift2
        low[at, :] = h.astype(BF16)
        h2t[:, at] = h.T.astype(BF16)
        return carry

    each(middle)
    acc[...] = jnp.zeros_like(acc)
    acc2[...] = jnp.zeros_like(acc2)
    gy_low = gkv
    gy_low[...] = gy[...].astype(BF16)

    def mlp(k, carry):
        t, s = lax.div(k, 2), lax.rem(k, 2)
        up, down = gw.at[2 + s, t], gw.at[4 + s, t]
        bias = vec[t, pl.ds(8 + 2 * s, 2), :]
        bias = jnp.concatenate([bias[0:1], bias[1:2]], axis=1)
        hidden = nn(low[...], up[...]) + bias
        act, slope = gelu_pair(hidden)
        act_low = act.astype(BF16)
        acc[...] += nt_dot(act_low, down[...])
        dw[4 + s, t] = nn(gyt[...], act_low).astype(BF16)
        grad = nn(gy_low[...], down[...]) * slope
        total = rowsum(grad)
        small[t, pl.ds(8 + 2 * s, 1), :] = total[:, :LANES]
        small[t, pl.ds(9 + 2 * s, 1), :] = total[:, LANES:]
        grad_low = grad.astype(BF16)
        dw[2 + s, t] = nn(h2t[...], grad_low).astype(BF16)
        acc2[...] += nt_dot(grad_low, up[...])
        return carry

    lax.fori_loop(0, 2 * nt, mlp, 0)
    b_down = wide(7)
    zero_row = jnp.zeros((1, C), F32)

    def turn(i, at, carry):
        slot = lax.div(i * half + lax.broadcasted_iota(jnp.int32, (half, 1), 0), PAD)
        xp[at, :] = jnp.where(slot < n_live, xp[at, :] + acc[at, :] + b_down, 0.0)
        e, normed, g = acc2[at, :], n2[at, :], gy[at, :]
        gx = norm_back(e * gain2, normed, r2[at, :]) + g
        gy[at, :] = gx
        low[at, :] = gx.astype(BF16)
        h2t[:, at] = gx.T.astype(BF16)
        sums = (rowsum(e * normed), rowsum(e), rowsum(gx), rowsum(g))
        return tuple(a + b for a, b in zip(carry, sums))

    sums = each(turn, (zero_row,) * 4)
    put_small(5, sums[0])
    put_small(6, sums[1])
    put_small(4, sums[2])
    put_small(7, sums[3])
    gather(xp, y_out)
    acc[...] = jnp.zeros_like(acc)

    def back(t, carry):
        gatt = gq
        dw[0, t, :, LANES:] = nn(h2t[...], att[t]).astype(BF16)
        gatt[...] = nn(low[...], gw[0, t][:, LANES:]).astype(BF16)

        def window(w, carry):
            at = pl.ds(pl.multiple_of(w * PAD, PAD), PAD)
            q4, g4 = stack(qs[t, at, :]), stack(gatt[at, :])
            p = probs[t, w]
            dp = nt_dot(kvs[t, at, LANES:], g4)
            ds = p * (dp - rowsum(p * dp))
            ds_low = ds.astype(BF16)
            pairs[t] += ds_low.astype(F32)
            gkv[at, :LANES] = nn(ds_low, q4).astype(BF16)
            gkv[at, LANES:CW] = nn(p.astype(BF16), g4).astype(BF16)
            gatt[at, :] = pick(tn_dot(ds_low, kvs[t, at, :LANES])).astype(BF16)
            return carry

        lax.fori_loop(0, slots, window, 0, unroll=2)
        gk_gv = gkv[:, :CW]
        dw[0, t, :, :LANES] = (nn(h1t[...], gatt[...]) * SCALE).astype(BF16)
        dw[1, t] = nn(h1t[...], gk_gv).astype(BF16)
        small[t, 2:3, :] = rowsum(gatt[...].astype(F32)) * SCALE
        small[t, 3:4, :] = rowsum(gkv[:, LANES:CW].astype(F32))
        acc[...] += nt_dot(gatt[...], gw[0, t][:, :LANES]) * SCALE + nt_dot(gk_gv, gw[1, t])
        return carry

    lax.fori_loop(0, nt, back, 0)

    def finish(i, at, carry):
        e, normed = acc[at, :], n1[at, :]
        xp[at, :] = norm_back(e * gain1, normed, r1[at, :]) + gy[at, :]
        sums = (rowsum(e * normed), rowsum(e))
        return tuple(a + b for a, b in zip(carry, sums))

    sums = each(finish, (zero_row,) * 2)
    put_small(0, sums[0])
    put_small(1, sums[1])
    gather(xp, g_out)


def work_call(nt, slots, live, xg, cg, gw, vg, rg, mask):
    rows, real = slots * PAD, xg.shape[1]
    heads4 = rg.shape[2]
    return pl.pallas_call(
        functools.partial(work, nt, slots),
        name="work",
        out_shape=(
            jax.ShapeDtypeStruct((nt, real, LANES), BF16),
            jax.ShapeDtypeStruct((nt, real, LANES), BF16),
            jax.ShapeDtypeStruct((NCH, nt, C, CW), BF16),
            jax.ShapeDtypeStruct((nt, SROWS, LANES), F32),
            jax.ShapeDtypeStruct((nt, PAD, heads4), F32),
        ),
        in_specs=[pl.BlockSpec(memory_space=pltpu.SMEM)] + [VM] * 6,
        out_specs=(VM,) * 5,
        scratch_shapes=[
            pltpu.VMEM((real, C), F32),
            pltpu.VMEM((rows, C), F32),
            pltpu.VMEM((rows, C), F32),
            pltpu.VMEM((rows, C), BF16),
            pltpu.VMEM((C, rows), BF16),
            pltpu.VMEM((C, rows), BF16),
            pltpu.VMEM((C, rows), BF16),
            pltpu.VMEM((nt, rows, LANES), BF16),
            pltpu.VMEM((nt, rows, CW), BF16),
            pltpu.VMEM((nt, slots, PAD, heads4), F32),
            pltpu.VMEM((nt, rows, LANES), BF16),
            pltpu.VMEM((rows, C), F32),
            pltpu.VMEM((rows, C), F32),
            pltpu.VMEM((rows, C), F32),
            pltpu.VMEM((rows, 1), F32),
            pltpu.VMEM((rows, C), F32),
            pltpu.VMEM((rows, 1), F32),
            pltpu.VMEM((rows, C), BF16),
            pltpu.VMEM((rows, C), BF16),
            pltpu.VMEM((rows, LANES), BF16),
        ],
        compiler_params=pltpu.CompilerParams(vmem_limit_bytes=56 * 2**20),
    )(live, xg, cg, gw, vg, rg, mask)


def send_back(nt, nz, nbits, y_in, g_in, dw, small, y_out, g_out, fin, tot, b0, b1, *rest):
    (dv, rc, r1a, r2a, r3, rz, sb, sc_r, sy_r, sx_r), sems = rest[:10], rest[10:]
    loc, ta_s, ta_r, k_s, k_r, p_s, p_r, q_s, q_r, z_s, z_r, s_s, s_r = sems
    a, t, x, z, c, y = place()
    xp = (z * 2 + (1 - x), t)
    yp = (a, (1 - y) * 2 + c)
    cp = (a, y * 2 + (1 - c))
    zs = [(lax.rem(z + d, nz) * 2 + x, t) for d in range(1, nz)]
    ts = [(a, lax.rem(t + d, nt)) for d in range(1, nt)]
    flips = []
    for b in range(nbits):
        bit = 2**b
        flips.append((a + bit - 2 * bit * lax.rem(lax.div(a, bit), 2), t))
    ins = [pltpu.make_async_copy(y_in.at[t], b0, loc.at[0])]
    ins.append(pltpu.make_async_copy(g_in.at[t], b1, loc.at[1]))
    for i in range(2):
        ins.append(pltpu.make_async_copy(dw.at[:, 2 * i + c], dv.at[:, i], loc.at[2 + i]))
    for copy in ins:
        copy.start()
    greet(zs + ts + flips)
    sends = []
    core = []
    for ch in range(NCH):
        for i in range(2):
            core.append(
                remote(dw.at[ch, 2 * i + 1 - c], rc.at[ch, i], k_s.at[ch, i], k_r.at[ch, i], cp)
            )
    for i in range(2):
        core.append(remote(small.at[2 * i + 1 - c], sc_r.at[i], s_s.at[i], s_r.at[i], cp))
    back = []
    for d, peer in enumerate(ts):
        for i, (src, dst) in enumerate(((y_in, y_out), (g_in, g_out))):
            back.append(remote(src.at[peer[1]], dst.at[t], ta_s.at[i, d], ta_r.at[i, d], peer))
    outs = []
    for i, (m, o) in enumerate(((b0, y_out), (b1, g_out))):
        ins[i].wait()
        outs.append(pltpu.make_async_copy(m, o.at[t], loc.at[i]))
        outs[-1].start()
    ins[2].wait()
    ins[3].wait()

    def add(left, right):
        return (left.astype(F32) + right.astype(F32)).astype(BF16)

    for i in range(2):
        core[2 * NCH + i].wait_recv()
    own_small = pltpu.make_async_copy(small, sb, loc.at[2])
    own_small.start()
    own_small.wait()
    sx_r[0] = sb[1 - y + 1 - y + c] + sc_r[1 - y]
    sx_r[1] = sb[y + y + c] + sc_r[y]
    sends.append(remote(sx_r.at[0], sy_r.at[0], s_s.at[2], s_r.at[2], yp))
    small_copy = sends[-1]
    first = []
    for ch in range(NCH):
        core[2 * ch].wait_recv()
        core[2 * ch + 1].wait_recv()
        for i in range(2):
            dv[ch, i] = add(dv[ch, i], rc[ch, i])
        if ch % 2 == 0:
            h = ch // 2
            first.append(
                (remote(dv.at[ch, 1 - y], r1a.at[h], p_s.at[ch, 0], p_r.at[ch, 0], yp),)
            )
        else:
            h = ch // 2
            first.append(
                tuple(
                    remote(
                        dv.at[ch, i, :, 1 - x], r2a.at[h, i], p_s.at[ch, i], p_r.at[ch, i], xp
                    )
                    for i in range(2)
                )
            )
    small_copy.wait_recv()
    sx_r[2] = sx_r[1] + sy_r[0]
    second = []
    for b in range(nbits):
        sends.append(
            remote(sx_r.at[2 + b], sy_r.at[1 + b], s_s.at[3 + b], s_r.at[3 + b], flips[b])
        )
        if b == 0:
            for ch in range(NCH):
                h = ch // 2
                for copy in first[ch]:
                    copy.wait_recv()
                if ch % 2 == 0:
                    dv[ch, y] = add(dv[ch, y], r1a[h])
                    second.append(
                        remote(
                            dv.at[ch, y, :, 1 - x], r3.at[ch], q_s.at[ch], q_r.at[ch], xp
                        )
                    )
                else:
                    for i in range(2):
                        dv[ch, i, :, x] = add(dv[ch, i, :, x], r2a[h, i])
                    second.append(
                        remote(
                            dv.at[ch, 1 - y, :, x], r3.at[ch], q_s.at[ch], q_r.at[ch], yp
                        )
                    )
        sends[-1].wait_recv()
        sx_r[3 + b] = sx_r[2 + b] + sy_r[1 + b]
    last = []
    for ch in range(NCH):
        second[ch].wait_recv()
        dv[ch, y, :, x] = add(dv[ch, y, :, x], r3[ch])
        for d, peer in enumerate(zs):
            last.append(
                remote(
                    dv.at[ch, y, lax.rem(z + d + 1, nz), x],
                    rz.at[ch, d],
                    z_s.at[ch, d],
                    z_r.at[ch, d],
                    peer,
                )
            )
    for ch in range(NCH):
        for d in range(nz - 1):
            last[ch * (nz - 1) + d].wait_recv()
        value = dv[ch, y, z, x].astype(F32)
        for d in range(nz - 1):
            value = value + rz[ch, d].astype(F32)
        fin[ch] = value
    tot[...] = sx_r[2 + nbits]
    for copy in back:
        copy.wait_recv()
    for copy in core + back + sends + second + last:
        copy.wait_send()
    for group in first:
        for copy in group:
            copy.wait_send()
    for copy in outs:
        copy.wait()


def back_call(nt, nz, y_in, g_in, dw, small):
    rows, deep = y_in.shape[1], dw.shape[4]
    nbits = (2 * nz - 1).bit_length()
    sem = pltpu.SemaphoreType.DMA
    return pl.pallas_call(
        functools.partial(send_back, nt, nz, nbits),
        name="send_back",
        out_shape=(
            jax.ShapeDtypeStruct((nt, rows, LANES), BF16),
            jax.ShapeDtypeStruct((nt, rows, LANES), BF16),
            jax.ShapeDtypeStruct((NCH, deep, CW), F32),
            jax.ShapeDtypeStruct(small.shape[1:], F32),
        ),
        in_specs=[ANY] * 4,
        out_specs=(ANY, ANY, VM, VM),
        scratch_shapes=[
            pltpu.VMEM((rows, LANES), BF16),
            pltpu.VMEM((rows, LANES), BF16),
            pltpu.VMEM((NCH, 2, nz, 2, deep, CW), BF16),
            pltpu.VMEM((NCH, 2, nz, 2, deep, CW), BF16),
            pltpu.VMEM((NCH // 2, nz, 2, deep, CW), BF16),
            pltpu.VMEM((NCH // 2, 2, nz, deep, CW), BF16),
            pltpu.VMEM((NCH, nz, deep, CW), BF16),
            pltpu.VMEM((NCH, nz - 1, deep, CW), BF16),
            pltpu.VMEM(small.shape, F32),
            pltpu.VMEM((2,) + small.shape[1:], F32),
            pltpu.VMEM((1 + nbits,) + small.shape[1:], F32),
            pltpu.VMEM((3 + nbits,) + small.shape[1:], F32),
            sem((4,)),
            sem((2, nt - 1)),
            sem((2, nt - 1)),
            sem((NCH, 2)),
            sem((NCH, 2)),
            sem((NCH, 2)),
            sem((NCH, 2)),
            sem((NCH,)),
            sem((NCH,)),
            sem((NCH, nz - 1)),
            sem((NCH, nz - 1)),
            sem((3 + nbits,)),
            sem((3 + nbits,)),
        ],
        compiler_params=pltpu.CompilerParams(collective_id=1, has_side_effects=True),
    )(y_in, g_in, dw, small)


def per_device(
    nt, na, tokens, gain_one, shift_one, w_query, w_key, w_value, b_query, b_value, w_out, b_out,
    gain_two, shift_two, w_hidden, b_hidden, w_down, b_down, bias_table, rel_index, region,
    win_count, cotangent,
):
    nz = na // 2
    heads = bias_table.shape[1]
    slots = region.shape[0] // nt
    real = slots * WT
    deep = w_query.shape[0]
    t = lax.axis_index("ta")
    tok = tokens.reshape(nt, real, LANES)
    cot = cotangent.reshape(nt, real, LANES)
    wp = jnp.stack(
        [
            jnp.concatenate([w_query, w_out.T], axis=1),
            jnp.concatenate([w_key, w_value], axis=1),
            w_hidden[:, :CW],
            w_hidden[:, CW:],
            w_down[:CW].T,
            w_down[CW:].T,
        ]
    )
    onehot = rel_index.T.reshape(-1)[:, None] == jnp.arange(TPAD, dtype=jnp.int32)[None, :]
    onehot = onehot.astype(F32)
    table = jnp.pad(bias_table, ((0, TPAD - TABLE), (0, 0)))
    flat = lax.dot_general(
        table, onehot, (((0,), (1,)), ((), ())), precision=lax.Precision.HIGHEST,
        preferred_element_type=F32,
    )
    edge = PAD - WT
    rb = jnp.pad(flat.reshape(heads, WT, WT), ((0, 0), (0, edge), (0, edge)))
    rb = rb.transpose(1, 0, 2).reshape(PAD, heads * PAD)
    vec = [gain_one, shift_one, b_query, b_value, b_out, gain_two, shift_two, b_down, b_hidden]
    vec = jnp.pad(jnp.concatenate(vec).reshape(-1, LANES), ((0, SROWS - 12), (0, 0)))
    mine = lax.dynamic_slice_in_dim(region, t * slots, slots, 0)
    mine = jnp.pad(mine, ((0, 0), (0, edge)))
    mask = jnp.where(mine[:, :, None] == mine[:, None, :], 0.0, -100.0).astype(F32)
    keep = jnp.arange(PAD, dtype=jnp.int32)[None, :, None] < WT
    mask = jnp.where(keep, mask, -1e30)
    mask = jnp.tile(mask, (1, 1, heads))
    live = win_count - t * slots
    xg, cg, gw, vg, rg = bring_call(nt, nz, tok, cot, wp, vec, rb)
    gw = gw.reshape(NCH, nt, C, CW)
    y_loc, g_loc, dw, small, pairs = work_call(nt, slots, live, xg, cg, gw, vg, rg, mask)
    pairs = pairs.reshape(nt, PAD, heads, PAD)[:, :WT, :, :WT].transpose(0, 2, 1, 3)
    part = jnp.dot(
        pairs.reshape(nt * heads, WT * WT), onehot, precision=lax.Precision.HIGHEST,
        preferred_element_type=F32,
    )
    part = part.reshape(nt, heads * TPAD // LANES, LANES)
    small = jnp.concatenate([small[:, :12], part, small[:, 20:]], axis=1)
    y_all, g_all, fin, tot = back_call(
        nt, nz, y_loc, g_loc, dw.reshape(NCH, nt, nz, 2, deep, CW), small
    )
    rows = tokens.shape[0]
    y_out = y_all.reshape(rows, LANES).astype(F32)
    grad_tokens = g_all.reshape(rows, LANES).astype(F32)
    return (
        y_out,
        grad_tokens,
        tot[0],
        tot[1],
        fin[0, :, :LANES],
        fin[1, :, :LANES],
        fin[1, :, LANES:],
        tot[2],
        tot[3],
        fin[0, :, LANES:].T,
        tot[4],
        tot[5],
        tot[6],
        jnp.concatenate([fin[2], fin[3]], axis=1),
        tot[8:12].reshape(-1),
        jnp.concatenate([fin[4].T, fin[5].T], axis=0),
        tot[7],
        tot[12:20].reshape(heads, TPAD)[:, :TABLE].T,
    )


def solution(mesh):
    return jax.shard_map(
        functools.partial(per_device, mesh.shape["ta"], mesh.shape["wa"]),
        mesh=mesh,
        in_specs=(
            P("wa", "ta"),
            P("ta"),
            P("ta"),
            P("wa", "ta"),
            P("wa", "ta"),
            P("wa", "ta"),
            P("ta"),
            P("ta"),
            P("ta", "wa"),
            P("ta"),
            P("ta"),
            P("ta"),
            P("wa", "ta"),
            P("ta"),
            P("ta", "wa"),
            P("ta"),
            P(None, "ta"),
            P(),
            P("wa", None),
            P("wa"),
            P("wa", "ta"),
        ),
        out_specs=(
            P("wa", "ta"),
            P("wa", "ta"),
            P("ta"),
            P("ta"),
            P("wa", "ta"),
            P("wa", "ta"),
            P("wa", "ta"),
            P("ta"),
            P("ta"),
            P("ta", "wa"),
            P("ta"),
            P("ta"),
            P("ta"),
            P("wa", "ta"),
            P("ta"),
            P("ta", "wa"),
            P("ta"),
            P(None, "ta"),
        ),
        check_vma=False,
    )
```

```python
import functools

import jax
import jax.numpy as jnp
from jax import lax
from jax.experimental import pallas as pl
from jax.experimental.pallas import tpu as pltpu
from jax.sharding import PartitionSpec as P

C = 512
HDIM = 32
WT = 49
PAD = 64
TABLE = 169
TPAD = 256
NCH = 6
CW = 256
LANES = 128
SROWS = 24
SCALE = HDIM ** (-0.5)
EPS = 1e-05
F32 = jnp.float32
BF16 = jnp.bfloat16
MESH = pl.DeviceIdType.MESH
ANY = pl.BlockSpec(memory_space=pl.ANY)
VM = pl.BlockSpec(memory_space=pltpu.VMEM)
SM = pl.BlockSpec(memory_space=pltpu.SMEM)
DMA = pltpu.SemaphoreType.DMA


def flip(bit, by):
    return bit + by - 2 * bit * by


def add(left, right):
    return (left.astype(F32) + right.astype(F32)).astype(BF16)


def nn(left, right):
    return jnp.dot(left, right, preferred_element_type=F32)


def nt_dot(left, right):
    return lax.dot_general(left, right, (((1,), (1,)), ((), ())), preferred_element_type=F32)


def tn_dot(left, right):
    return lax.dot_general(left, right, (((0,), (0,)), ((), ())), preferred_element_type=F32)


def norm(value):
    mean = jnp.mean(value, axis=1, keepdims=True)
    spread = jnp.mean(value * value, axis=1, keepdims=True) - mean * mean
    rstd = lax.rsqrt(spread + EPS)
    return (value - mean) * rstd, rstd


def norm_back(scaled, normed, rstd):
    first = jnp.mean(scaled, axis=1, keepdims=True)
    second = jnp.mean(scaled * normed, axis=1, keepdims=True)
    return rstd * (scaled - first - normed * second)


def gelu_pair(u):
    cdf = 0.5 + 0.5 * lax.erf(u * (0.5**0.5))
    pdf = jnp.exp(-0.5 * u * u) * ((2.0 * jnp.pi) ** -0.5)
    return u * cdf, cdf + u * pdf


def rowsum(value):
    return jnp.sum(value, axis=0, keepdims=True)


def block(nt, nz, slots, nbits, *refs):
    (
        live, tok, cot, wq, wk, wv, wo, wh, wd, g1, s1, bq, bv, bo, g2, s2, bd, bh, tab, rel, reg,
        y_all, g_all, fin, tot,
        xg, cg, gw, vg, rg, dv, rc, ry, rx, r3, rz, scr, syr, sx, small, yb, gb, square, mask, inv,
        xs, xp, gy, h1, h1t, h2t, gyt, qs, kvs, probs, att, acc, acc2, n1, r1, n2, r2, low, gkv, gq,
        pairs,
        loc, tok_s, tok_r, out_s, out_r, az_s, az_r, ax_s, ax_r, ay_s, ay_r, ac_s, ac_r,
        bx_s, bx_r, k_s, k_r, p_s, p_r, q_s, q_r, rz_s, rz_r, sm_s, sm_r,
    ) = refs
    heads = LANES // HDIM
    rows = slots * PAD
    half = 2 * PAD
    nhalf = rows // half
    a, t = lax.axis_index("wa"), lax.axis_index("ta")
    x, z, c, y = lax.rem(a, 2), lax.div(a, 2), lax.rem(t, 2), lax.div(t, 2)

    def group(m):
        return 2 * flip(y, m // 2 if isinstance(m, int) else lax.div(m, 2)) + flip(
            c, m % 2 if isinstance(m, int) else lax.rem(m, 2)
        )

    t1, t2, t3 = group(1), group(2), group(3)
    xpeer, ypeer, cpeer = (z * 2 + (1 - x), t), (a, t2), (a, t1)
    zs = [(lax.rem(z + d, nz) * 2 + x, t) for d in range(1, nz)]
    ts = [(a, tt) for tt in (t1, t2, t3)]
    flips = []
    for b in range(nbits):
        bit = 2**b
        flips.append((a + bit - 2 * bit * lax.rem(lax.div(a, bit), 2), t))
    peers = zs + ts + [xpeer]
    barrier = pltpu.get_barrier_semaphore()
    for peer in peers:
        pl.semaphore_signal(barrier, inc=1, device_id=peer, device_id_type=MESH)

    def far(src, dst, send, recv, peer):
        return pltpu.make_async_remote_copy(
            src_ref=src, dst_ref=dst, send_sem=send, recv_sem=recv, device_id=peer,
            device_id_type=MESH,
        )

    def tok_copy(i, d):
        src, dst = ((tok, xg), (cot, cg), (vg, vg), (rg, rg))[i]
        peer = ts[d]
        src = src.at[peer[1]] if i < 2 else src.at[t]
        return far(src, dst.at[t], tok_s.at[i, d], tok_r.at[i, d], peer)

    def out_copy(i, d):
        src, dst = ((yb, y_all), (gb, g_all))[i]
        peer = ts[d]
        return far(src.at[peer[1]], dst.at[t], out_s.at[i, d], out_r.at[i, d], peer)

    def az(ch, d):
        ref = gw.at[ch, t, z, x]
        return far(ref, ref, az_s.at[ch, d], az_r.at[ch, d], zs[d])

    def ax(ch, d):
        ref = gw.at[ch, t, lax.rem(z + nz - d, nz), x]
        return far(ref, ref, ax_s.at[ch, d], ax_r.at[ch, d], xpeer)

    def ay(ch, d):
        ref = gw.at[ch, t, lax.rem(z + nz - d, nz)]
        return far(ref, ref, ay_s.at[ch, d], ay_r.at[ch, d], ypeer)

    def by(ch):
        ref = gw.at[ch, t, :, x]
        return far(ref, ref, ay_s.at[ch, 0], ay_r.at[ch, 0], ypeer)

    def bx(ch, j):
        ref = gw.at[ch, t2 if j else t, :, x]
        return far(ref, ref, bx_s.at[ch, j], bx_r.at[ch, j], xpeer)

    def ac(ch, j):
        ref = gw.at[ch, t2 if j else t]
        return far(ref, ref, ac_s.at[ch, j], ac_r.at[ch, j], cpeer)

    def kc(ch, j):
        return far(dv.at[ch, t1 if j else t3], rc.at[ch, j], k_s.at[ch, j], k_r.at[ch, j], cpeer)

    def ya(ch):
        return far(dv.at[ch, t2], ry.at[ch], p_s.at[ch, 0], p_r.at[ch, 0], ypeer)

    def xa(ch):
        return far(dv.at[ch, t, :, 1 - x], r3.at[ch], q_s.at[ch], q_r.at[ch], xpeer)

    def xb(ch, j):
        src = dv.at[ch, t if j else t2, :, 1 - x]
        return far(src, rx.at[ch - 4, j], p_s.at[ch, j], p_r.at[ch, j], xpeer)

    def yb2(ch):
        return far(dv.at[ch, t2, :, x], r3.at[ch], q_s.at[ch], q_r.at[ch], ypeer)

    def zr(ch, d):
        src = dv.at[ch, t, lax.rem(z + d + 1, nz), x]
        return far(src, rz.at[ch, d], rz_s.at[ch, d], rz_r.at[ch, d], zs[d])

    def core_first(ch):
        kc(ch, 0).wait_recv()
        dv[ch, t2] = add(dv[ch, t2], rc[ch, 0])

    def core_second(ch):
        kc(ch, 1).wait_recv()
        dv[ch, t] = add(dv[ch, t], rc[ch, 1])

    def second_a(ch):
        ya(ch).wait_recv()
        dv[ch, t] = add(dv[ch, t], ry[ch])
        xa(ch).start()

    def second_b(ch):
        for j, tt in enumerate((t2, t)):
            xb(ch, j).wait_recv()
            dv[ch, tt, :, x] = add(dv[ch, tt, :, x], rx[ch - 4, j])
        yb2(ch).start()

    def third(ch):
        (xa(ch) if ch < 4 else yb2(ch)).wait_recv()
        dv[ch, t, :, x] = add(dv[ch, t, :, x], r3[ch])
        for d in range(nz - 1):
            zr(ch, d).start()

    def fourth(ch):
        value = dv[ch, t, z, x].astype(F32)
        for d in range(nz - 1):
            zr(ch, d).wait_recv()
            value = value + rz[ch, d].astype(F32)
        fin[ch] = value

    def small_core(j):
        return far(small.at[t1 if j else t3], scr.at[j], sm_s.at[j], sm_r.at[j], cpeer)

    def small_y():
        return far(sx.at[0], syr.at[0], sm_s.at[2], sm_r.at[2], ypeer)

    def small_flip(b):
        return far(sx.at[2 + b], syr.at[1 + b], sm_s.at[3 + b], sm_r.at[3 + b], flips[b])

    def flat(value):
        return value.astype(F32).T.astype(BF16)

    gw[0, t, z, x, :, :LANES] = wq[...]
    gw[0, t, z, x, :, LANES:] = flat(wo[...])
    gw[1, t, z, x, :, :LANES] = wk[...]
    gw[1, t, z, x, :, LANES:] = wv[...]
    for i, ref in enumerate((g1, s1, bq, bv, bo, g2, s2, bd)):
        vg[t, i : i + 1, :] = ref[...]
    vg[t, 8:12, :] = bh[...]
    vg[t, 12:, :] = jnp.zeros((SROWS - 12, LANES), F32)
    pl.semaphore_wait(barrier, len(peers))
    own_tok = pltpu.make_async_copy(tok.at[t], xg.at[t], loc.at[0])
    own_cot = pltpu.make_async_copy(cot.at[t], cg.at[t], loc.at[1])
    own_tok.start()
    own_cot.start()
    for ch in range(2):
        for d in range(nz - 1):
            az(ch, d).start()
        ax(ch, 0).start()
    for d in range(3):
        tok_copy(0, d).start()
    for d in range(3):
        tok_copy(2, d).start()
    square[...] = jnp.zeros_like(square)
    square[:TABLE, :heads] = tab[...]
    table = square[...].T
    square[...] = jnp.zeros_like(square)
    square[:WT, :WT] = rel[...].astype(F32)
    rel_t = square[:LANES, :].T[:PAD, :PAD]
    pick_at = jnp.concatenate([rel_t, rel_t], axis=1).astype(jnp.int32)
    lane = lax.broadcasted_iota(jnp.int32, (PAD, LANES), 1)
    low_at, high_at = jnp.minimum(pick_at, LANES - 1), jnp.maximum(pick_at - LANES, 0)

    def take(value, at):
        return jnp.take_along_axis(value, at, axis=1, mode="promise_in_bounds")

    def entry(h):
        first = jnp.broadcast_to(table[h : h + 1, :LANES], (PAD, LANES))
        second = jnp.broadcast_to(table[h : h + 1, LANES:], (PAD, LANES))
        return jnp.where(pick_at < LANES, take(first, low_at), take(second, high_at))

    for q in range(heads // 2):
        rg[t, :, q * LANES : (q + 1) * LANES] = jnp.where(
            lane < PAD, entry(2 * q), entry(2 * q + 1)
        )
    for d in range(3):
        tok_copy(3, d).start()
    number = lax.broadcasted_iota(jnp.int32, (PAD, TPAD), 1).astype(F32)
    found = jnp.full((PAD, TPAD), -1.0, F32)
    for i in range(WT):
        found = jnp.where(rel_t[:, i : i + 1] == number, float(i), found)
    inv[...] = found.astype(jnp.int32)
    square[...] = jnp.zeros_like(square)
    mine = reg[pl.ds(pl.multiple_of(t * slots, slots), slots), :]
    square[:slots, :WT] = mine.astype(F32)
    reg_row = square[:slots, :PAD]
    reg_row = jnp.concatenate([reg_row] * heads, axis=1)
    reg_col = square[:LANES, :].T[:PAD, :slots]
    real = lax.broadcasted_iota(jnp.int32, (PAD, heads * PAD), 0) < WT
    for w in range(slots):
        same = reg_col[:, w : w + 1] == reg_row[w : w + 1, :]
        mask[w] = jnp.where(real, jnp.where(same, 0.0, -100.0), -1e30)
    for s in range(2):
        gw[2 + s, t, z, x] = wh[:, s * CW : (s + 1) * CW]
        gw[4 + s, t, z, x] = flat(wd[s * CW : (s + 1) * CW, :])
    for ch in range(2):
        for d in range(nz - 1):
            az(ch, d).wait_recv()
            ax(ch, d + 1).start()
    for ch in (2, 4, 3, 5):
        for d in range(nz - 1):
            az(ch, d).start()

    def wide(i):
        return jnp.concatenate([vg[tt, i : i + 1, :] for tt in range(nt)], axis=1)

    def put_small(i, value):
        for tt in range(nt):
            small[tt, i : i + 1, :] = value[:, tt * LANES : (tt + 1) * LANES]

    def spread(source, target):
        for tt in range(nt):
            xs[:, tt * LANES : (tt + 1) * LANES] = source[tt].astype(F32)
        zero = jnp.zeros((PAD - WT, C), F32)
        for w in range(slots):
            target[w * PAD : w * PAD + WT, :] = xs[w * WT : (w + 1) * WT, :]
            target[w * PAD + WT : (w + 1) * PAD, :] = zero

    def gather(source, target):
        for w in range(slots):
            xs[w * WT : (w + 1) * WT, :] = source[w * PAD : w * PAD + WT, :]
        for tt in range(nt):
            target[tt] = xs[:, tt * LANES : (tt + 1) * LANES].astype(BF16)

    def each(body, init=0):
        def step(i, carry):
            return body(i, pl.ds(pl.multiple_of(i * half, half), half), carry)

        return lax.fori_loop(0, nhalf, step, init)

    def weight(ch, tt, start=0, size=CW):
        return gw[ch, tt, :, :, :, start : start + size].reshape(C, size)

    def put_grad(ch, tt, value):
        dv[ch, tt] = value.astype(BF16).reshape(dv.shape[2:])

    n_live = live[0] - t * slots
    small[...] = jnp.zeros_like(small)
    own_tok.wait()
    for i in (0, 2):
        for d in range(3):
            tok_copy(i, d).wait_recv()
    spread(xg, xp)
    gain1, shift1 = wide(0), wide(1)

    def start(i, at, carry):
        normed, rstd = norm(xp[at, :])
        n1[at, :] = normed
        r1[at, :] = rstd
        h = normed * gain1 + shift1
        h1[at, :] = h.astype(BF16)
        h1t[:, at] = h.T.astype(BF16)
        return carry

    each(start)
    for ch in range(2):
        for d in range(nz):
            ax(ch, d).wait_recv()
            ay(ch, d).start()
        ac(ch, 0).start()
    for d in range(3):
        tok_copy(3, d).wait_recv()
    for d in range(3):
        tok_copy(1, d).start()
    lane_head = lax.broadcasted_iota(jnp.int32, (PAD, LANES), 1) // HDIM
    ones = [(lane_head == h).astype(F32).astype(BF16) for h in range(heads)]

    def stack(value):
        return jnp.concatenate([value * ones[h] for h in range(heads)], axis=0)

    def pick(value):
        out = value[0:PAD]
        for h in range(1, heads):
            out = jnp.where(lane_head == h, value[h * PAD : (h + 1) * PAD], out)
        return out

    acc[...] = jnp.zeros_like(acc)

    def attend(i, carry):
        tt = group(i)

        @pl.when(i == 1)
        def _():
            for ch in range(2):
                ac(ch, 0).wait_recv()

        @pl.when(i == 2)
        def _():
            for ch in range(2):
                for d in range(nz):
                    ay(ch, d).wait_recv()
                ac(ch, 1).start()

        @pl.when(i == 3)
        def _():
            for ch in range(2):
                ac(ch, 1).wait_recv()

        q = (nn(h1[...], weight(0, tt, 0, LANES)) + vg[tt, 2:3, :]) * SCALE
        qs[tt] = q.astype(BF16)
        kv = nn(h1[...], weight(1, tt))
        kvs[tt, :, :LANES] = kv[:, :LANES].astype(BF16)
        kvs[tt, :, LANES:] = (kv[:, LANES:] + vg[tt, 3:4, :]).astype(BF16)

        def window(w, carry):
            at = pl.ds(pl.multiple_of(w * PAD, PAD), PAD)
            s = nt_dot(kvs[tt, at, :LANES], stack(qs[tt, at, :])) + rg[tt] + mask[w]
            e = jnp.exp(s - jnp.max(s, axis=0, keepdims=True))
            p = e / rowsum(e)
            probs[tt, w] = p
            att[tt, at, :] = pick(tn_dot(p.astype(BF16), kvs[tt, at, LANES:])).astype(BF16)
            return carry

        lax.fori_loop(0, slots, window, 0, unroll=2)
        acc[...] += nt_dot(att[tt], weight(0, tt, LANES, LANES))

        def feed(chs):
            for ch in chs:
                for d in range(nz - 1):
                    az(ch, d).wait_recv()
                by(ch).start()

        def feed_x(chs):
            for ch in chs:
                by(ch).wait_recv()
                for j in range(2):
                    bx(ch, j).start()

        @pl.when(i == 0)
        def _():
            feed((2, 4))

        @pl.when(i == 1)
        def _():
            feed((3, 5))

        @pl.when(i == 2)
        def _():
            feed_x((2, 4))

        @pl.when(i == 3)
        def _():
            feed_x((3, 5))

        return carry

    lax.fori_loop(0, nt, attend, 0)

    def feed_core(chs):
        for ch in chs:
            for j in range(2):
                bx(ch, j).wait_recv()
            for j in range(2):
                ac(ch, j).start()

    own_cot.wait()
    for d in range(3):
        tok_copy(1, d).wait_recv()
    spread(cg, gy)
    feed_core((2, 4))
    b_out, gain2, shift2 = wide(4), wide(5), wide(6)

    def live_rows(i):
        slot = lax.div(i * half + lax.broadcasted_iota(jnp.int32, (half, 1), 0), PAD)
        return slot < n_live

    def middle(i, at, carry):
        x1 = xp[at, :] + acc[at, :] + b_out
        xp[at, :] = x1
        normed, rstd = norm(x1)
        n2[at, :] = normed
        r2[at, :] = rstd
        h = normed * gain2 + shift2
        low[at, :] = h.astype(BF16)
        h2t[:, at] = h.T.astype(BF16)
        g = jnp.where(live_rows(i), gy[at, :], 0.0)
        gy[at, :] = g
        gkv[at, :] = g.astype(BF16)
        gyt[:, at] = g.T.astype(BF16)
        return carry

    each(middle)
    acc[...] = jnp.zeros_like(acc)
    acc2[...] = jnp.zeros_like(acc2)
    for ch in (2, 4):
        for j in range(2):
            ac(ch, j).wait_recv()

    def mlp(k, carry):
        s, i = lax.div(k, nt), lax.rem(k, nt)
        tt = group(3 - i)
        up, down = 2 + s, 4 + s

        @pl.when(k == 2)
        def _():
            feed_core((3, 5))

        @pl.when(k == 4)
        def _():
            for ch in (3, 5):
                for j in range(2):
                    ac(ch, j).wait_recv()

        bias = vg[tt, pl.ds(8 + 2 * s, 2), :]
        bias = jnp.concatenate([bias[0:1], bias[1:2]], axis=1)
        hidden = nn(low[...], weight(up, tt)) + bias
        act, slope = gelu_pair(hidden)
        act_low = act.astype(BF16)
        acc[...] += nt_dot(act_low, weight(down, tt))
        put_grad(down, tt, nn(gyt[...], act_low))
        grad = nn(gkv[...], weight(down, tt)) * slope
        total = rowsum(grad)
        small[tt, pl.ds(8 + 2 * s, 1), :] = total[:, :LANES]
        small[tt, pl.ds(9 + 2 * s, 1), :] = total[:, LANES:]
        grad_low = grad.astype(BF16)
        put_grad(up, tt, nn(h2t[...], grad_low))
        acc2[...] += nt_dot(grad_low, weight(up, tt))

        @pl.when(i == 0)
        def _():
            kc(down, 0).start()
            kc(up, 0).start()

        @pl.when(i == 1)
        def _():
            core_first(up)
            ya(up).start()
            core_first(down)

        @pl.when(i == 2)
        def _():
            kc(down, 1).start()
            kc(up, 1).start()

        @pl.when(i == 3)
        def _():
            core_second(down)
            for j in range(2):
                xb(down, j).start()
            core_second(up)

        return carry

    lax.fori_loop(0, 2 * nt, mlp, 0)
    second_a(2)
    second_b(4)
    b_down = wide(7)
    zero_row = jnp.zeros((1, C), F32)

    def turn(i, at, carry):
        xp[at, :] = jnp.where(live_rows(i), xp[at, :] + acc[at, :] + b_down, 0.0)
        e, normed, g = acc2[at, :], n2[at, :], gy[at, :]
        gx = norm_back(e * gain2, normed, r2[at, :]) + g
        gy[at, :] = gx
        low[at, :] = gx.astype(BF16)
        h2t[:, at] = gx.T.astype(BF16)
        sums = (rowsum(e * normed), rowsum(e), rowsum(gx), rowsum(g))
        return tuple(p + q for p, q in zip(carry, sums))

    sums = each(turn, (zero_row,) * 4)
    put_small(5, sums[0])
    put_small(6, sums[1])
    put_small(4, sums[2])
    put_small(7, sums[3])
    gather(xp, yb)
    own_y = pltpu.make_async_copy(yb.at[t], y_all.at[t], loc.at[2])
    own_y.start()
    for d in range(3):
        out_copy(0, d).start()
    acc[...] = jnp.zeros_like(acc)

    def back(i, carry):
        tt = group(3 - i)
        gatt = gq
        gatt[...] = nn(low[...], weight(0, tt, LANES, LANES)).astype(BF16)
        pairs[...] = jnp.zeros_like(pairs)

        def window(w, carry):
            at = pl.ds(pl.multiple_of(w * PAD, PAD), PAD)
            q4, g4 = stack(qs[tt, at, :]), stack(gatt[at, :])
            p = probs[tt, w]
            dp = nt_dot(kvs[tt, at, LANES:], g4)
            ds = p * (dp - rowsum(p * dp))
            ds_low = ds.astype(BF16)
            pairs[...] += ds_low.astype(F32)
            gkv[at, :LANES] = nn(ds_low, q4).astype(BF16)
            gkv[at, LANES:CW] = nn(p.astype(BF16), g4).astype(BF16)
            gatt[at, :] = pick(tn_dot(ds_low, kvs[tt, at, :LANES])).astype(BF16)
            return carry

        lax.fori_loop(0, slots, window, 0, unroll=2)
        gk_gv = gkv[:, :CW]
        put_grad(1, tt, nn(h1t[...], gk_gv))
        left = nn(h1t[...], gatt[...]) * SCALE
        put_grad(0, tt, jnp.concatenate([left, nn(h2t[...], att[tt])], axis=1))

        @pl.when(i == 0)
        def _():
            kc(1, 0).start()
            kc(0, 0).start()

        @pl.when(i == 2)
        def _():
            kc(1, 1).start()
            kc(0, 1).start()

        small[tt, 2:3, :] = rowsum(gatt[...].astype(F32)) * SCALE
        small[tt, 3:4, :] = rowsum(gkv[:, LANES:CW].astype(F32))
        grad_q = nt_dot(gatt[...], weight(0, tt, 0, LANES)) * SCALE
        acc[...] += grad_q + nt_dot(gk_gv, weight(1, tt))
        for h in range(heads):
            lanes = h // 2 * LANES
            source = pairs[:, lanes : lanes + LANES]
            for q in range(TPAD // LANES):
                where = inv[:, q * LANES : (q + 1) * LANES]
                value = take(source, jnp.maximum(where, 0) + h % 2 * PAD)
                value = jnp.where(where >= 0, value, 0.0)
                small[tt, pl.ds(12 + 2 * h + q, 1), :] = rowsum(value)

        @pl.when(i == 0)
        def _():
            third(2)
            third(4)

        @pl.when(i == 1)
        def _():
            for ch in range(2):
                core_first(ch)
                ya(ch).start()
            second_a(3)
            second_b(5)

        @pl.when(i == 2)
        def _():
            third(3)
            third(5)
            fourth(2)
            fourth(4)

        @pl.when(i == 3)
        def _():
            for ch in range(2):
                core_second(ch)

        return carry

    lax.fori_loop(0, nt, back, 0)

    def finish(i, at, carry):
        e, normed = acc[at, :], n1[at, :]
        xp[at, :] = norm_back(e * gain1, normed, r1[at, :]) + gy[at, :]
        sums = (rowsum(e * normed), rowsum(e))
        return tuple(p + q for p, q in zip(carry, sums))

    sums = each(finish, (zero_row,) * 2)
    put_small(0, sums[0])
    put_small(1, sums[1])
    for j in range(2):
        small_core(j).start()
    second_a(0)
    gather(xp, gb)
    own_g = pltpu.make_async_copy(gb.at[t], g_all.at[t], loc.at[3])
    own_g.start()
    for d in range(3):
        out_copy(1, d).start()
    for j in range(2):
        small_core(j).wait_recv()
    sx[0] = small[t2] + scr[0]
    sx[1] = small[t] + scr[1]
    small_y().start()
    second_a(1)
    small_y().wait_recv()
    sx[2] = sx[1] + syr[0]
    small_flip(0).start()
    fourth(3)
    third(0)
    third(1)
    fourth(5)
    for b in range(nbits):
        small_flip(b).wait_recv()
        sx[3 + b] = sx[2 + b] + syr[1 + b]
        if b + 1 < nbits:
            small_flip(b + 1).start()
    fourth(0)
    fourth(1)
    tot[...] = sx[2 + nbits]
    for i in range(2):
        for d in range(3):
            out_copy(i, d).wait_recv()
    sent = [tok_copy(i, d) for i in range(4) for d in range(3)]
    sent += [out_copy(i, d) for i in range(2) for d in range(3)]
    for ch in range(NCH):
        sent += [az(ch, d) for d in range(nz - 1)] + [zr(ch, d) for d in range(nz - 1)]
        sent += [ac(ch, j) for j in range(2)] + [kc(ch, j) for j in range(2)]
        if ch < 2:
            sent += [ax(ch, d) for d in range(nz)] + [ay(ch, d) for d in range(nz)]
        else:
            sent += [by(ch), bx(ch, 0), bx(ch, 1)]
        sent += [ya(ch), xa(ch)] if ch < 4 else [xb(ch, 0), xb(ch, 1), yb2(ch)]
    sent += [small_core(0), small_core(1), small_y()] + [small_flip(b) for b in range(nbits)]
    for copy in sent:
        copy.wait_send()
    own_y.wait()
    own_g.wait()


def block_call(nt, nz, slots, *args):
    tok, deep, heads = args[1], args[3].shape[0], args[18].shape[1]
    real = tok.shape[1]
    rows, wide = slots * PAD, heads * PAD
    nbits = (2 * nz - 1).bit_length()
    piece = (nz, 2, deep, CW)
    row = (nt, real, LANES)

    def vm(shape, kind=BF16):
        return pltpu.VMEM(shape, kind)

    def pair(*shape):
        return [DMA(shape), DMA(shape)]

    small = (SROWS, LANES)
    return pl.pallas_call(
        functools.partial(block, nt, nz, slots, nbits),
        name="block",
        out_shape=(
            jax.ShapeDtypeStruct(row, BF16),
            jax.ShapeDtypeStruct(row, BF16),
            jax.ShapeDtypeStruct((NCH, deep, CW), F32),
            jax.ShapeDtypeStruct(small, F32),
        ),
        in_specs=[SM, ANY, ANY] + [VM] * 18,
        out_specs=(ANY, ANY, VM, VM),
        scratch_shapes=[
            vm(row),
            vm(row),
            vm((NCH, nt) + piece),
            vm((nt,) + small, F32),
            vm((nt, PAD, wide), F32),
            vm((NCH, nt) + piece),
            vm((NCH, 2) + piece),
            vm((4,) + piece),
            vm((2, 2, nz, deep, CW)),
            vm((NCH, nz, deep, CW)),
            vm((NCH, nz - 1, deep, CW)),
            vm((2,) + small, F32),
            vm((1 + nbits,) + small, F32),
            vm((3 + nbits,) + small, F32),
            vm((nt,) + small, F32),
            vm(row),
            vm(row),
            vm((TPAD, LANES), F32),
            vm((slots, PAD, wide), F32),
            vm((PAD, TPAD), jnp.int32),
            vm((real, C), F32),
            vm((rows, C), F32),
            vm((rows, C), F32),
            vm((rows, C)),
            vm((C, rows)),
            vm((C, rows)),
            vm((C, rows)),
            vm((nt, rows, LANES)),
            vm((nt, rows, CW)),
            vm((nt, slots, PAD, wide), F32),
            vm((nt, rows, LANES)),
            vm((rows, C), F32),
            vm((rows, C), F32),
            vm((rows, C), F32),
            vm((rows, 1), F32),
            vm((rows, C), F32),
            vm((rows, 1), F32),
            vm((rows, C)),
            vm((rows, C)),
            vm((rows, LANES)),
            vm((PAD, wide), F32),
            DMA((4,)),
        ]
        + pair(4, 3)
        + pair(2, 3)
        + pair(NCH, nz - 1)
        + pair(2, nz)
        + pair(NCH, nz)
        + pair(NCH, 2)
        + pair(NCH, 2)
        + pair(NCH, 2)
        + pair(NCH, 2)
        + pair(NCH)
        + pair(NCH, nz - 1)
        + pair(3 + nbits),
        compiler_params=pltpu.CompilerParams(
            collective_id=0, has_side_effects=True, vmem_limit_bytes=60 * 2**20
        ),
    )(*args)


def spell(y_all, g_all, fin, tot, *outs):
    (
        y_out, g_out, d_g1, d_s1, d_wq, d_wk, d_wv, d_bq, d_bv, d_wo, d_bo, d_g2, d_s2, d_wh, d_bh,
        d_wd, d_bd, d_tab,
    ) = outs
    y_out[...] = y_all[...].astype(F32)
    g_out[...] = g_all[...].astype(F32)
    d_wq[...] = fin[0, :, :LANES]
    d_wk[...] = fin[1, :, :LANES]
    d_wv[...] = fin[1, :, LANES:]
    d_wo[...] = fin[0, :, LANES:].T
    for s in range(2):
        d_wh[:, s * CW : (s + 1) * CW] = fin[2 + s]
        d_wd[s * CW : (s + 1) * CW, :] = fin[4 + s].T
    for i, ref in enumerate((d_g1, d_s1, d_bq, d_bv, d_bo, d_g2, d_s2, d_bd)):
        ref[...] = tot[i : i + 1, :]
    d_bh[...] = tot[8:12, :]
    heads = d_tab.shape[1]
    table = [
        jnp.concatenate([tot[12 + 2 * h : 13 + 2 * h], tot[13 + 2 * h : 14 + 2 * h]], axis=1)
        for h in range(heads)
    ]
    table = jnp.concatenate(table + [jnp.zeros((8 - heads, TPAD), F32)], axis=0).T
    d_tab[...] = table[:TABLE, :heads]


def spell_call(outs, *args):
    return pl.pallas_call(
        spell,
        name="spell",
        out_shape=outs,
        in_specs=[VM] * 4,
        out_specs=(VM,) * len(outs),
        compiler_params=pltpu.CompilerParams(vmem_limit_bytes=24 * 2**20),
    )(*args)


def per_device(
    nt, na, tokens, gain_one, shift_one, w_query, w_key, w_value, b_query, b_value, w_out, b_out,
    gain_two, shift_two, w_hidden, b_hidden, w_down, b_down, bias_table, rel_index, region,
    win_count, cotangent,
):
    slots = region.shape[0] // nt
    cut = (nt, slots * WT, LANES)
    vectors = [gain_one, shift_one, b_query, b_value, b_out, gain_two, shift_two, b_down]
    parts = block_call(
        nt, na // 2, slots,
        win_count, tokens.reshape(cut), cotangent.reshape(cut),
        w_query, w_key, w_value, w_out, w_hidden, w_down,
        *[v.reshape(1, LANES) for v in vectors],
        b_hidden.reshape(-1, LANES), bias_table, rel_index, region,
    )

    def out(like, shape=None):
        return jax.ShapeDtypeStruct(shape or like.shape, F32)

    one = (1, LANES)
    shapes = (
        out(tokens, cut), out(tokens, cut), out(gain_one, one), out(gain_one, one), out(w_query),
        out(w_key), out(w_value), out(b_query, one), out(b_value, one), out(w_out),
        out(b_out, one), out(gain_two, one), out(shift_two, one), out(w_hidden),
        out(b_hidden, (b_hidden.shape[0] // LANES, LANES)), out(w_down), out(b_down, one),
        out(bias_table),
    )
    likes = (
        tokens, tokens, gain_one, gain_one, w_query, w_key, w_value, b_query, b_value, w_out,
        b_out, gain_two, shift_two, w_hidden, b_hidden, w_down, b_down, bias_table,
    )
    values = spell_call(shapes, *parts)
    return tuple(v.reshape(like.shape) for v, like in zip(values, likes))


def solution(mesh):
    return jax.shard_map(
        functools.partial(per_device, mesh.shape["ta"], mesh.shape["wa"]),
        mesh=mesh,
        in_specs=(
            P("wa", "ta"),
            P("ta"),
            P("ta"),
            P("wa", "ta"),
            P("wa", "ta"),
            P("wa", "ta"),
            P("ta"),
            P("ta"),
            P("ta", "wa"),
            P("ta"),
            P("ta"),
            P("ta"),
            P("wa", "ta"),
            P("ta"),
            P("ta", "wa"),
            P("ta"),
            P(None, "ta"),
            P(),
            P("wa", None),
            P("wa"),
            P("wa", "ta"),
        ),
        out_specs=(
            P("wa", "ta"),
            P("wa", "ta"),
            P("ta"),
            P("ta"),
            P("wa", "ta"),
            P("wa", "ta"),
            P("wa", "ta"),
            P("ta"),
            P("ta"),
            P("ta", "wa"),
            P("ta"),
            P("ta"),
            P("ta"),
            P("wa", "ta"),
            P("ta"),
            P("ta", "wa"),
            P("ta"),
            P(None, "ta"),
        ),
        check_vma=False,
    )
```

```python
import functools

import jax
import jax.numpy as jnp
from jax import lax
from jax.experimental import pallas as pl
from jax.experimental.pallas import tpu as pltpu
from jax.sharding import PartitionSpec as P

C = 512
HDIM = 32
WT = 49
PAD = 64
TABLE = 169
TPAD = 256
NCH = 6
CW = 256
LANES = 128
SROWS = 24
SCALE = HDIM ** (-0.5)
EPS = 1e-05
F32 = jnp.float32
BF16 = jnp.bfloat16
MESH = pl.DeviceIdType.MESH
ANY = pl.BlockSpec(memory_space=pl.ANY)
VM = pl.BlockSpec(memory_space=pltpu.VMEM)
SM = pl.BlockSpec(memory_space=pltpu.SMEM)
DMA = pltpu.SemaphoreType.DMA


def flip(bit, by):
    return bit + by - 2 * bit * by


def add(left, right):
    return (left.astype(F32) + right.astype(F32)).astype(BF16)


def nn(left, right):
    return jnp.dot(left, right, preferred_element_type=F32)


def nt_dot(left, right):
    return lax.dot_general(left, right, (((1,), (1,)), ((), ())), preferred_element_type=F32)


def tn_dot(left, right):
    return lax.dot_general(left, right, (((0,), (0,)), ((), ())), preferred_element_type=F32)


def norm(value):
    mean = jnp.mean(value, axis=1, keepdims=True)
    spread = jnp.mean(value * value, axis=1, keepdims=True) - mean * mean
    rstd = lax.rsqrt(spread + EPS)
    return (value - mean) * rstd, rstd


def norm_back(scaled, normed, rstd):
    first = jnp.mean(scaled, axis=1, keepdims=True)
    second = jnp.mean(scaled * normed, axis=1, keepdims=True)
    return rstd * (scaled - first - normed * second)


def gelu_pair(u):
    cdf = 0.5 + 0.5 * lax.erf(u * (0.5**0.5))
    pdf = jnp.exp(-0.5 * u * u) * ((2.0 * jnp.pi) ** -0.5)
    return u * cdf, cdf + u * pdf


def rowsum(value):
    return jnp.sum(value, axis=0, keepdims=True)


def block(nt, nz, slots, *refs):
    (
        live, tok, cot, wq, wk, wv, wo, wh, wd, g1, s1, bq, bv, bo, g2, s2, bd, bh, tab, rel, reg,
        y_all, g_all, fin, tot,
        xg, cg, gw, vg, rg, dv, rc, ry, rx, r3, rz, scr, syr, sx, zb, small, yb, gb, square, mask, inv,
        xs, xp, gy, h1, h1t, h2t, gyt, qs, kvs, probs, att, acc, acc2, n1, r1, n2, r2, low, gkv, gq,
        pairs,
        loc, tok_s, tok_r, out_s, out_r, az_s, az_r, ax_s, ax_r, ay_s, ay_r, ac_s, ac_r,
        bx_s, bx_r, by_s, by_r, cz_s, cz_r, k_s, k_r, p_s, p_r, q_s, q_r, rz_s, rz_r, sm_s, sm_r,
    ) = refs
    heads = LANES // HDIM
    rows = slots * PAD
    half = 2 * PAD
    nhalf = rows // half
    a, t = lax.axis_index("wa"), lax.axis_index("ta")
    x, z, c, y = lax.rem(a, 2), lax.div(a, 2), lax.rem(t, 2), lax.div(t, 2)

    def group(m):
        return 2 * flip(y, m // 2 if isinstance(m, int) else lax.div(m, 2)) + flip(
            c, m % 2 if isinstance(m, int) else lax.rem(m, 2)
        )

    t1, t2, t3 = group(1), group(2), group(3)
    xpeer, ypeer, cpeer = (z * 2 + (1 - x), t), (a, t2), (a, t1)
    zs = [(lax.rem(z + d, nz) * 2 + x, t) for d in range(1, nz)]
    ts = [(a, tt) for tt in (t1, t2, t3)]
    peers = zs + ts + [xpeer]
    barrier = pltpu.get_barrier_semaphore()
    for peer in peers:
        pl.semaphore_signal(barrier, inc=1, device_id=peer, device_id_type=MESH)

    def far(src, dst, send, recv, peer):
        return pltpu.make_async_remote_copy(
            src_ref=src, dst_ref=dst, send_sem=send, recv_sem=recv, device_id=peer,
            device_id_type=MESH,
        )

    def tok_copy(i, d):
        src, dst = ((tok, xg), (cot, cg), (vg, vg), (rg, rg))[i]
        peer = ts[d]
        src = src.at[peer[1]] if i < 2 else src.at[t]
        return far(src, dst.at[t], tok_s.at[i, d], tok_r.at[i, d], peer)

    def out_copy(i, d):
        src, dst = ((yb, y_all), (gb, g_all))[i]
        peer = ts[d]
        return far(src.at[peer[1]], dst.at[t], out_s.at[i, d], out_r.at[i, d], peer)

    def far_z(d):
        return lax.rem(z + nz - d, nz)

    def az(ch, d):
        ref = gw.at[ch, t, z, x]
        return far(ref, ref, az_s.at[ch, d], az_r.at[ch, d], zs[d])

    def ax(ch, d):
        ref = gw.at[ch, t, far_z(d), x]
        return far(ref, ref, ax_s.at[ch, d], ax_r.at[ch, d], xpeer)

    def ay(ch, d):
        ref = gw.at[ch, t, far_z(d)] if ch == 0 else gw.at[ch, t, far_z(d), x]
        return far(ref, ref, ay_s.at[ch, d], ay_r.at[ch, d], ypeer)

    def bx(ch, j):
        ref = gw.at[ch, t2 if j else t, :, x]
        return far(ref, ref, bx_s.at[ch, j], bx_r.at[ch, j], xpeer)

    def by(ch):
        ref = gw.at[ch, t, :, x]
        return far(ref, ref, by_s.at[ch], by_r.at[ch], ypeer)

    def cy():
        ref = gw.at[5, t, z, x]
        return far(ref, ref, by_s.at[5], by_r.at[5], ypeer)

    def cx(j):
        ref = gw.at[5, t2 if j else t, z, x]
        return far(ref, ref, bx_s.at[5, j], bx_r.at[5, j], xpeer)

    def cz(d, j):
        ref = gw.at[5, t2 if j else t, z]
        return far(ref, ref, cz_s.at[d, j], cz_r.at[d, j], zs[d])

    def ac(ch, j):
        ref = gw.at[ch, t2 if j else t]
        return far(ref, ref, ac_s.at[ch, j], ac_r.at[ch, j], cpeer)

    def kc(ch, j):
        return far(dv.at[ch, t1 if j else t3], rc.at[ch, j], k_s.at[ch, j], k_r.at[ch, j], cpeer)

    def ya(ch):
        return far(dv.at[ch, t2], ry.at[ch - 2], p_s.at[ch, 0], p_r.at[ch, 0], ypeer)

    def xa(ch):
        return far(dv.at[ch, t, :, 1 - x], r3.at[ch], q_s.at[ch], q_r.at[ch], xpeer)

    def slot_b(ch):
        return ch if isinstance(ch, int) and ch < 2 else ch - 2

    def xb(ch, j):
        src = dv.at[ch, t if j else t2, :, 1 - x]
        return far(src, rx.at[slot_b(ch), j], p_s.at[ch, j], p_r.at[ch, j], xpeer)

    def yb2(ch):
        return far(dv.at[ch, t2, :, x], r3.at[ch], q_s.at[ch], q_r.at[ch], ypeer)

    def zr(ch, d):
        src = dv.at[ch, t, lax.rem(z + d + 1, nz), x]
        return far(src, rz.at[ch, d], rz_s.at[ch, d], rz_r.at[ch, d], zs[d])

    def core_first(ch):
        kc(ch, 0).wait_recv()
        dv[ch, t2] = add(dv[ch, t2], rc[ch, 0])

    def core_second(ch):
        kc(ch, 1).wait_recv()
        dv[ch, t] = add(dv[ch, t], rc[ch, 1])

    def second_a(ch):
        ya(ch).wait_recv()
        dv[ch, t] = add(dv[ch, t], ry[ch - 2])
        xa(ch).start()

    def first_half(ch):
        xb(ch, 0).wait_recv()
        dv[ch, t2, :, x] = add(dv[ch, t2, :, x], rx[slot_b(ch), 0])
        yb2(ch).start()

    def second_half(ch):
        xb(ch, 1).wait_recv()
        dv[ch, t, :, x] = add(dv[ch, t, :, x], rx[slot_b(ch), 1])

    def second_b(ch):
        first_half(ch)
        second_half(ch)

    def third(ch):
        (xa(ch) if ch in (2, 3) else yb2(ch)).wait_recv()
        dv[ch, t, :, x] = add(dv[ch, t, :, x], r3[ch])
        for d in range(nz - 1):
            zr(ch, d).start()

    def fourth(ch):
        value = dv[ch, t, z, x].astype(F32)
        for d in range(nz - 1):
            zr(ch, d).wait_recv()
            value = value + rz[ch, d].astype(F32)
        fin[ch] = value

    def small_core(j):
        return far(small.at[t1 if j else t3], scr.at[j], sm_s.at[j], sm_r.at[j], cpeer)

    def small_y():
        return far(sx.at[0], syr.at[0], sm_s.at[2], sm_r.at[2], ypeer)

    def small_z(d):
        return far(zb.at[z], zb.at[z], sm_s.at[3 + d], sm_r.at[3 + d], zs[d])

    def small_x():
        return far(sx.at[2], syr.at[1], sm_s.at[2 + nz], sm_r.at[2 + nz], xpeer)

    gw[0, t, z, x, :, :LANES] = wq[...]
    gw[0, t, z, x, :, LANES:] = wo[...]
    gw[1, t, z, x, :, :LANES] = wk[...]
    gw[1, t, z, x, :, LANES:] = wv[...]
    for i, ref in enumerate((g1, s1, bq, bv, bo, g2, s2, bd)):
        vg[t, i : i + 1, :] = ref[...]
    vg[t, 8:12, :] = bh[...]
    vg[t, 12:, :] = jnp.zeros((SROWS - 12, LANES), F32)
    for s in range(2):
        gw[2 + s, t, z, x] = wh[:, s * CW : (s + 1) * CW]
        gw[4 + s, t, z, x] = wd[:, s * CW : (s + 1) * CW]
    pl.semaphore_wait(barrier, len(peers))
    own_tok = pltpu.make_async_copy(tok.at[t], xg.at[t], loc.at[0])
    own_cot = pltpu.make_async_copy(cot.at[t], cg.at[t], loc.at[1])
    own_tok.start()
    own_cot.start()
    for d in range(nz - 1):
        az(0, d).start()
    for d in range(3):
        tok_copy(0, d).start()
    ax(0, 0).start()
    for d in range(nz - 1):
        az(1, d).start()
    for d in range(3):
        tok_copy(2, d).start()
    ax(1, 0).start()
    cy().start()
    ay(1, 0).start()
    for ch in (2, 4, 3):
        for d in range(nz - 1):
            az(ch, d).start()
    square[...] = jnp.zeros_like(square)
    table = tab[...]
    square[:WT, :WT] = rel[...].astype(F32)
    rel_t = square[...].T[:PAD, :PAD]
    pick_at = jnp.concatenate([rel_t, rel_t], axis=1).astype(jnp.int32)
    lane = lax.broadcasted_iota(jnp.int32, (PAD, LANES), 1)
    low_at, high_at = jnp.minimum(pick_at, LANES - 1), jnp.maximum(pick_at - LANES, 0)

    def take(value, at):
        return jnp.take_along_axis(value, at, axis=1, mode="promise_in_bounds")

    def entry(h):
        first = jnp.broadcast_to(table[h : h + 1, :LANES], (PAD, LANES))
        second = jnp.concatenate(
            [table[h : h + 1, LANES:], jnp.zeros((1, TPAD - TABLE), F32)], axis=1
        )
        second = jnp.broadcast_to(second, (PAD, LANES))
        return jnp.where(pick_at < LANES, take(first, low_at), take(second, high_at))

    for q in range(heads // 2):
        rg[t, :, q * LANES : (q + 1) * LANES] = jnp.where(
            lane < PAD, entry(2 * q), entry(2 * q + 1)
        )
    for d in range(3):
        tok_copy(3, d).start()
    number = lax.broadcasted_iota(jnp.int32, (PAD, TPAD), 1).astype(F32)
    found = jnp.full((PAD, TPAD), -1.0, F32)
    for i in range(WT):
        found = jnp.where(rel_t[:, i : i + 1] == number, float(i), found)
    inv[...] = found.astype(jnp.int32)
    square[...] = jnp.zeros_like(square)
    mine = reg[pl.ds(pl.multiple_of(t * slots, slots), slots), :]
    square[:slots, :WT] = mine.astype(F32)
    reg_row = square[:slots, :PAD]
    reg_row = jnp.concatenate([reg_row] * heads, axis=1)
    reg_col = square[...].T[:PAD, :slots]
    real = lax.broadcasted_iota(jnp.int32, (PAD, heads * PAD), 0) < WT
    for w in range(slots):
        same = reg_col[:, w : w + 1] == reg_row[w : w + 1, :]
        mask[w] = jnp.where(real, jnp.where(same, 0.0, -100.0), -1e30)
    for d in range(nz - 1):
        az(0, d).wait_recv()
        ax(0, d + 1).start()
    cy().wait_recv()
    for j in range(2):
        cx(j).start()

    def wide(i):
        return jnp.concatenate([vg[tt, i : i + 1, :] for tt in range(nt)], axis=1)

    def put_small(i, value):
        for tt in range(nt):
            small[tt, i : i + 1, :] = value[:, tt * LANES : (tt + 1) * LANES]

    def spread(source, target):
        for tt in range(nt):
            xs[:, tt * LANES : (tt + 1) * LANES] = source[tt].astype(F32)
        zero = jnp.zeros((PAD - WT, C), F32)
        for w in range(slots):
            target[w * PAD : w * PAD + WT, :] = xs[w * WT : (w + 1) * WT, :]
            target[w * PAD + WT : (w + 1) * PAD, :] = zero

    def gather(source, target):
        for w in range(slots):
            xs[w * WT : (w + 1) * WT, :] = source[w * PAD : w * PAD + WT, :]
        for tt in range(nt):
            target[tt] = xs[:, tt * LANES : (tt + 1) * LANES].astype(BF16)

    def each(body, init=0):
        def step(i, carry):
            return body(i, pl.ds(pl.multiple_of(i * half, half), half), carry)

        return lax.fori_loop(0, nhalf, step, init)

    def weight(ch, tt, start=0, size=CW):
        return gw[ch, tt, :, :, :, start : start + size].reshape(C, size)

    def put_grad(ch, tt, value):
        dv[ch, tt] = value.astype(BF16).reshape(dv.shape[2:])

    n_live = live[0] - t * slots
    small[...] = jnp.zeros_like(small)
    own_tok.wait()
    for i in (0, 2):
        for d in range(3):
            tok_copy(i, d).wait_recv()
    spread(xg, xp)
    gain1, shift1 = wide(0), wide(1)

    def start(i, at, carry):
        normed, rstd = norm(xp[at, :])
        n1[at, :] = normed
        r1[at, :] = rstd
        h = normed * gain1 + shift1
        h1[at, :] = h.astype(BF16)
        h1t[:, at] = h.T.astype(BF16)
        return carry

    each(start)
    for d in range(nz - 1):
        az(1, d).wait_recv()
        ax(1, d + 1).start()
        ay(1, d + 1).start()
    for d in range(nz):
        ax(0, d).wait_recv()
        ay(0, d).start()
    ac(0, 0).start()
    for d in range(3):
        tok_copy(3, d).wait_recv()
    for d in range(nz):
        ax(1, d).wait_recv()
    ac(1, 0).start()
    lane_head = lax.broadcasted_iota(jnp.int32, (PAD, LANES), 1) // HDIM
    ones = [(lane_head == h).astype(F32).astype(BF16) for h in range(heads)]

    def stack(value):
        return jnp.concatenate([value * ones[h] for h in range(heads)], axis=0)

    def pick(value):
        out = value[0:PAD]
        for h in range(1, heads):
            out = jnp.where(lane_head == h, value[h * PAD : (h + 1) * PAD], out)
        return out

    acc[...] = jnp.zeros_like(acc)

    def events(i, table):
        for when, todo in table.items():

            @pl.when(i == when)
            def _(todo=todo):
                for act in todo:
                    act()

    def z_to_xy(ch):
        for d in range(nz - 1):
            az(ch, d).wait_recv()
        bx(ch, 0).start()
        by(ch).start()

    def y_to_x(ch):
        by(ch).wait_recv()
        bx(ch, 1).start()

    def x_to_core(ch, j):
        bx(ch, j).wait_recv()
        ac(ch, j).start()

    def ay_to_bx():
        for d in range(nz):
            ay(1, d).wait_recv()
        bx(1, 1).start()

    def start_cz():
        for j in range(2):
            cx(j).wait_recv()
        for d in range(nz - 1):
            for j in range(2):
                cz(d, j).start()

    def groups_in():
        for d in range(nz):
            ay(0, d).wait_recv()
        ac(0, 1).start()
        x_to_core(1, 1)

    def start_cot():
        for d in range(3):
            tok_copy(1, d).start()

    def end_cz():
        for d in range(nz - 1):
            for j in range(2):
                cz(d, j).wait_recv()
        for j in range(2):
            ac(5, j).start()

    in_first = {
        0: [ay_to_bx, lambda: z_to_xy(2)],
        2: [lambda: y_to_x(2), lambda: z_to_xy(3)],
        3: [lambda: x_to_core(4, 0), lambda: x_to_core(2, 1)],
    }
    in_second = {
        0: [lambda: z_to_xy(4), start_cz],
        1: [groups_in, start_cot],
        2: [lambda: y_to_x(4), lambda: x_to_core(2, 0)],
        3: [lambda: x_to_core(4, 1)],
    }

    def attend(i, carry):
        tt = group(i)

        @pl.when(i == 1)
        def _():
            for ch in range(2):
                ac(ch, 0).wait_recv()

        @pl.when(i == 3)
        def _():
            for ch in range(2):
                ac(ch, 1).wait_recv()

        q = (nn(h1[...], weight(0, tt, 0, LANES)) + vg[tt, 2:3, :]) * SCALE
        qs[tt] = q.astype(BF16)
        kv = nn(h1[...], weight(1, tt))
        kvs[tt, :, :LANES] = kv[:, :LANES].astype(BF16)
        kvs[tt, :, LANES:] = (kv[:, LANES:] + vg[tt, 3:4, :]).astype(BF16)

        def window(w, carry):
            at = pl.ds(pl.multiple_of(w * PAD, PAD), PAD)
            s = nt_dot(kvs[tt, at, :LANES], stack(qs[tt, at, :])) + rg[tt] + mask[w]
            e = jnp.exp(s - jnp.max(s, axis=0, keepdims=True))
            p = e / rowsum(e)
            probs[tt, w] = p
            att[tt, at, :] = pick(tn_dot(p.astype(BF16), kvs[tt, at, LANES:])).astype(BF16)
            return carry

        lax.fori_loop(0, slots // 2, window, 0, unroll=2)
        events(i, in_first)
        lax.fori_loop(slots // 2, slots, window, 0, unroll=2)
        acc[...] += nt_dot(att[tt], weight(0, tt, LANES, LANES))
        events(i, in_second)
        return carry

    lax.fori_loop(0, nt, attend, 0)
    own_cot.wait()
    for d in range(3):
        tok_copy(1, d).wait_recv()
    spread(cg, gy)
    b_out, gain2, shift2 = wide(4), wide(5), wide(6)

    def live_rows(i):
        slot = lax.div(i * half + lax.broadcasted_iota(jnp.int32, (half, 1), 0), PAD)
        return slot < n_live

    def middle(i, at, carry):
        x1 = xp[at, :] + acc[at, :] + b_out
        xp[at, :] = x1
        normed, rstd = norm(x1)
        n2[at, :] = normed
        r2[at, :] = rstd
        h = normed * gain2 + shift2
        low[at, :] = h.astype(BF16)
        h2t[:, at] = h.T.astype(BF16)
        g = jnp.where(live_rows(i), gy[at, :], 0.0)
        gy[at, :] = g
        gkv[at, :] = g.astype(BF16)
        gyt[:, at] = g.T.astype(BF16)
        return carry

    each(middle)
    acc[...] = jnp.zeros_like(acc)
    acc2[...] = jnp.zeros_like(acc2)
    for ch in (2, 4):
        for j in range(2):
            ac(ch, j).wait_recv()

    mlp_events = {
        0: [lambda: y_to_x(3), lambda: x_to_core(3, 0)],
        2: [lambda: x_to_core(3, 1), end_cz],
    }

    def mlp(k, carry):
        s, i = lax.div(k, nt), lax.rem(k, nt)
        tt = group(3 - i)
        up, down = 2 + s, 4 + s

        @pl.when(k == 4)
        def _():
            for ch in (3, 5):
                for j in range(2):
                    ac(ch, j).wait_recv()

        bias = vg[tt, pl.ds(8 + 2 * s, 2), :]
        bias = jnp.concatenate([bias[0:1], bias[1:2]], axis=1)
        hidden = nn(low[...], weight(up, tt)) + bias
        act, slope = gelu_pair(hidden)
        act_low = act.astype(BF16)
        acc[...] += nt_dot(act_low, weight(down, tt))
        put_grad(down, tt, nn(gyt[...], act_low))
        grad = nn(gkv[...], weight(down, tt)) * slope
        total = rowsum(grad)
        small[tt, pl.ds(8 + 2 * s, 1), :] = total[:, :LANES]
        small[tt, pl.ds(9 + 2 * s, 1), :] = total[:, LANES:]
        grad_low = grad.astype(BF16)
        put_grad(up, tt, nn(h2t[...], grad_low))
        acc2[...] += nt_dot(grad_low, weight(up, tt))

        events(k, mlp_events)

        @pl.when(i == 0)
        def _():
            kc(down, 0).start()
            kc(up, 0).start()

        @pl.when(i == 1)
        def _():
            core_first(up)
            ya(up).start()
            core_first(down)

        @pl.when(i == 2)
        def _():
            kc(down, 1).start()
            kc(up, 1).start()

        @pl.when(i == 3)
        def _():
            core_second(down)
            for j in range(2):
                xb(down, j).start()
            core_second(up)

        return carry

    lax.fori_loop(0, 2 * nt, mlp, 0)
    second_a(2)
    b_down = wide(7)
    zero_row = jnp.zeros((1, C), F32)

    def turn(i, at, carry):
        xp[at, :] = jnp.where(live_rows(i), xp[at, :] + acc[at, :] + b_down, 0.0)
        e, normed, g = acc2[at, :], n2[at, :], gy[at, :]
        gx = norm_back(e * gain2, normed, r2[at, :]) + g
        gy[at, :] = gx
        low[at, :] = gx.astype(BF16)
        h2t[:, at] = gx.T.astype(BF16)
        sums = (rowsum(e * normed), rowsum(e), rowsum(gx), rowsum(g))
        return tuple(p + q for p, q in zip(carry, sums))

    sums = each(turn, (zero_row,) * 4)
    put_small(5, sums[0])
    put_small(6, sums[1])
    put_small(4, sums[2])
    put_small(7, sums[3])
    gather(xp, yb)
    own_y = pltpu.make_async_copy(yb.at[t], y_all.at[t], loc.at[2])
    own_y.start()
    second_b(4)
    acc[...] = jnp.zeros_like(acc)

    def start_y():
        for d in range(3):
            out_copy(0, d).start()

    def core_zero():
        for ch in range(2):
            core_first(ch)
            xb(ch, 0).start()

    def core_one():
        for ch in range(2):
            core_second(ch)
            xb(ch, 1).start()

    out_first = {
        1: [lambda: third(4)],
        2: [lambda: third(3)],
        3: [lambda: first_half(0), lambda: first_half(1)],
    }
    out_second = {
        0: [lambda: second_a(3)],
        1: [lambda: third(2), core_zero, lambda: second_b(5), start_y],
        2: [lambda: third(5), lambda: fourth(2), lambda: fourth(4)],
        3: [core_one],
    }

    def back(i, carry):
        tt = group(3 - i)
        gatt = gq
        gatt[...] = nn(low[...], weight(0, tt, LANES, LANES)).astype(BF16)
        pairs[...] = jnp.zeros_like(pairs)

        def window(w, carry):
            at = pl.ds(pl.multiple_of(w * PAD, PAD), PAD)
            q4, g4 = stack(qs[tt, at, :]), stack(gatt[at, :])
            p = probs[tt, w]
            dp = nt_dot(kvs[tt, at, LANES:], g4)
            ds = p * (dp - rowsum(p * dp))
            ds_low = ds.astype(BF16)
            pairs[...] += ds_low.astype(F32)
            gkv[at, :LANES] = nn(ds_low, q4).astype(BF16)
            gkv[at, LANES:CW] = nn(p.astype(BF16), g4).astype(BF16)
            gatt[at, :] = pick(tn_dot(ds_low, kvs[tt, at, :LANES])).astype(BF16)
            return carry

        lax.fori_loop(0, slots // 2, window, 0, unroll=2)
        events(i, out_first)
        lax.fori_loop(slots // 2, slots, window, 0, unroll=2)
        gk_gv = gkv[:, :CW]
        put_grad(1, tt, nn(h1t[...], gk_gv))
        left = nn(h1t[...], gatt[...]) * SCALE
        put_grad(0, tt, jnp.concatenate([left, nn(h2t[...], att[tt])], axis=1))

        @pl.when(i == 0)
        def _():
            kc(1, 0).start()
            kc(0, 0).start()

        @pl.when(i == 2)
        def _():
            kc(1, 1).start()
            kc(0, 1).start()

        small[tt, 2:3, :] = rowsum(gatt[...].astype(F32)) * SCALE
        small[tt, 3:4, :] = rowsum(gkv[:, LANES:CW].astype(F32))
        grad_q = nt_dot(gatt[...], weight(0, tt, 0, LANES)) * SCALE
        acc[...] += grad_q + nt_dot(gk_gv, weight(1, tt))
        for h in range(heads):
            lanes = h // 2 * LANES
            source = pairs[:, lanes : lanes + LANES]
            for q in range(TPAD // LANES):
                where = inv[:, q * LANES : (q + 1) * LANES]
                value = take(source, jnp.maximum(where, 0) + h % 2 * PAD)
                value = jnp.where(where >= 0, value, 0.0)
                small[tt, pl.ds(12 + 2 * h + q, 1), :] = rowsum(value)

        events(i, out_second)
        return carry

    lax.fori_loop(0, nt, back, 0)

    def finish(i, at, carry):
        e, normed = acc[at, :], n1[at, :]
        xp[at, :] = norm_back(e * gain1, normed, r1[at, :]) + gy[at, :]
        sums = (rowsum(e * normed), rowsum(e))
        return tuple(p + q for p, q in zip(carry, sums))

    sums = each(finish, (zero_row,) * 2)
    put_small(0, sums[0])
    put_small(1, sums[1])
    for j in range(2):
        small_core(j).start()
    gather(xp, gb)
    own_g = pltpu.make_async_copy(gb.at[t], g_all.at[t], loc.at[3])
    own_g.start()
    for j in range(2):
        small_core(j).wait_recv()
    sx[0] = small[t2] + scr[0]
    sx[1] = small[t] + scr[1]
    small_y().start()
    for d in range(3):
        out_copy(1, d).start()
    fourth(3)
    fourth(5)
    small_y().wait_recv()
    zb[z] = sx[1] + syr[0]
    for d in range(nz - 1):
        small_z(d).start()
    second_half(0)
    third(0)
    for d in range(nz - 1):
        small_z(d).wait_recv()
    value = zb[0]
    for zz in range(1, nz):
        value = value + zb[zz]
    sx[2] = value
    small_x().start()
    second_half(1)
    third(1)
    small_x().wait_recv()
    tot[...] = sx[2] + syr[1]
    fourth(0)
    fourth(1)
    for i in range(2):
        for d in range(3):
            out_copy(i, d).wait_recv()
    sent = [tok_copy(i, d) for i in range(4) for d in range(3)]
    sent += [out_copy(i, d) for i in range(2) for d in range(3)]
    for ch in range(NCH):
        sent += [zr(ch, d) for d in range(nz - 1)]
        sent += [ac(ch, j) for j in range(2)] + [kc(ch, j) for j in range(2)]
        sent += [az(ch, d) for d in range(nz - 1)] if ch < 5 else [cy(), cx(0), cx(1)]
        if ch < 2:
            sent += [ax(ch, d) for d in range(nz)] + [ay(ch, d) for d in range(nz)]
            sent += [bx(1, 1)] if ch == 1 else []
        elif ch < 5:
            sent += [by(ch), bx(ch, 0), bx(ch, 1)]
        sent += [ya(ch), xa(ch)] if ch in (2, 3) else [xb(ch, 0), xb(ch, 1), yb2(ch)]
    sent += [cz(d, j) for d in range(nz - 1) for j in range(2)]
    sent += [small_core(0), small_core(1), small_y(), small_x()]
    sent += [small_z(d) for d in range(nz - 1)]
    for copy in sent:
        copy.wait_send()
    own_y.wait()
    own_g.wait()


def block_call(nt, nz, slots, *args):
    tok, deep, heads = args[1], args[3].shape[0], args[18].shape[0]
    real = tok.shape[1]
    rows, wide = slots * PAD, heads * PAD
    piece = (nz, 2, deep, CW)
    row = (nt, real, LANES)

    def vm(shape, kind=BF16):
        return pltpu.VMEM(shape, kind)

    def pair(*shape):
        return [DMA(shape), DMA(shape)]

    small = (SROWS, LANES)
    return pl.pallas_call(
        functools.partial(block, nt, nz, slots),
        name="block",
        out_shape=(
            jax.ShapeDtypeStruct(row, BF16),
            jax.ShapeDtypeStruct(row, BF16),
            jax.ShapeDtypeStruct((NCH, deep, CW), F32),
            jax.ShapeDtypeStruct(small, F32),
        ),
        in_specs=[SM, ANY, ANY] + [VM] * 18,
        out_specs=(ANY, ANY, VM, VM),
        scratch_shapes=[
            vm(row),
            vm(row),
            vm((NCH, nt) + piece),
            vm((nt,) + small, F32),
            vm((nt, PAD, wide), F32),
            vm((NCH, nt) + piece),
            vm((NCH, 2) + piece),
            vm((2,) + piece),
            vm((4, 2, nz, deep, CW)),
            vm((NCH, nz, deep, CW)),
            vm((NCH, nz - 1, deep, CW)),
            vm((2,) + small, F32),
            vm((2,) + small, F32),
            vm((3,) + small, F32),
            vm((nz,) + small, F32),
            vm((nt,) + small, F32),
            vm(row),
            vm(row),
            vm((LANES, LANES), F32),
            vm((slots, PAD, wide), F32),
            vm((PAD, TPAD), jnp.int32),
            vm((real, C), F32),
            vm((rows, C), F32),
            vm((rows, C), F32),
            vm((rows, C)),
            vm((C, rows)),
            vm((C, rows)),
            vm((C, rows)),
            vm((nt, rows, LANES)),
            vm((nt, rows, CW)),
            vm((nt, slots, PAD, wide), F32),
            vm((nt, rows, LANES)),
            vm((rows, C), F32),
            vm((rows, C), F32),
            vm((rows, C), F32),
            vm((rows, 1), F32),
            vm((rows, C), F32),
            vm((rows, 1), F32),
            vm((rows, C)),
            vm((rows, C)),
            vm((rows, LANES)),
            vm((PAD, wide), F32),
            DMA((4,)),
        ]
        + pair(4, 3)
        + pair(2, 3)
        + pair(NCH, nz - 1)
        + pair(2, nz)
        + pair(2, nz)
        + pair(NCH, 2)
        + pair(NCH, 2)
        + pair(NCH)
        + pair(nz - 1, 2)
        + pair(NCH, 2)
        + pair(NCH, 2)
        + pair(NCH)
        + pair(NCH, nz - 1)
        + pair(3 + nz),
        compiler_params=pltpu.CompilerParams(
            collective_id=0, has_side_effects=True, vmem_limit_bytes=60 * 2**20
        ),
    )(*args)


def spell(y_all, g_all, fin, tot, *outs):
    (
        y_out, g_out, d_g1, d_s1, d_wq, d_wk, d_wv, d_bq, d_bv, d_wo, d_bo, d_g2, d_s2, d_wh, d_bh,
        d_wd, d_bd, d_tab,
    ) = outs
    y_out[...] = y_all[...].astype(F32)
    g_out[...] = g_all[...].astype(F32)
    d_wq[...] = fin[0, :, :LANES]
    d_wk[...] = fin[1, :, :LANES]
    d_wv[...] = fin[1, :, LANES:]
    d_wo[...] = fin[0, :, LANES:]
    for s in range(2):
        d_wh[:, s * CW : (s + 1) * CW] = fin[2 + s]
        d_wd[:, s * CW : (s + 1) * CW] = fin[4 + s]
    for i, ref in enumerate((d_g1, d_s1, d_bq, d_bv, d_bo, d_g2, d_s2, d_bd)):
        ref[...] = tot[i : i + 1, :]
    d_bh[...] = tot[8:12, :]
    for h in range(d_tab.shape[0]):
        d_tab[h : h + 1, :LANES] = tot[12 + 2 * h : 13 + 2 * h]
        d_tab[h : h + 1, LANES:] = tot[13 + 2 * h : 14 + 2 * h, : TABLE - LANES]


def spell_call(outs, *args):
    return pl.pallas_call(
        spell,
        name="spell",
        out_shape=outs,
        in_specs=[VM] * 4,
        out_specs=(VM,) * len(outs),
        compiler_params=pltpu.CompilerParams(vmem_limit_bytes=60 * 2**20),
    )(*args)


def per_device(
    nt, na, tokens, gain_one, shift_one, w_query, w_key, w_value, b_query, b_value, w_out, b_out,
    gain_two, shift_two, w_hidden, b_hidden, w_down, b_down, bias_table, rel_index, region,
    win_count, cotangent,
):
    slots = region.shape[0] // nt
    cut = (nt, slots * WT, LANES)
    vectors = [gain_one, shift_one, b_query, b_value, b_out, gain_two, shift_two, b_down]
    parts = block_call(
        nt, na // 2, slots,
        win_count, tokens.reshape(cut), cotangent.reshape(cut),
        w_query, w_key, w_value, w_out.T, w_hidden, w_down.T,
        *[v.reshape(1, LANES) for v in vectors],
        b_hidden.reshape(-1, LANES), bias_table.T, rel_index, region,
    )

    def out(like, shape=None):
        return jax.ShapeDtypeStruct(shape or like.shape, F32)

    one = (1, LANES)
    shapes = (
        out(tokens, cut), out(tokens, cut), out(gain_one, one), out(gain_one, one), out(w_query),
        out(w_key), out(w_value), out(b_query, one), out(b_value, one), out(w_out, w_out.shape[::-1]),
        out(b_out, one), out(gain_two, one), out(shift_two, one), out(w_hidden),
        out(b_hidden, (b_hidden.shape[0] // LANES, LANES)), out(w_down, w_down.shape[::-1]),
        out(b_down, one), out(bias_table, bias_table.shape[::-1]),
    )
    likes = (
        tokens, tokens, gain_one, gain_one, w_query, w_key, w_value, b_query, b_value, w_out,
        b_out, gain_two, shift_two, w_hidden, b_hidden, w_down, b_down, bias_table,
    )
    values = spell_call(shapes, *parts)
    turned = (9, 15, 17)
    return tuple(
        v.T if i in turned else v.reshape(like.shape)
        for i, (v, like) in enumerate(zip(values, likes))
    )


def solution(mesh):
    return jax.shard_map(
        functools.partial(per_device, mesh.shape["ta"], mesh.shape["wa"]),
        mesh=mesh,
        in_specs=(
            P("wa", "ta"),
            P("ta"),
            P("ta"),
            P("wa", "ta"),
            P("wa", "ta"),
            P("wa", "ta"),
            P("ta"),
            P("ta"),
            P("ta", "wa"),
            P("ta"),
            P("ta"),
            P("ta"),
            P("wa", "ta"),
            P("ta"),
            P("ta", "wa"),
            P("ta"),
            P(None, "ta"),
            P(),
            P("wa", None),
            P("wa"),
            P("wa", "ta"),
        ),
        out_specs=(
            P("wa", "ta"),
            P("wa", "ta"),
            P("ta"),
            P("ta"),
            P("wa", "ta"),
            P("wa", "ta"),
            P("wa", "ta"),
            P("ta"),
            P("ta"),
            P("ta", "wa"),
            P("ta"),
            P("ta"),
            P("ta"),
            P("wa", "ta"),
            P("ta"),
            P("ta", "wa"),
            P("ta"),
            P(None, "ta"),
        ),
        check_vma=False,
    )
```

```python
import functools

import jax
import jax.numpy as jnp
from jax import lax
from jax.experimental import pallas as pl
from jax.experimental.pallas import tpu as pltpu
from jax.sharding import PartitionSpec as P

C = 512
HDIM = 32
WT = 49
PAD = 64
TABLE = 169
TPAD = 256
NCH = 6
CW = 256
LANES = 128
SROWS = 24
SCALE = HDIM ** (-0.5)
EPS = 1e-05
F32 = jnp.float32
BF16 = jnp.bfloat16
MESH = pl.DeviceIdType.MESH
ANY = pl.BlockSpec(memory_space=pl.ANY)
VM = pl.BlockSpec(memory_space=pltpu.VMEM)
SM = pl.BlockSpec(memory_space=pltpu.SMEM)
DMA = pltpu.SemaphoreType.DMA


def flip(bit, by):
    return bit + by - 2 * bit * by


def add(left, right):
    return (left.astype(F32) + right.astype(F32)).astype(BF16)


def nn(left, right):
    return jnp.dot(left, right, preferred_element_type=F32)


def nt_dot(left, right):
    return lax.dot_general(left, right, (((1,), (1,)), ((), ())), preferred_element_type=F32)


def tn_dot(left, right):
    return lax.dot_general(left, right, (((0,), (0,)), ((), ())), preferred_element_type=F32)


def norm(value):
    mean = jnp.mean(value, axis=1, keepdims=True)
    spread = jnp.mean(value * value, axis=1, keepdims=True) - mean * mean
    rstd = lax.rsqrt(spread + EPS)
    return (value - mean) * rstd, rstd


def norm_back(scaled, normed, rstd):
    first = jnp.mean(scaled, axis=1, keepdims=True)
    second = jnp.mean(scaled * normed, axis=1, keepdims=True)
    return rstd * (scaled - first - normed * second)


def gelu_pair(u):
    cdf = 0.5 + 0.5 * lax.erf(u * (0.5**0.5))
    pdf = jnp.exp(-0.5 * u * u) * ((2.0 * jnp.pi) ** -0.5)
    return u * cdf, cdf + u * pdf


def rowsum(value):
    return jnp.sum(value, axis=0, keepdims=True)


def block(nt, nz, slots, *refs):
    (
        live, tok, cot, wq, wk, wv, wo, wh, wd, g1, s1, bq, bv, bo, g2, s2, bd, bh, tab, rel, reg,
        y_all, g_all, fin, tot,
        xg, cg, gw, vg, rg, dv, rc, ry, rx, r3, rz, rzc, rxc, scr, syr, sx, zb, small, yb, gb, square, mask, inv,
        xs, xp, gy, h1, h1t, h2t, gyt, qs, kvs, probs, att, acc, acc2, n1, r1, n2, r2, low, gkv, gq,
        pairs,
        loc, tok_s, tok_r, out_s, out_r, ln_s, ln_r, az_s, az_r, ax_s, ax_r, ay_s, ay_r, ac_s, ac_r,
        bx_s, bx_r, by_s, by_r, cz_s, cz_r, px_s, px_r, zc_s, zc_r, xc_s,
        xc_r, k_s, k_r, p_s, p_r, q_s, q_r, rz_s, rz_r, sm_s, sm_r,
    ) = refs
    heads = LANES // HDIM
    rows = slots * PAD
    half = 2 * PAD
    nhalf = rows // half
    a, t = lax.axis_index("wa"), lax.axis_index("ta")
    x, z, c, y = lax.rem(a, 2), lax.div(a, 2), lax.rem(t, 2), lax.div(t, 2)

    def group(m):
        return 2 * flip(y, m // 2 if isinstance(m, int) else lax.div(m, 2)) + flip(
            c, m % 2 if isinstance(m, int) else lax.rem(m, 2)
        )

    t1, t2, t3 = group(1), group(2), group(3)
    xpeer, ypeer, cpeer = (z * 2 + (1 - x), t), (a, t2), (a, t1)
    zs = [(lax.rem(z + d, nz) * 2 + x, t) for d in range(1, nz)]
    ts = [(a, tt) for tt in (t1, t2, t3)]
    peers = zs + ts + [xpeer]
    barrier = pltpu.get_barrier_semaphore()
    for peer in peers:
        pl.semaphore_signal(barrier, inc=1, device_id=peer, device_id_type=MESH)

    def far(src, dst, send, recv, peer):
        return pltpu.make_async_remote_copy(
            src_ref=src, dst_ref=dst, send_sem=send, recv_sem=recv, device_id=peer,
            device_id_type=MESH,
        )

    def tok_copy(i, d):
        src, dst = ((tok, xg), (cot, cg), (vg, vg))[i]
        peer = ts[d]
        src = src.at[peer[1]] if i < 2 else src.at[t]
        return far(src, dst.at[t], tok_s.at[i, d], tok_r.at[i, d], peer)

    def out_copy(i, d):
        src, dst = ((yb, y_all), (gb, g_all))[i]
        peer = ts[d]
        return far(src.at[peer[1]], dst.at[t], out_s.at[i, d], out_r.at[i, d], peer)

    def az(ch, d):
        ref = gw.at[ch, t, z, x]
        return far(ref, ref, az_s.at[ch, d], az_r.at[ch, d], zs[d])

    def far_first(k):
        rising = k + jnp.where(z > k, 0, 1)
        falling = nz - 1 - k - jnp.where(z < nz - 1 - k, 0, 1)
        zz = jnp.where(2 * z < nz, falling, rising)
        return zz, lax.rem(zz - z + nz, nz) - 1

    def line(ch, zz, up):
        ref = gw.at[ch, t, zz, x]
        there = (lax.rem(z + nz + (1 if up else -1), nz) * 2 + x, t)
        return far(ref, ref, ln_s.at[ch, up, zz], ln_r.at[ch, zz], there)

    def pass_on(ch, zz):
        @pl.when((zz <= z) & (z < nz - 1))
        def _():
            line(ch, zz, 1).start()

        @pl.when((zz >= z) & (z > 0))
        def _():
            line(ch, zz, 0).start()

        ax(ch, zz).start()
        if ch == 1:
            ay(ch, zz).start()

    def line_step(ch, step):
        for zz, there in ((z - step, z >= step), (z + step, z + step < nz)):

            @pl.when(there)
            def _(zz=zz):
                line(ch, zz, 0).wait_recv()
                pass_on(ch, zz)

    def line_sent(ch):
        for zz in range(nz):

            @pl.when((zz <= z) & (z < nz - 1))
            def _(zz=zz):
                line(ch, zz, 1).wait_send()

            @pl.when((zz >= z) & (z > 0))
            def _(zz=zz):
                line(ch, zz, 0).wait_send()

    def az_start(ch):
        ref = gw.at[ch, t, z, x]
        for k in range(nz - 1):
            zz, d = far_first(k)
            far(ref, ref, az_s.at[ch, d], az_r.at[ch, d], (zz * 2 + x, t)).start()

    def zr_start(ch, k):
        zz, d = far_first(k)
        src = dv.at[ch, t, zz, x]
        far(src, rz.at[ch, d], rz_s.at[ch, d], rz_r.at[ch, d], (zz * 2 + x, t)).start()

    def ax(ch, zz):
        ref = gw.at[ch, t, zz, x]
        return far(ref, ref, ax_s.at[ch, zz], ax_r.at[ch, zz], xpeer)

    def ay(ch, zz):
        ref = gw.at[ch, t, zz] if ch == 0 else gw.at[ch, t, zz, x]
        return far(ref, ref, ay_s.at[ch, zz], ay_r.at[ch, zz], ypeer)

    def bx(ch, j):
        ref = gw.at[ch, t2 if j else t, :, x]
        return far(ref, ref, bx_s.at[ch, j], bx_r.at[ch, j], xpeer)

    def by(ch):
        ref = gw.at[ch, t, :, x]
        return far(ref, ref, by_s.at[ch], by_r.at[ch], ypeer)

    def cy():
        ref = gw.at[5, t, z, x]
        return far(ref, ref, by_s.at[5], by_r.at[5], ypeer)

    def cx(j):
        ref = gw.at[5, t2 if j else t, z, x]
        return far(ref, ref, bx_s.at[5, j], bx_r.at[5, j], xpeer)

    def cz(d, j):
        ref = gw.at[5, t2 if j else t, z]
        return far(ref, ref, cz_s.at[d, j], cz_r.at[d, j], zs[d])

    def ac(ch, j):
        ref = gw.at[ch, t2 if j else t]
        return far(ref, ref, ac_s.at[ch, j], ac_r.at[ch, j], cpeer)

    def kc(ch, j):
        return far(dv.at[ch, t1 if j else t3], rc.at[ch, j], k_s.at[ch, j], k_r.at[ch, j], cpeer)

    def ya(ch):
        return far(dv.at[ch, t2], ry.at[ch - 2], p_s.at[ch, 0], p_r.at[ch, 0], ypeer)

    def xa(ch):
        return far(dv.at[ch, t, :, 1 - x], r3.at[ch], q_s.at[ch], q_r.at[ch], xpeer)

    def zc(d, j):
        src = dv.at[5, t if j else t2, lax.rem(z + d + 1, nz)]
        return far(src, rzc.at[d, j], zc_s.at[d, j], zc_r.at[d, j], zs[d])

    def xc(j):
        src = dv.at[5, t if j else t2, z, 1 - x]
        return far(src, rxc.at[j], xc_s.at[j], xc_r.at[j], xpeer)

    def yc():
        return far(dv.at[5, t2, z, x], rxc.at[2], xc_s.at[2], xc_r.at[2], ypeer)

    def c_start():
        for k in range(nz - 1):
            zz, d = far_first(k)
            for j in range(2):
                src = dv.at[5, t if j else t2, zz]
                far(src, rzc.at[d, j], zc_s.at[d, j], zc_r.at[d, j], (zz * 2 + x, t)).start()

    def c_sum():
        for j, tt in enumerate((t2, t)):
            value = dv[5, tt, z].astype(F32)
            for d in range(nz - 1):
                zc(d, j).wait_recv()
                value = value + rzc[d, j].astype(F32)
            dv[5, tt, z] = value.astype(BF16)
            xc(j).start()

    def c_x():
        for j, tt in enumerate((t2, t)):
            xc(j).wait_recv()
            dv[5, tt, z, x] = add(dv[5, tt, z, x], rxc[j])
        yc().start()

    def c_end():
        yc().wait_recv()
        fin[5] = dv[5, t, z, x].astype(F32) + rxc[2].astype(F32)

    def slot_b(ch):
        return ch if isinstance(ch, int) and ch < 2 else ch - 2

    def piece_of(d):
        return far_first(d)[0] if d < nz - 1 else z

    def xp1(ch, d):
        zz = piece_of(d)
        src, dst = dv.at[ch, t, zz, 1 - x], rx.at[slot_b(ch), 1, zz]
        return far(src, dst, px_s.at[ch, d], px_r.at[ch, d], xpeer)

    def xb(ch, j):
        src = dv.at[ch, t if j else t2, :, 1 - x]
        return far(src, rx.at[slot_b(ch), j], p_s.at[ch, j], p_r.at[ch, j], xpeer)

    def yb2(ch):
        return far(dv.at[ch, t2, :, x], r3.at[ch], q_s.at[ch], q_r.at[ch], ypeer)

    def zr(ch, d):
        src = dv.at[ch, t, lax.rem(z + d + 1, nz), x]
        return far(src, rz.at[ch, d], rz_s.at[ch, d], rz_r.at[ch, d], zs[d])

    def core_first(ch):
        kc(ch, 0).wait_recv()
        dv[ch, t2] = add(dv[ch, t2], rc[ch, 0])

    def core_second(ch):
        kc(ch, 1).wait_recv()
        dv[ch, t] = add(dv[ch, t], rc[ch, 1])

    def second_a(ch):
        ya(ch).wait_recv()
        dv[ch, t] = add(dv[ch, t], ry[ch - 2])
        xa(ch).start()

    def first_half(ch):
        xb(ch, 0).wait_recv()
        dv[ch, t2, :, x] = add(dv[ch, t2, :, x], rx[slot_b(ch), 0])
        yb2(ch).start()

    def second_half(ch):
        xb(ch, 1).wait_recv()
        dv[ch, t, :, x] = add(dv[ch, t, :, x], rx[slot_b(ch), 1])

    def second_b(ch):
        first_half(ch)
        second_half(ch)

    def third(ch):
        (xa(ch) if ch in (2, 3) else yb2(ch)).wait_recv()
        dv[ch, t, :, x] = add(dv[ch, t, :, x], r3[ch])
        for k in range(nz - 1):
            zr_start(ch, k)

    def last_out(ch):
        core_second(ch)
        for d in range(nz):
            xp1(ch, d).start()

    def last_third(ch):
        yb2(ch).wait_recv()
        for d in range(nz):
            zz = piece_of(d)
            xp1(ch, d).wait_recv()
            value = dv[ch, t, zz, x].astype(F32) + rx[slot_b(ch), 1, zz].astype(F32)
            dv[ch, t, zz, x] = (value + r3[ch, zz].astype(F32)).astype(BF16)
            if d < nz - 1:
                zr_start(ch, d)

    def fourth(ch):
        value = dv[ch, t, z, x].astype(F32)
        for d in range(nz - 1):
            zr(ch, d).wait_recv()
            value = value + rz[ch, d].astype(F32)
        fin[ch] = value

    def small_t(d):
        return far(small.at[ts[d][1]], scr.at[d], sm_s.at[d], sm_r.at[d], ts[d])

    def small_z(d):
        return far(zb.at[z], zb.at[z], sm_s.at[3 + d], sm_r.at[3 + d], zs[d])

    def small_x():
        return far(sx, syr, sm_s.at[2 + nz], sm_r.at[2 + nz], xpeer)

    gw[0, t, z, x, :, :LANES] = wq[...]
    gw[0, t, z, x, :, LANES:] = wo[...]
    gw[1, t, z, x, :, :LANES] = wk[...]
    gw[1, t, z, x, :, LANES:] = wv[...]
    for i, ref in enumerate((g1, s1, bq, bv, bo, g2, s2, bd)):
        vg[t, i : i + 1, :] = ref[...]
    vg[t, 8:12, :] = bh[...]
    for h in range(heads):
        vg[t, 12 + 2 * h : 13 + 2 * h, :] = tab[h : h + 1, :LANES]
        vg[t, 13 + 2 * h : 14 + 2 * h, : TABLE - LANES] = tab[h : h + 1, LANES:]
        vg[t, 13 + 2 * h : 14 + 2 * h, TABLE - LANES :] = jnp.zeros((1, TPAD - TABLE), F32)
    vg[t, 12 + 2 * heads :, :] = jnp.zeros((SROWS - 12 - 2 * heads, LANES), F32)
    for s in range(2):
        gw[2 + s, t, z, x] = wh[:, s * CW : (s + 1) * CW]
        gw[4 + s, t, z, x] = wd[:, s * CW : (s + 1) * CW]
    pl.semaphore_wait(barrier, len(peers))
    own_tok = pltpu.make_async_copy(tok.at[t], xg.at[t], loc.at[0])
    own_cot = pltpu.make_async_copy(cot.at[t], cg.at[t], loc.at[1])
    own_tok.start()
    own_cot.start()
    for d in range(3):
        tok_copy(2, d).start()
    pass_on(1, z)
    pass_on(0, z)
    for d in range(3):
        tok_copy(0, d).start()
    cy().start()
    square[...] = jnp.zeros_like(square)
    square[:WT, :WT] = rel[...].astype(F32)
    rel_t = square[...].T[:PAD, :PAD]
    pick_at = jnp.concatenate([rel_t, rel_t], axis=1).astype(jnp.int32)
    lane = lax.broadcasted_iota(jnp.int32, (PAD, LANES), 1)
    low_at, high_at = jnp.minimum(pick_at, LANES - 1), jnp.maximum(pick_at - LANES, 0)

    def take(value, at):
        return jnp.take_along_axis(value, at, axis=1, mode="promise_in_bounds")

    def entry(tt, h):
        first = jnp.broadcast_to(vg[tt, 12 + 2 * h : 13 + 2 * h, :], (PAD, LANES))
        second = jnp.broadcast_to(vg[tt, 13 + 2 * h : 14 + 2 * h, :], (PAD, LANES))
        return jnp.where(pick_at < LANES, take(first, low_at), take(second, high_at))

    def bias_of(tt):
        for q in range(heads // 2):
            rg[tt, :, q * LANES : (q + 1) * LANES] = jnp.where(
                lane < PAD, entry(tt, 2 * q), entry(tt, 2 * q + 1)
            )

    number = lax.broadcasted_iota(jnp.int32, (PAD, TPAD), 1).astype(F32)
    found = jnp.full((PAD, TPAD), -1.0, F32)
    for i in range(WT):
        found = jnp.where(rel_t[:, i : i + 1] == number, float(i), found)
    inv[...] = found.astype(jnp.int32)
    square[...] = jnp.zeros_like(square)
    mine = reg[pl.ds(pl.multiple_of(t * slots, slots), slots), :]
    square[:slots, :WT] = mine.astype(F32)
    reg_row = square[:slots, :PAD]
    reg_row = jnp.concatenate([reg_row] * heads, axis=1)
    reg_col = square[...].T[:PAD, :slots]
    real = lax.broadcasted_iota(jnp.int32, (PAD, heads * PAD), 0) < WT
    for w in range(slots):
        same = reg_col[:, w : w + 1] == reg_row[w : w + 1, :]
        mask[w] = jnp.where(real, jnp.where(same, 0.0, -100.0), -1e30)
    for step in range(1, nz):
        line_step(1, step)
        line_step(0, step)
    az_start(2)
    az_start(4)
    cy().wait_recv()
    for j in range(2):
        cx(j).start()

    def wide(i):
        return jnp.concatenate([vg[tt, i : i + 1, :] for tt in range(nt)], axis=1)

    def put_small(i, value):
        for tt in range(nt):
            small[tt, i : i + 1, :] = value[:, tt * LANES : (tt + 1) * LANES]

    def spread(source, target):
        for tt in range(nt):
            xs[:, tt * LANES : (tt + 1) * LANES] = source[tt].astype(F32)
        zero = jnp.zeros((PAD - WT, C), F32)
        for w in range(slots):
            target[w * PAD : w * PAD + WT, :] = xs[w * WT : (w + 1) * WT, :]
            target[w * PAD + WT : (w + 1) * PAD, :] = zero

    def gather(source, target):
        for w in range(slots):
            xs[w * WT : (w + 1) * WT, :] = source[w * PAD : w * PAD + WT, :]
        for tt in range(nt):
            target[tt] = xs[:, tt * LANES : (tt + 1) * LANES].astype(BF16)

    def each(body, init=0):
        def step(i, carry):
            return body(i, pl.ds(pl.multiple_of(i * half, half), half), carry)

        return lax.fori_loop(0, nhalf, step, init)

    def weight(ch, tt, start=0, size=CW):
        return gw[ch, tt, :, :, :, start : start + size].reshape(C, size)

    def put_grad(ch, tt, value):
        dv[ch, tt] = value.astype(BF16).reshape(dv.shape[2:])

    def events(i, table):
        for when, todo in table.items():

            @pl.when(i == when)
            def _(todo=todo):
                for act in todo:
                    act()

    def z_to_xy(ch):
        for d in range(nz - 1):
            az(ch, d).wait_recv()
        bx(ch, 0).start()
        by(ch).start()

    def y_to_x(ch):
        by(ch).wait_recv()
        bx(ch, 1).start()

    def x_to_core(ch, j):
        bx(ch, j).wait_recv()
        ac(ch, j).start()

    def ay_to_bx():
        for d in range(nz):
            ay(1, d).wait_recv()
        bx(1, 1).start()

    def start_cz():
        for j in range(2):
            cx(j).wait_recv()
        for d in range(nz - 1):
            for j in range(2):
                cz(d, j).start()

    def groups_in():
        for d in range(nz):
            ay(0, d).wait_recv()
        ac(0, 1).start()
        x_to_core(1, 1)

    def start_cot():
        for d in range(3):
            tok_copy(1, d).start()

    def end_cz():
        for d in range(nz - 1):
            for j in range(2):
                cz(d, j).wait_recv()
        for j in range(2):
            ac(5, j).start()

    n_live = live[0] - t * slots
    small[...] = jnp.zeros_like(small)
    own_tok.wait()
    for i in (2, 0):
        for d in range(3):
            tok_copy(i, d).wait_recv()
    spread(xg, xp)
    gain1, shift1 = wide(0), wide(1)

    def start(i, at, carry):
        normed, rstd = norm(xp[at, :])
        n1[at, :] = normed
        r1[at, :] = rstd
        h = normed * gain1 + shift1
        h1[at, :] = h.astype(BF16)
        h1t[:, at] = h.T.astype(BF16)
        return carry

    each(start)
    for tt in range(nt):
        bias_of(tt)
    for d in range(nz):
        ax(1, d).wait_recv()
    ac(1, 0).start()
    for d in range(nz):
        ax(0, d).wait_recv()
        ay(0, d).start()
    ac(0, 0).start()
    z_to_xy(2)
    lane_head = lax.broadcasted_iota(jnp.int32, (PAD, LANES), 1) // HDIM
    ones = [(lane_head == h).astype(F32).astype(BF16) for h in range(heads)]

    def stack(value):
        return jnp.concatenate([value * ones[h] for h in range(heads)], axis=0)

    def pick(value):
        out = value[0:PAD]
        for h in range(1, heads):
            out = jnp.where(lane_head == h, value[h * PAD : (h + 1) * PAD], out)
        return out

    acc[...] = jnp.zeros_like(acc)

    in_first = {
        0: [ay_to_bx, lambda: az_start(3)],
        1: [start_cz],
        2: [lambda: y_to_x(2)],
        3: [lambda: y_to_x(4), lambda: z_to_xy(3)],
    }
    in_second = {
        0: [lambda: z_to_xy(4)],
        1: [groups_in, start_cot],
        2: [lambda: x_to_core(2, 0), lambda: x_to_core(4, 0)],
        3: [lambda: x_to_core(2, 1)],
    }

    def attend(i, carry):
        tt = group(i)

        @pl.when(i == 1)
        def _():
            for ch in range(2):
                ac(ch, 0).wait_recv()

        @pl.when(i == 3)
        def _():
            for ch in range(2):
                ac(ch, 1).wait_recv()

        q = (nn(h1[...], weight(0, tt, 0, LANES)) + vg[tt, 2:3, :]) * SCALE
        qs[tt] = q.astype(BF16)
        kv = nn(h1[...], weight(1, tt))
        kvs[tt, :, :LANES] = kv[:, :LANES].astype(BF16)
        kvs[tt, :, LANES:] = (kv[:, LANES:] + vg[tt, 3:4, :]).astype(BF16)

        def window(w, carry):
            at = pl.ds(pl.multiple_of(w * PAD, PAD), PAD)
            s = nt_dot(kvs[tt, at, :LANES], stack(qs[tt, at, :])) + rg[tt] + mask[w]
            e = jnp.exp(s - jnp.max(s, axis=0, keepdims=True))
            p = e / rowsum(e)
            probs[tt, w] = p
            att[tt, at, :] = pick(tn_dot(p.astype(BF16), kvs[tt, at, LANES:])).astype(BF16)
            return carry

        lax.fori_loop(0, slots // 2, window, 0, unroll=4)
        events(i, in_first)
        lax.fori_loop(slots // 2, slots, window, 0, unroll=4)
        acc[...] += nt_dot(att[tt], weight(0, tt, LANES, LANES))
        events(i, in_second)
        return carry

    lax.fori_loop(0, nt, attend, 0)
    own_cot.wait()
    for d in range(3):
        tok_copy(1, d).wait_recv()
    spread(cg, gy)
    b_out, gain2, shift2 = wide(4), wide(5), wide(6)

    def live_rows(i):
        slot = lax.div(i * half + lax.broadcasted_iota(jnp.int32, (half, 1), 0), PAD)
        return slot < n_live

    def middle(i, at, carry):
        x1 = xp[at, :] + acc[at, :] + b_out
        xp[at, :] = x1
        normed, rstd = norm(x1)
        n2[at, :] = normed
        r2[at, :] = rstd
        h = normed * gain2 + shift2
        low[at, :] = h.astype(BF16)
        h2t[:, at] = h.T.astype(BF16)
        g = jnp.where(live_rows(i), gy[at, :], 0.0)
        gy[at, :] = g
        gkv[at, :] = g.astype(BF16)
        gyt[:, at] = g.T.astype(BF16)
        return carry

    each(middle)
    acc[...] = jnp.zeros_like(acc)
    acc2[...] = jnp.zeros_like(acc2)
    def from_core(chs, j):
        for ch in chs:
            ac(ch, j).wait_recv()

    def sums_out():
        core_first(2)
        ya(2).start()
        core_first(4)
        for j in range(2):
            xb(4, j).start()

    mlp_before = {
        1: [lambda: from_core((2, 4), 0)],
        3: [lambda: from_core((2, 4), 1)],
        5: [lambda: from_core((3, 5), 0)],
        7: [lambda: from_core((3, 5), 1)],
    }
    mlp_after = {
        0: [lambda: x_to_core(4, 1)],
        1: [lambda: y_to_x(3), lambda: x_to_core(3, 0)],
        2: [end_cz],
        4: [lambda: core_second(2), lambda: core_second(4)],
        5: [sums_out, lambda: x_to_core(3, 1)],
    }

    def mlp(k, carry):
        s, i = lax.div(k, nt), lax.rem(k, nt)
        tt = group(i)
        up, down = 2 + s, 4 + s
        events(k, mlp_before)

        bias = vg[tt, pl.ds(8 + 2 * s, 2), :]
        bias = jnp.concatenate([bias[0:1], bias[1:2]], axis=1)
        hidden = nn(low[...], weight(up, tt)) + bias
        act, slope = gelu_pair(hidden)
        act_low = act.astype(BF16)
        acc[...] += nt_dot(act_low, weight(down, tt))
        put_grad(down, tt, nn(gyt[...], act_low))
        grad = nn(gkv[...], weight(down, tt)) * slope
        total = rowsum(grad)
        small[tt, pl.ds(8 + 2 * s, 1), :] = total[:, :LANES]
        small[tt, pl.ds(9 + 2 * s, 1), :] = total[:, LANES:]
        grad_low = grad.astype(BF16)
        put_grad(up, tt, nn(h2t[...], grad_low))
        acc2[...] += nt_dot(grad_low, weight(up, tt))

        for when, j in ((1, 1), (3, 0)):

            @pl.when(i == when)
            def _(j=j):
                kc(down, j).start()
                kc(up, j).start()

        events(k, mlp_after)
        return carry

    lax.fori_loop(0, 2 * nt, mlp, 0)
    b_down = wide(7)
    zero_row = jnp.zeros((1, C), F32)

    def turn(i, at, carry):
        xp[at, :] = jnp.where(live_rows(i), xp[at, :] + acc[at, :] + b_down, 0.0)
        e, normed, g = acc2[at, :], n2[at, :], gy[at, :]
        gx = norm_back(e * gain2, normed, r2[at, :]) + g
        gy[at, :] = gx
        low[at, :] = gx.astype(BF16)
        h2t[:, at] = gx.T.astype(BF16)
        sums = (rowsum(e * normed), rowsum(e), rowsum(gx), rowsum(g))
        return tuple(p + q for p, q in zip(carry, sums))

    sums = each(turn, (zero_row,) * 4)
    put_small(5, sums[0])
    put_small(6, sums[1])
    put_small(4, sums[2])
    put_small(7, sums[3])
    gather(xp, yb)
    own_y = pltpu.make_async_copy(yb.at[t], y_all.at[t], loc.at[2])
    own_y.start()
    core_second(5)
    core_first(5)
    c_start()
    core_second(3)
    core_first(3)
    ya(3).start()
    acc[...] = jnp.zeros_like(acc)

    def start_y():
        for d in range(3):
            out_copy(0, d).start()

    out_first = {
        0: [lambda: second_a(2)],
        1: [lambda: second_a(3)],
        2: [c_sum, lambda: third(2)],
        3: [lambda: first_half(1), lambda: first_half(0), c_x],
    }
    out_second = {
        0: [lambda: second_b(4), start_y],
        2: [lambda: third(4), lambda: third(3)],
        3: [lambda: fourth(2), lambda: fourth(4)],
    }

    def back(i, carry):
        tt = group(3 - i)
        gatt = gq
        gatt[...] = nn(low[...], weight(0, tt, LANES, LANES)).astype(BF16)
        pairs[...] = jnp.zeros_like(pairs)

        def window(w, carry):
            at = pl.ds(pl.multiple_of(w * PAD, PAD), PAD)
            q4, g4 = stack(qs[tt, at, :]), stack(gatt[at, :])
            p = probs[tt, w]
            dp = nt_dot(kvs[tt, at, LANES:], g4)
            ds = p * (dp - rowsum(p * dp))
            ds_low = ds.astype(BF16)
            pairs[...] += ds_low.astype(F32)
            gkv[at, :LANES] = nn(ds_low, q4).astype(BF16)
            gkv[at, LANES:CW] = nn(p.astype(BF16), g4).astype(BF16)
            gatt[at, :] = pick(tn_dot(ds_low, kvs[tt, at, :LANES])).astype(BF16)
            return carry

        lax.fori_loop(0, slots // 2, window, 0, unroll=4)
        events(i, out_first)
        lax.fori_loop(slots // 2, slots, window, 0, unroll=4)
        gk_gv = gkv[:, :CW]
        put_grad(1, tt, nn(h1t[...], gk_gv))

        @pl.when(i == 1)
        def _():
            core_first(1)
            xb(1, 0).start()

        @pl.when(i == 3)
        def _():
            last_out(1)

        left = nn(h1t[...], gatt[...]) * SCALE
        put_grad(0, tt, jnp.concatenate([left, nn(h2t[...], att[tt])], axis=1))

        @pl.when(i == 0)
        def _():
            kc(1, 0).start()
            kc(0, 0).start()

        @pl.when(i == 2)
        def _():
            kc(1, 1).start()
            kc(0, 1).start()

        @pl.when(i == 1)
        def _():
            core_first(0)
            xb(0, 0).start()

        @pl.when(i == 3)
        def _():
            last_out(0)

        small[tt, 2:3, :] = rowsum(gatt[...].astype(F32)) * SCALE
        small[tt, 3:4, :] = rowsum(gkv[:, LANES:CW].astype(F32))
        grad_q = nt_dot(gatt[...], weight(0, tt, 0, LANES)) * SCALE
        acc[...] += grad_q + nt_dot(gk_gv, weight(1, tt))
        for h in range(heads):
            lanes = h // 2 * LANES
            source = pairs[:, lanes : lanes + LANES]
            for q in range(TPAD // LANES):
                where = inv[:, q * LANES : (q + 1) * LANES]
                value = take(source, jnp.maximum(where, 0) + h % 2 * PAD)
                value = jnp.where(where >= 0, value, 0.0)
                small[tt, pl.ds(12 + 2 * h + q, 1), :] = rowsum(value)

        events(i, out_second)
        return carry

    lax.fori_loop(0, nt, back, 0)

    def finish(i, at, carry):
        e, normed = acc[at, :], n1[at, :]
        xp[at, :] = norm_back(e * gain1, normed, r1[at, :]) + gy[at, :]
        sums = (rowsum(e * normed), rowsum(e))
        return tuple(p + q for p, q in zip(carry, sums))

    sums = each(finish, (zero_row,) * 2)
    put_small(0, sums[0])
    put_small(1, sums[1])
    for d in range(3):
        small_t(d).start()
    gather(xp, gb)
    own_g = pltpu.make_async_copy(gb.at[t], g_all.at[t], loc.at[3])
    own_g.start()
    for d in range(3):
        out_copy(1, d).start()
    last_third(1)
    for d in range(3):
        small_t(d).wait_recv()
    zb[z] = small[t] + scr[0] + (scr[1] + scr[2])
    for d in range(nz - 1):
        small_z(d).start()
    fourth(3)
    c_end()
    last_third(0)
    for d in range(nz - 1):
        small_z(d).wait_recv()
    value = zb[0]
    for zz in range(1, nz):
        value = value + zb[zz]
    sx[...] = value
    small_x().start()
    fourth(1)
    fourth(0)
    small_x().wait_recv()
    tot[...] = sx[...] + syr[...]
    for i in range(2):
        for d in range(3):
            out_copy(i, d).wait_recv()
    sent = [tok_copy(i, d) for i in range(3) for d in range(3)]
    sent += [out_copy(i, d) for i in range(2) for d in range(3)]
    for ch in range(NCH):
        sent += [ac(ch, j) for j in range(2)] + [kc(ch, j) for j in range(2)]
        if ch < 5:
            sent += [az(ch, d) for d in range(nz - 1) if ch > 1]
            sent += [zr(ch, d) for d in range(nz - 1)]
        if ch < 2:
            sent += [ax(ch, d) for d in range(nz)] + [ay(ch, d) for d in range(nz)]
            sent += [xp1(ch, d) for d in range(nz)] + [xb(ch, 0), yb2(ch)]
        elif ch < 5:
            sent += [by(ch), bx(ch, 0), bx(ch, 1)]
    sent += [bx(1, 1), cy(), cx(0), cx(1)]
    sent += [ya(2), xa(2), ya(3), xa(3), xb(4, 0), xb(4, 1), yb2(4), xc(0), xc(1), yc()]
    sent += [zc(d, j) for d in range(nz - 1) for j in range(2)]
    sent += [cz(d, j) for d in range(nz - 1) for j in range(2)]
    sent += [small_t(d) for d in range(3)] + [small_x()]
    sent += [small_z(d) for d in range(nz - 1)]
    for copy in sent:
        copy.wait_send()
    line_sent(0)
    line_sent(1)
    own_y.wait()
    own_g.wait()


def block_call(nt, nz, slots, *args):
    tok, deep, heads = args[1], args[3].shape[0], args[18].shape[0]
    real = tok.shape[1]
    rows, wide = slots * PAD, heads * PAD
    piece = (nz, 2, deep, CW)
    row = (nt, real, LANES)

    def vm(shape, kind=BF16):
        return pltpu.VMEM(shape, kind)

    def pair(*shape):
        return [DMA(shape), DMA(shape)]

    small = (SROWS, LANES)
    return pl.pallas_call(
        functools.partial(block, nt, nz, slots),
        name="block",
        out_shape=(
            jax.ShapeDtypeStruct(row, BF16),
            jax.ShapeDtypeStruct(row, BF16),
            jax.ShapeDtypeStruct((NCH, deep, CW), F32),
            jax.ShapeDtypeStruct(small, F32),
        ),
        in_specs=[SM, ANY, ANY] + [VM] * 18,
        out_specs=(ANY, ANY, VM, VM),
        scratch_shapes=[
            vm(row),
            vm(row),
            vm((NCH, nt) + piece),
            vm((nt,) + small, F32),
            vm((nt, PAD, wide), F32),
            vm((NCH, nt) + piece),
            vm((NCH, 2) + piece),
            vm((2,) + piece),
            vm((3, 2, nz, deep, CW)),
            vm((NCH, nz, deep, CW)),
            vm((NCH, nz - 1, deep, CW)),
            vm((nz - 1, 2, 2, deep, CW)),
            vm((3, deep, CW)),
            vm((3,) + small, F32),
            vm(small, F32),
            vm(small, F32),
            vm((nz,) + small, F32),
            vm((nt,) + small, F32),
            vm(row),
            vm(row),
            vm((LANES, LANES), F32),
            vm((slots, PAD, wide), F32),
            vm((PAD, TPAD), jnp.int32),
            vm((real, C), F32),
            vm((rows, C), F32),
            vm((rows, C), F32),
            vm((rows, C)),
            vm((C, rows)),
            vm((C, rows)),
            vm((C, rows)),
            vm((nt, rows, LANES)),
            vm((nt, rows, CW)),
            vm((nt, slots, PAD, wide), F32),
            vm((nt, rows, LANES)),
            vm((rows, C), F32),
            vm((rows, C), F32),
            vm((rows, C), F32),
            vm((rows, 1), F32),
            vm((rows, C), F32),
            vm((rows, 1), F32),
            vm((rows, C)),
            vm((rows, C)),
            vm((rows, LANES)),
            vm((PAD, wide), F32),
            DMA((4,)),
        ]
        + pair(3, 3)
        + pair(2, 3)
        + [DMA((2, 2, nz)), DMA((2, nz))]
        + pair(NCH, nz - 1)
        + pair(2, nz)
        + pair(2, nz)
        + pair(NCH, 2)
        + pair(NCH, 2)
        + pair(NCH)
        + pair(nz - 1, 2)
        + pair(2, nz)
        + pair(nz - 1, 2)
        + pair(3)
        + pair(NCH, 2)
        + pair(NCH, 2)
        + pair(NCH)
        + pair(NCH, nz - 1)
        + pair(3 + nz),
        compiler_params=pltpu.CompilerParams(
            collective_id=0, has_side_effects=True, vmem_limit_bytes=60 * 2**20
        ),
    )(*args)


def spell(y_all, g_all, fin, tot, *outs):
    (
        y_out, g_out, d_g1, d_s1, d_wq, d_wk, d_wv, d_bq, d_bv, d_wo, d_bo, d_g2, d_s2, d_wh, d_bh,
        d_wd, d_bd, d_tab,
    ) = outs
    y_out[...] = y_all[...].astype(F32)
    g_out[...] = g_all[...].astype(F32)
    d_wq[...] = fin[0, :, :LANES]
    d_wk[...] = fin[1, :, :LANES]
    d_wv[...] = fin[1, :, LANES:]
    d_wo[...] = fin[0, :, LANES:]
    for s in range(2):
        d_wh[:, s * CW : (s + 1) * CW] = fin[2 + s]
        d_wd[:, s * CW : (s + 1) * CW] = fin[4 + s]
    for i, ref in enumerate((d_g1, d_s1, d_bq, d_bv, d_bo, d_g2, d_s2, d_bd)):
        ref[...] = tot[i : i + 1, :]
    d_bh[...] = tot[8:12, :]
    for h in range(d_tab.shape[0]):
        d_tab[h : h + 1, :LANES] = tot[12 + 2 * h : 13 + 2 * h]
        d_tab[h : h + 1, LANES:] = tot[13 + 2 * h : 14 + 2 * h, : TABLE - LANES]


def spell_call(outs, *args):
    return pl.pallas_call(
        spell,
        name="spell",
        out_shape=outs,
        in_specs=[VM] * 4,
        out_specs=(VM,) * len(outs),
        compiler_params=pltpu.CompilerParams(vmem_limit_bytes=60 * 2**20),
    )(*args)


def per_device(
    nt, na, tokens, gain_one, shift_one, w_query, w_key, w_value, b_query, b_value, w_out, b_out,
    gain_two, shift_two, w_hidden, b_hidden, w_down, b_down, bias_table, rel_index, region,
    win_count, cotangent,
):
    slots = region.shape[0] // nt
    cut = (nt, slots * WT, LANES)
    vectors = [gain_one, shift_one, b_query, b_value, b_out, gain_two, shift_two, b_down]
    parts = block_call(
        nt, na // 2, slots,
        win_count, tokens.reshape(cut), cotangent.reshape(cut),
        w_query, w_key, w_value, w_out.T, w_hidden, w_down.T,
        *[v.reshape(1, LANES) for v in vectors],
        b_hidden.reshape(-1, LANES), bias_table.T, rel_index, region,
    )

    def out(like, shape=None):
        return jax.ShapeDtypeStruct(shape or like.shape, F32)

    one = (1, LANES)
    shapes = (
        out(tokens, cut), out(tokens, cut), out(gain_one, one), out(gain_one, one), out(w_query),
        out(w_key), out(w_value), out(b_query, one), out(b_value, one), out(w_out, w_out.shape[::-1]),
        out(b_out, one), out(gain_two, one), out(shift_two, one), out(w_hidden),
        out(b_hidden, (b_hidden.shape[0] // LANES, LANES)), out(w_down, w_down.shape[::-1]),
        out(b_down, one), out(bias_table, bias_table.shape[::-1]),
    )
    likes = (
        tokens, tokens, gain_one, gain_one, w_query, w_key, w_value, b_query, b_value, w_out,
        b_out, gain_two, shift_two, w_hidden, b_hidden, w_down, b_down, bias_table,
    )
    values = spell_call(shapes, *parts)
    turned = (9, 15, 17)
    return tuple(
        v.T if i in turned else v.reshape(like.shape)
        for i, (v, like) in enumerate(zip(values, likes))
    )


def solution(mesh):
    return jax.shard_map(
        functools.partial(per_device, mesh.shape["ta"], mesh.shape["wa"]),
        mesh=mesh,
        in_specs=(
            P("wa", "ta"),
            P("ta"),
            P("ta"),
            P("wa", "ta"),
            P("wa", "ta"),
            P("wa", "ta"),
            P("ta"),
            P("ta"),
            P("ta", "wa"),
            P("ta"),
            P("ta"),
            P("ta"),
            P("wa", "ta"),
            P("ta"),
            P("ta", "wa"),
            P("ta"),
            P(None, "ta"),
            P(),
            P("wa", None),
            P("wa"),
            P("wa", "ta"),
        ),
        out_specs=(
            P("wa", "ta"),
            P("wa", "ta"),
            P("ta"),
            P("ta"),
            P("wa", "ta"),
            P("wa", "ta"),
            P("wa", "ta"),
            P("ta"),
            P("ta"),
            P("ta", "wa"),
            P("ta"),
            P("ta"),
            P("ta"),
            P("wa", "ta"),
            P("ta"),
            P("ta", "wa"),
            P("ta"),
            P(None, "ta"),
        ),
        check_vma=False,
    )
```

```python
import functools

import jax
import jax.numpy as jnp
from jax import lax
from jax.experimental import pallas as pl
from jax.experimental.pallas import tpu as pltpu
from jax.sharding import PartitionSpec as P

C = 512
HDIM = 32
WT = 49
PAD = 64
TABLE = 169
TPAD = 256
NCH = 6
CW = 256
LANES = 128
SROWS = 24
SCALE = HDIM ** (-0.5)
EPS = 1e-05
F32 = jnp.float32
BF16 = jnp.bfloat16
MESH = pl.DeviceIdType.MESH
ANY = pl.BlockSpec(memory_space=pl.ANY)
VM = pl.BlockSpec(memory_space=pltpu.VMEM)
SM = pl.BlockSpec(memory_space=pltpu.SMEM)
DMA = pltpu.SemaphoreType.DMA


WAY_IN = ("A", "B", "A", "B", "E", "C")
WAY_OUT = ("B", "B", "B", "C", "A", "B")
MLP_ORDER = (0, 1, 3, 2)
PLAN = {
    "h0": ("az2",),
    "h1": ("az4", "yx1",),
    "h2": ("zx2", "ay0",),
    "h3": ("az3",),
    "a0f": ("c11", "cot",),
    "a1f": ("zt4", "az5", "xy2", "zx4",),
    "a1s": ("c02", "zy3", "c10",),
    "a3f": ("zx3",),
    "a3s": ("c04",),
    "mid": ("c12", "c14",),
    "m1": ("yx3", "c03",),
    "m2": ("c15",),
    "m3": ("c05",),
    "m4": ("o14", "c13", "ot2", "oo2",),
    "m7": ("o22", "oo3", "oo5",),
    "turn": ("ot3",),
    "b0f": ("ot5", "yout",),
    "b0d": ("o24",),
    "b0s": ("o32",),
    "b1d": ("ot1", "o25", "ot0",),
    "b2d": ("o34",),
    "b3f": ("o21",),
    "b3d": ("oo1", "oo0",),
    "b3s": ("o35",),
    "t1": ("o20", "o23",),
    "t2": ("g",),
    "t3": ("o31", "o30",),
    "t4": ("o33",),
}


def plan_order(sched):
    out = list(sched.get("h0", ())) + list(sched.get("h1", ()))
    out += list(sched.get("h2", ())) + ["use_a0"]
    out += sched.get("h3", ())
    for i in range(4):
        out += ([f"use_a{i}"] if i else []) + list(sched.get(f"a{i}f", ()))
        out += sched.get(f"a{i}s", ())
    out += list(sched.get("mid", ()))
    for k in range(8):
        out += [f"use_m{k}"] + list(sched.get(f"m{k}", ()))
    out += sched.get("turn", ())
    for i in range(4):
        for part in "fds":
            out += sched.get(f"b{i}{part}", ())
    for i in range(1, 6):
        out += sched.get(f"t{i}", ())
    return out + ["end"]


def flip(bit, by):
    return bit + by - 2 * bit * by


def add(left, right):
    return (left.astype(F32) + right.astype(F32)).astype(BF16)


def nn(left, right):
    return jnp.dot(left, right, preferred_element_type=F32)


def nt_dot(left, right):
    return lax.dot_general(left, right, (((1,), (1,)), ((), ())), preferred_element_type=F32)


def tn_dot(left, right):
    return lax.dot_general(left, right, (((0,), (0,)), ((), ())), preferred_element_type=F32)


def norm(value):
    mean = jnp.mean(value, axis=1, keepdims=True)
    spread = jnp.mean(value * value, axis=1, keepdims=True) - mean * mean
    rstd = lax.rsqrt(spread + EPS)
    return (value - mean) * rstd, rstd


def norm_back(scaled, normed, rstd):
    first = jnp.mean(scaled, axis=1, keepdims=True)
    second = jnp.mean(scaled * normed, axis=1, keepdims=True)
    return rstd * (scaled - first - normed * second)


def gelu_pair(u):
    cdf = 0.5 + 0.5 * lax.erf(u * (0.5**0.5))
    pdf = jnp.exp(-0.5 * u * u) * ((2.0 * jnp.pi) ** -0.5)
    return u * cdf, cdf + u * pdf


def rowsum(value):
    return jnp.sum(value, axis=0, keepdims=True)


def block(nt, nz, slots, *refs):
    live, tok, cot, wq, wk, wv, wo, wh, wd = refs[:9]
    outside, refs = refs[9:21], refs[21:]
    inside, refs = refs[4:16], refs[:4] + refs[16:]
    g1, s1, bq, bv, bo, g2, s2, bd, bh, tab, rel, reg = inside
    (
        y_all, g_all, fin, tot,
        xg, cg, gw, vg, rg, dv, rc, ry, rx, r3, rz, rzc, rxc, scr, syr, sx, zb, small, yb, gb, square, mask, inv,
        xs, xp, gy, h1, h1t, h2t, gyt, qs, kvs, probs, att, acc, acc2, n1, r1, n2, r2, low, gkv, gq, gatt,
        pairs,
        loc, ld, tok_s, tok_r, out_s, out_r, az_s, az_r, ax_s, ax_r, ay_s, ay_r, ac_s, ac_r,
        bx_s, bx_r, by_s, by_r, px_s, px_r, zc_s, zc_r, xc_s,
        xc_r, k_s, k_r, p_s, p_r, q_s, q_r, rz_s, rz_r, sm_s, sm_r,
    ) = refs
    heads = LANES // HDIM
    rows = slots * PAD
    half = 2 * PAD
    nhalf = rows // half
    a, t = lax.axis_index("wa"), lax.axis_index("ta")
    x, z, c, y = lax.rem(a, 2), lax.div(a, 2), lax.rem(t, 2), lax.div(t, 2)

    def group(m):
        return 2 * flip(y, m // 2 if isinstance(m, int) else lax.div(m, 2)) + flip(
            c, m % 2 if isinstance(m, int) else lax.rem(m, 2)
        )

    t1, t2, t3 = group(1), group(2), group(3)
    xpeer, ypeer, cpeer = (z * 2 + (1 - x), t), (a, t2), (a, t1)
    zs = [(lax.rem(z + d, nz) * 2 + x, t) for d in range(1, nz)]
    ts = [(a, tt) for tt in (t1, t2, t3)]
    peers = zs + ts + [xpeer]
    barrier = pltpu.get_barrier_semaphore()
    for peer in peers:
        pl.semaphore_signal(barrier, inc=1, device_id=peer, device_id_type=MESH)

    def far(src, dst, send, recv, peer):
        return pltpu.make_async_remote_copy(
            src_ref=src, dst_ref=dst, send_sem=send, recv_sem=recv, device_id=peer,
            device_id_type=MESH,
        )

    def tok_copy(i, d):
        src, dst = ((tok, xg), (cot, cg), (vg, vg))[i]
        peer = ts[d]
        src = src.at[peer[1]] if i < 2 else src.at[t]
        return far(src, dst.at[t], tok_s.at[i, d], tok_r.at[i, d], peer)

    def out_copy(i, d):
        src, dst = ((yb, y_all), (gb, g_all))[i]
        peer = ts[d]
        return far(src.at[peer[1]], dst.at[t], out_s.at[i, d], out_r.at[i, d], peer)

    def az(ch, d, j=0):
        far_t = t2 if j else t
        ref = gw.at[ch, far_t, z] if WAY_IN[ch] == "C" else gw.at[ch, far_t, z, x]
        return far(ref, ref, az_s.at[ch, d, j], az_r.at[ch, d, j], zs[d])

    def az_all(ch):
        both = 2 if WAY_IN[ch] in "CE" else 1
        return [az(ch, d, j) for d in range(nz - 1) for j in range(both)]

    def az_from(ch, zz):
        ref, d = gw.at[ch, t, z, x], lax.rem(z - zz + nz, nz) - 1
        return far(ref, ref, az_s.at[ch, d, 0], az_r.at[ch, d, 0], xpeer)

    def far_first(k):
        rising = k + jnp.where(z > k, 0, 1)
        falling = nz - 1 - k - jnp.where(z < nz - 1 - k, 0, 1)
        zz = jnp.where(2 * z < nz, falling, rising)
        return zz, lax.rem(zz - z + nz, nz) - 1

    def az_start(ch):
        for k in range(nz - 1):
            zz, d = far_first(k)
            for j in range(2 if WAY_IN[ch] in "CE" else 1):
                far_t = t2 if j else t
                ref = gw.at[ch, far_t, z] if WAY_IN[ch] == "C" else gw.at[ch, far_t, z, x]
                peer = (zz * 2 + x, t)
                far(ref, ref, az_s.at[ch, d, j], az_r.at[ch, d, j], peer).start()

    def zr_start(ch, k):
        zz, d = far_first(k)
        src = dv.at[ch, t, zz, x]
        far(src, rz.at[ch, d], rz_s.at[ch, d], rz_r.at[ch, d], (zz * 2 + x, t)).start()

    def ax(ch, zz):
        ref = gw.at[ch, t, zz, x]
        return far(ref, ref, ax_s.at[ch, zz], ax_r.at[ch, zz], xpeer)

    def ay(ch, zz):
        ref = gw.at[ch, t, zz] if ch == 0 else gw.at[ch, t, zz, x]
        return far(ref, ref, ay_s.at[ch, zz], ay_r.at[ch, zz], ypeer)

    def bx(ch, j):
        ref = gw.at[ch, t2 if j else t, :, x]
        return far(ref, ref, bx_s.at[ch, j], bx_r.at[ch, j], xpeer)

    def by(ch):
        ref = gw.at[ch, t] if WAY_IN[ch] == "A" else gw.at[ch, t, :, x]
        return far(ref, ref, by_s.at[ch], by_r.at[ch], ypeer)

    def cy(ch):
        ref = gw.at[ch, t, z, x]
        return far(ref, ref, by_s.at[ch], by_r.at[ch], ypeer)

    def cx(ch, j):
        ref = gw.at[ch, t2 if j else t, z, x]
        return far(ref, ref, bx_s.at[ch, j], bx_r.at[ch, j], xpeer)

    def ac(ch, j):
        ref = gw.at[ch, t2 if j else t]
        return far(ref, ref, ac_s.at[ch, j], ac_r.at[ch, j], cpeer)

    def kc(ch, j):
        return far(dv.at[ch, t1 if j else t3], rc.at[ch, j], k_s.at[ch, j], k_r.at[ch, j], cpeer)

    a_slot = {ch: i for i, ch in enumerate(c for c in range(NCH) if WAY_OUT[c] == "A")}
    b_slot = {ch: i for i, ch in enumerate(c for c in range(NCH) if WAY_OUT[c] == "B")}
    c_slot = {ch: i for i, ch in enumerate(c for c in range(NCH) if WAY_OUT[c] == "C")}

    def ya(ch):
        return far(dv.at[ch, t2], ry.at[a_slot[ch]], p_s.at[ch, 0], p_r.at[ch, 0], ypeer)

    def xa(ch):
        return far(dv.at[ch, t, :, 1 - x], r3.at[ch], q_s.at[ch], q_r.at[ch], xpeer)

    def piece_of(d):
        return far_first(d)[0] if d < nz - 1 else z

    def xp1(ch, d):
        zz = piece_of(d)
        src, dst = dv.at[ch, t, zz, 1 - x], rx.at[b_slot[ch], 1, zz]
        return far(src, dst, px_s.at[ch, d], px_r.at[ch, d], xpeer)

    def xb(ch, j):
        src = dv.at[ch, t if j else t2, :, 1 - x]
        return far(src, rx.at[b_slot[ch], j], p_s.at[ch, j], p_r.at[ch, j], xpeer)

    def yb2(ch):
        return far(dv.at[ch, t2, :, x], r3.at[ch], q_s.at[ch], q_r.at[ch], ypeer)

    def zr(ch, d):
        src = dv.at[ch, t, lax.rem(z + d + 1, nz), x]
        return far(src, rz.at[ch, d], rz_s.at[ch, d], rz_r.at[ch, d], zs[d])

    def zc(ch, d, j):
        src, i = dv.at[ch, t if j else t2, lax.rem(z + d + 1, nz)], c_slot[ch]
        return far(src, rzc.at[i, d, j], zc_s.at[i, d, j], zc_r.at[i, d, j], zs[d])

    def zc_start(ch, j):
        i = c_slot[ch]
        for k in range(nz - 1):
            zz, d = far_first(k)
            src, peer = dv.at[ch, t if j else t2, zz], (zz * 2 + x, t)
            far(src, rzc.at[i, d, j], zc_s.at[i, d, j], zc_r.at[i, d, j], peer).start()

    def xc(ch, j):
        src, i = dv.at[ch, t if j else t2, z, 1 - x], c_slot[ch]
        return far(src, rxc.at[i, j], xc_s.at[i, j], xc_r.at[i, j], xpeer)

    def yc(ch):
        i = c_slot[ch]
        return far(dv.at[ch, t2, z, x], rxc.at[i, 2], xc_s.at[i, 2], xc_r.at[i, 2], ypeer)

    def small_t(d):
        return far(small.at[ts[d][1]], scr.at[d], sm_s.at[d], sm_r.at[d], ts[d])

    def small_z(d):
        return far(zb.at[z], zb.at[z], sm_s.at[3 + d], sm_r.at[3 + d], zs[d])

    def small_x():
        return far(sx, syr, sm_s.at[2 + nz], sm_r.at[2 + nz], xpeer)

    def lanes(ch, i, size):
        return gw.at[ch, t, z, x, :, pl.ds(i * size, size)]

    loads = [(wq, lanes(0, 0, LANES)), (wo, lanes(0, 1, LANES))]
    loads += [(wk, lanes(1, 0, LANES)), (wv, lanes(1, 1, LANES))]
    for i in range(2):
        loads += [(wh.at[:, pl.ds(i * CW, CW)], gw.at[2 + i, t, z, x])]
        loads += [(wd.at[:, pl.ds(i * CW, CW)], gw.at[4 + i, t, z, x])]
    loads += list(zip(outside, inside))
    loads = [pltpu.make_async_copy(*pair, ld.at[i]) for i, pair in enumerate(loads)]
    for copy in loads:
        copy.start()
    for copy in loads:
        copy.wait()
    for i, ref in enumerate((g1, s1, bq, bv, bo, g2, s2, bd)):
        vg[t, i : i + 1, :] = ref[...]
    vg[t, 8:12, :] = bh[...]
    for h in range(heads):
        vg[t, 12 + 2 * h : 13 + 2 * h, :] = tab[h : h + 1, :LANES]
        vg[t, 13 + 2 * h : 14 + 2 * h, : TABLE - LANES] = tab[h : h + 1, LANES:]
        vg[t, 13 + 2 * h : 14 + 2 * h, TABLE - LANES :] = jnp.zeros((1, TPAD - TABLE), F32)
    vg[t, 12 + 2 * heads :, :] = jnp.zeros((SROWS - 12 - 2 * heads, LANES), F32)
    pl.semaphore_wait(barrier, len(peers))
    own_tok = pltpu.make_async_copy(tok.at[t], xg.at[t], loc.at[0])
    own_cot = pltpu.make_async_copy(cot.at[t], cg.at[t], loc.at[1])
    own_tok.start()
    own_cot.start()
    early = [ch for ch in range(2, NCH) if WAY_IN[ch] in "CE"]
    first = [ch for ch in early if f"az{ch}" in PLAN.get("h0", ())]
    for ch in first:
        cy(ch).start()
    for d in range(3):
        tok_copy(2, d).start()
    az_start(1)
    ax(1, z).start()
    ay(1, z).start()
    az_start(0)
    ax(0, z).start()
    for d in range(3):
        tok_copy(0, d).start()
    for ch in early:
        if ch not in first:
            cy(ch).start()
    square[...] = jnp.zeros_like(square)
    square[:WT, :WT] = rel[...].astype(F32)
    rel_t = square[...].T[:PAD, :PAD]
    pick_at = jnp.concatenate([rel_t, rel_t], axis=1).astype(jnp.int32)
    lane = lax.broadcasted_iota(jnp.int32, (PAD, LANES), 1)
    low_at, high_at = jnp.minimum(pick_at, LANES - 1), jnp.maximum(pick_at - LANES, 0)

    def take(value, at):
        return jnp.take_along_axis(value, at, axis=1, mode="promise_in_bounds")

    def entry(tt, h):
        first = jnp.broadcast_to(vg[tt, 12 + 2 * h : 13 + 2 * h, :], (PAD, LANES))
        second = jnp.broadcast_to(vg[tt, 13 + 2 * h : 14 + 2 * h, :], (PAD, LANES))
        return jnp.where(pick_at < LANES, take(first, low_at), take(second, high_at))

    def bias_of(tt):
        for q in range(heads // 2):
            rg[tt, :, q * LANES : (q + 1) * LANES] = jnp.where(
                lane < PAD, entry(tt, 2 * q), entry(tt, 2 * q + 1)
            )

    number = lax.broadcasted_iota(jnp.int32, (PAD, TPAD), 1).astype(F32)
    found = jnp.full((PAD, TPAD), -1.0, F32)
    for i in range(WT):
        found = jnp.where(rel_t[:, i : i + 1] == number, float(i), found)
    inv[...] = found.astype(jnp.int32)
    square[...] = jnp.zeros_like(square)
    mine = reg[pl.ds(pl.multiple_of(t * slots, slots), slots), :]
    square[:slots, :WT] = mine.astype(F32)
    reg_row = square[:slots, :PAD]
    reg_row = jnp.concatenate([reg_row] * heads, axis=1)
    reg_col = square[...].T[:PAD, :slots]
    real = lax.broadcasted_iota(jnp.int32, (PAD, heads * PAD), 0) < WT
    for w in range(slots):
        same = reg_col[:, w : w + 1] == reg_row[w : w + 1, :]
        mask[w] = jnp.where(real, jnp.where(same, 0.0, -100.0), -1e30)
    def cross(ch):
        cy(ch).wait_recv()
        if WAY_IN[ch] == "C":
            for j in range(2):
                cx(ch, j).start()

    for ch in first:
        cross(ch)

    def wide(i):
        return jnp.concatenate([vg[tt, i : i + 1, :] for tt in range(nt)], axis=1)

    def put_small(i, value):
        for tt in range(nt):
            small[tt, i : i + 1, :] = value[:, tt * LANES : (tt + 1) * LANES]

    def spread(source, target):
        for tt in range(nt):
            xs[:, tt * LANES : (tt + 1) * LANES] = source[tt].astype(F32)
        zero = jnp.zeros((PAD - WT, C), F32)
        for w in range(slots):
            target[w * PAD : w * PAD + WT, :] = xs[w * WT : (w + 1) * WT, :]
            target[w * PAD + WT : (w + 1) * PAD, :] = zero

    def gather(source, target):
        for w in range(slots):
            xs[w * WT : (w + 1) * WT, :] = source[w * PAD : w * PAD + WT, :]
        for tt in range(nt):
            target[tt] = xs[:, tt * LANES : (tt + 1) * LANES].astype(BF16)

    def each(body, init=0):
        def step(i, carry):
            return body(i, pl.ds(pl.multiple_of(i * half, half), half), carry)

        return lax.fori_loop(0, nhalf, step, init)

    def weight(ch, tt, start=0, size=CW):
        return gw[ch, tt, :, :, :, start : start + size].reshape(C, size)

    def put_grad(ch, tt, value):
        dv[ch, tt] = value.astype(BF16).reshape(dv.shape[2:])

    def tok_all(i):
        return [tok_copy(i, d) for d in range(3)]

    def arrivals(name):
        kind, ch = name[:-1], int(name[-1])
        if kind == "x":
            return [ax(ch, zz) for zz in range(nz)]
        if kind == "ay":
            return [ay(ch, zz) for zz in range(nz)]
        if kind == "z":
            return az_all(ch)
        if kind in ("xo", "xt"):
            return [bx(ch, int(kind == "xt"))]
        if kind == "yo":
            return [by(ch)]
        if kind in ("k0", "k1"):
            return [ac(ch, int(kind == "k1"))]
        if kind in ("r0", "r1"):
            return [kc(ch, int(kind == "r1"))]
        if kind == "ya":
            return [ya(ch)]
        if kind == "xa":
            return [xa(ch)]
        if kind == "xbt":
            return [xb(ch, 0)]
        if kind == "xbo":
            return [xb(ch, 1)]
        if kind == "yb":
            return [yb2(ch)]
        if kind == "zc":
            return [zc(ch, d, j) for d in range(nz - 1) for j in range(2)]
        assert kind == "xc"
        return [xc(ch, 0), xc(ch, 1)]

    def own_of(ch):
        return ("z%d" if WAY_IN[ch] == "C" else "xo%d") % ch

    def other_y_of(ch):
        return {"A": "yo%d", "B": "xt%d", "C": "z%d", "E": "xt%d"}[WAY_IN[ch]] % ch

    def waits_of(entry):
        fixed = {
            "use_a0": ("x1", "x0"), "use_a1": ("k01", "k00"), "use_a2": ("xt1", "ay0"),
            "use_a3": ("k11", "k10"), "yx1": ("ay1",), "c11": ("xt1",), "c10": ("ay0",),
            "ay0": ("x0",), "end": (), "cot": (), "yout": (), "g": (),
        }
        if entry in fixed:
            return fixed[entry]
        if entry.startswith("use_m"):
            k = int(entry[-1])
            chs, m = ((2, 4) if k < nt else (3, 5)), MLP_ORDER[k % nt]
            names = {0: own_of, 1: "k0{}".format, 2: other_y_of, 3: "k1{}".format}[m]
            return tuple(names(ch) for ch in chs)
        kind, ch = entry[:-1], int(entry[-1])
        way = WAY_OUT[ch]
        names = {
            "az": (), "zx": ("z",), "zy": ("z",), "zt": ("z",), "yx": ("yo",), "xy": ("xo",),
            "o1": ("r0",), "oo": ("r1",), "ot": ("r0",),
            "o2": {"A": ("ya", "r1"), "B": ("xbt",), "C": ("zc",)}[way],
            "o3": {"A": ("xa",), "B": ("yb",) if ch < 2 else ("xbo", "yb"), "C": ("xc",)}[way],
        }
        if kind == "c0":
            return (own_of(ch),)
        if kind == "c1":
            return (other_y_of(ch),)
        return tuple(f"{n}{ch}" for n in names[kind])

    first_use = {}
    for item in plan_order(PLAN):
        for name in waits_of(item):
            first_use.setdefault(name, item)

    def arrive(entry):
        for name in waits_of(entry):
            if first_use[name] == entry:
                for copy in arrivals(name):
                    copy.wait_recv()

    def act(entry):
        arrive(entry)
        if entry == "cot":
            for copy in tok_all(1):
                copy.start()
            return
        if entry in ("yout", "g"):
            for d in range(3):
                out_copy(int(entry == "g"), d).start()
            return
        kind, ch = entry[:-1], int(entry[-1])
        way = WAY_OUT[ch]
        if kind == "ay":
            for zz in range(nz):
                ay(ch, zz).start()
        elif kind == "az":
            for j in range(2 if WAY_IN[ch] == "C" else 0):
                cx(ch, j).wait_recv()
            az_start(ch)
        elif kind == "zx":
            bx(ch, 0).start()
        elif kind in ("zt", "yx"):
            bx(ch, 1).start()
        elif kind in ("zy", "xy"):
            by(ch).start()
        elif kind in ("c0", "c1"):
            ac(ch, int(kind == "c1")).start()
        elif kind == "o1":
            dv[ch, t2] = add(dv[ch, t2], rc[ch, 0])
            ya(ch).start()
        elif kind == "ot":
            dv[ch, t2] = add(dv[ch, t2], rc[ch, 0])
            if way == "B":
                xb(ch, 0).start()
            else:
                zc_start(ch, 0)
        elif kind == "oo":
            dv[ch, t] = add(dv[ch, t], rc[ch, 1])
            if way == "C":
                zc_start(ch, 1)
            elif ch < 2:
                for d in range(nz):
                    xp1(ch, d).start()
            else:
                xb(ch, 1).start()
        elif kind == "o2" and way == "A":
            value = dv[ch, t].astype(F32) + rc[ch, 1].astype(F32)
            dv[ch, t] = (value + ry[a_slot[ch]].astype(F32)).astype(BF16)
            xa(ch).start()
        elif kind == "o2" and way == "B":
            dv[ch, t2, :, x] = add(dv[ch, t2, :, x], rx[b_slot[ch], 0])
            yb2(ch).start()
        elif kind == "o2":
            for j, tt in enumerate((t2, t)):
                value = dv[ch, tt, z].astype(F32)
                for d in range(nz - 1):
                    value = value + rzc[c_slot[ch], d, j].astype(F32)
                dv[ch, tt, z] = value.astype(BF16)
                xc(ch, j).start()
        elif kind == "o3" and way == "C":
            for j, tt in enumerate((t2, t)):
                dv[ch, tt, z, x] = add(dv[ch, tt, z, x], rxc[c_slot[ch], j])
            yc(ch).start()
        elif kind == "o3" and ch < 2:
            for d in range(nz):
                zz = piece_of(d)
                xp1(ch, d).wait_recv()
                value = dv[ch, t, zz, x].astype(F32) + rx[b_slot[ch], 1, zz].astype(F32)
                dv[ch, t, zz, x] = (value + r3[ch, zz].astype(F32)).astype(BF16)
                if d < nz - 1:
                    zr_start(ch, d)
        else:
            assert kind == "o3"
            value = dv[ch, t, :, x].astype(F32) + r3[ch].astype(F32)
            if way == "B":
                value = value + rx[b_slot[ch], 1].astype(F32)
            dv[ch, t, :, x] = value.astype(BF16)
            for k in range(nz - 1):
                zr_start(ch, k)

    def last(ch):
        if WAY_OUT[ch] == "C":
            yc(ch).wait_recv()
            fin[ch] = dv[ch, t, z, x].astype(F32) + rxc[c_slot[ch], 2].astype(F32)
            return
        value = dv[ch, t, z, x].astype(F32)
        for d in range(nz - 1):
            zr(ch, d).wait_recv()
            value = value + rz[ch, d].astype(F32)
        fin[ch] = value

    def run(slot):
        for entry in PLAN.get(slot, ()):
            act(entry)

    def run_at(index, pattern, count):
        for i in range(count):
            if PLAN.get(pattern % i):

                @pl.when(index == i)
                def _(i=i):
                    run(pattern % i)

    def use_at(index, pattern, count, start=0):
        for i in range(start, count):
            if any(first_use[n] == pattern % i for n in waits_of(pattern % i)):

                @pl.when(index == i)
                def _(i=i):
                    arrive(pattern % i)

    n_live = live[0] - t * slots
    small[...] = jnp.zeros_like(small)
    own_tok.wait()
    run("h0")
    for ch in (1, 0):
        for k in range(nz - 1):
            zz, _ = far_first(nz - 2 - k)
            az_from(ch, zz).wait_recv()
            ax(ch, zz).start()
            if ch == 1:
                ay(ch, zz).start()
    for ch in early:
        if ch not in first:
            cross(ch)
    run("h1")
    for copy in tok_all(2):
        copy.wait_recv()
    for tt in range(nt):
        bias_of(tt)
    for d in range(3):
        tok_copy(0, d).wait_recv()
    spread(xg, xp)
    gain1, shift1 = wide(0), wide(1)

    def start(i, at, carry):
        normed, rstd = norm(xp[at, :])
        n1[at, :] = normed
        r1[at, :] = rstd
        h = normed * gain1 + shift1
        h1[at, :] = h.astype(BF16)
        h1t[:, at] = h.T.astype(BF16)
        return carry

    each(start)
    run("h2")
    arrive("use_a0")
    ac(1, 0).start()
    ac(0, 0).start()
    run("h3")
    lane_head = lax.broadcasted_iota(jnp.int32, (PAD, LANES), 1) // HDIM
    ones = [(lane_head == h).astype(F32).astype(BF16) for h in range(heads)]

    def stack(value):
        return jnp.concatenate([value * ones[h] for h in range(heads)], axis=0)

    def pick(value):
        out = value[0:PAD]
        for h in range(1, heads):
            out = jnp.where(lane_head == h, value[h * PAD : (h + 1) * PAD], out)
        return out

    acc[...] = jnp.zeros_like(acc)

    def attend(i, carry):
        tt = group(i)

        use_at(i, "use_a%d", nt, 1)
        q = (nn(h1[...], weight(0, tt, 0, LANES)) + vg[tt, 2:3, :]) * SCALE
        qs[tt] = q.astype(BF16)
        kv = nn(h1[...], weight(1, tt))
        kvs[tt, :, :LANES] = kv[:, :LANES].astype(BF16)
        kvs[tt, :, LANES:] = (kv[:, LANES:] + vg[tt, 3:4, :]).astype(BF16)

        def window(w):
            at = pl.ds(pl.multiple_of(w * PAD, PAD), PAD)
            s = nt_dot(kvs[tt, at, :LANES], stack(qs[tt, at, :])) + rg[tt] + mask[w]
            e = jnp.exp(s - jnp.max(s, axis=0, keepdims=True))
            p = e / rowsum(e)
            probs[tt, w] = p
            att[tt, at, :] = pick(tn_dot(p.astype(BF16), kvs[tt, at, LANES:])).astype(BF16)

        def four(hh, carry):
            for j in range(slots // 2):
                window(hh * (slots // 2) + j)

            @pl.when(hh == 0)
            def _():
                run_at(i, "a%df", nt)

            return carry

        lax.fori_loop(0, 2, four, 0)
        acc[...] += nt_dot(att[tt], weight(0, tt, LANES, LANES))
        run_at(i, "a%ds", nt)
        return carry

    lax.fori_loop(0, nt, attend, 0)
    own_cot.wait()
    for d in range(3):
        tok_copy(1, d).wait_recv()
    spread(cg, gy)
    b_out, gain2, shift2 = wide(4), wide(5), wide(6)

    def live_rows(i):
        slot = lax.div(i * half + lax.broadcasted_iota(jnp.int32, (half, 1), 0), PAD)
        return slot < n_live

    def middle(i, at, carry):
        x1 = xp[at, :] + acc[at, :] + b_out
        xp[at, :] = x1
        normed, rstd = norm(x1)
        n2[at, :] = normed
        r2[at, :] = rstd
        h = normed * gain2 + shift2
        low[at, :] = h.astype(BF16)
        h2t[:, at] = h.T.astype(BF16)
        g = jnp.where(live_rows(i), gy[at, :], 0.0)
        gy[at, :] = g
        gkv[at, :] = g.astype(BF16)
        gyt[:, at] = g.T.astype(BF16)
        return carry

    each(middle)
    run("mid")
    acc[...] = jnp.zeros_like(acc)
    acc2[...] = jnp.zeros_like(acc2)
    def mlp(k, carry):
        s, i = lax.div(k, nt), lax.rem(k, nt)
        turn_at = MLP_ORDER[nt - 1]
        for j in range(nt - 1):
            turn_at = jnp.where(i == j, MLP_ORDER[j], turn_at)
        tt = group(turn_at)
        up, down = 2 + s, 4 + s
        use_at(k, "use_m%d", 2 * nt)

        bias = vg[tt, pl.ds(8 + 2 * s, 2), :]
        bias = jnp.concatenate([bias[0:1], bias[1:2]], axis=1)
        hidden = nn(low[...], weight(up, tt)) + bias
        act, slope = gelu_pair(hidden)
        act_low = act.astype(BF16)
        acc[...] += nt_dot(act_low, weight(down, tt))
        put_grad(down, tt, nn(gyt[...], act_low))
        grad = nn(gkv[...], weight(down, tt)) * slope
        total = rowsum(grad)
        small[tt, pl.ds(8 + 2 * s, 1), :] = total[:, :LANES]
        small[tt, pl.ds(9 + 2 * s, 1), :] = total[:, LANES:]
        grad_low = grad.astype(BF16)
        put_grad(up, tt, nn(h2t[...], grad_low))
        acc2[...] += nt_dot(grad_low, weight(up, tt))

        for when, j in ((MLP_ORDER.index(1), 1), (MLP_ORDER.index(3), 0)):

            @pl.when(i == when)
            def _(j=j):
                kc(up, j).start()
                kc(down, j).start()

        run_at(k, "m%d", 2 * nt)
        return carry

    lax.fori_loop(0, 2 * nt, mlp, 0)
    b_down = wide(7)
    zero_row = jnp.zeros((1, C), F32)

    def turn(i, at, carry):
        xp[at, :] = jnp.where(live_rows(i), xp[at, :] + acc[at, :] + b_down, 0.0)
        e, normed, g = acc2[at, :], n2[at, :], gy[at, :]
        gx = norm_back(e * gain2, normed, r2[at, :]) + g
        gy[at, :] = gx
        low[at, :] = gx.astype(BF16)
        h2t[:, at] = gx.T.astype(BF16)
        sums = (rowsum(e * normed), rowsum(e), rowsum(gx), rowsum(g))
        return tuple(p + q for p, q in zip(carry, sums))

    sums = each(turn, (zero_row,) * 4)
    put_small(5, sums[0])
    put_small(6, sums[1])
    put_small(4, sums[2])
    put_small(7, sums[3])
    gather(xp, yb)
    own_y = pltpu.make_async_copy(yb.at[t], y_all.at[t], loc.at[2])
    own_y.start()
    run("turn")
    acc[...] = jnp.zeros_like(acc)

    def back(i, carry):
        tt = group(3 - i)
        gatt[...] = nn(low[...], weight(0, tt, LANES, LANES)).astype(BF16)
        pairs[...] = jnp.zeros_like(pairs)

        def window(w):
            at = pl.ds(pl.multiple_of(w * PAD, PAD), PAD)
            q4, g4 = stack(qs[tt, at, :]), stack(gatt[at, :])
            p = probs[tt, w]
            dp = nt_dot(kvs[tt, at, LANES:], g4)
            ds = p * (dp - rowsum(p * dp))
            ds_low = ds.astype(BF16)
            gkv[at, :LANES] = nn(ds_low, q4).astype(BF16)
            gkv[at, LANES:CW] = nn(p.astype(BF16), g4).astype(BF16)
            gq[at, :] = pick(tn_dot(ds_low, kvs[tt, at, :LANES])).astype(BF16)
            return ds_low.astype(F32)

        def four(hh, carry):
            total = window(hh * (slots // 2))
            for j in range(1, slots // 2):
                total = total + window(hh * (slots // 2) + j)
            pairs[...] += total

            @pl.when(hh == 0)
            def _():
                run_at(i, "b%df", nt)

            return carry

        lax.fori_loop(0, 2, four, 0)
        gk_gv = gkv[:, :CW]
        put_grad(1, tt, nn(h1t[...], gk_gv))

        left = nn(h1t[...], gq[...]) * SCALE
        put_grad(0, tt, jnp.concatenate([left, nn(h2t[...], att[tt])], axis=1))

        @pl.when(i == 0)
        def _():
            kc(1, 0).start()
            kc(0, 0).start()

        @pl.when(i == 2)
        def _():
            kc(1, 1).start()
            kc(0, 1).start()

        run_at(i, "b%dd", nt)
        small[tt, 2:3, :] = rowsum(gq[...].astype(F32)) * SCALE
        small[tt, 3:4, :] = rowsum(gkv[:, LANES:CW].astype(F32))
        grad_q = nt_dot(gq[...], weight(0, tt, 0, LANES)) * SCALE
        acc[...] += grad_q + nt_dot(gk_gv, weight(1, tt))
        for h in range(heads):
            lanes = h // 2 * LANES
            source = pairs[:, lanes : lanes + LANES]
            for q in range(TPAD // LANES):
                where = inv[:, q * LANES : (q + 1) * LANES]
                value = take(source, jnp.maximum(where, 0) + h % 2 * PAD)
                value = jnp.where(where >= 0, value, 0.0)
                small[tt, pl.ds(12 + 2 * h + q, 1), :] = rowsum(value)

        run_at(i, "b%ds", nt)
        return carry

    lax.fori_loop(0, nt, back, 0)

    def finish(i, at, carry):
        e, normed = acc[at, :], n1[at, :]
        xp[at, :] = norm_back(e * gain1, normed, r1[at, :]) + gy[at, :]
        sums = (rowsum(e * normed), rowsum(e))
        return tuple(p + q for p, q in zip(carry, sums))

    sums = each(finish, (zero_row,) * 2)
    put_small(0, sums[0])
    put_small(1, sums[1])
    for d in range(3):
        small_t(d).start()
    gather(xp, gb)
    own_g = pltpu.make_async_copy(gb.at[t], g_all.at[t], loc.at[3])
    own_g.start()
    run("t1")
    run("t2")
    for d in range(3):
        small_t(d).wait_recv()
    zb[z] = small[t] + scr[0] + (scr[1] + scr[2])
    for d in range(nz - 1):
        small_z(d).start()
    run("t3")
    for d in range(nz - 1):
        small_z(d).wait_recv()
    value = zb[0]
    for zz in range(1, nz):
        value = value + zb[zz]
    sx[...] = value
    small_x().start()
    run("t4")
    run("t5")
    for ch in (2, 4, 3, 5, 1, 0):
        last(ch)
    small_x().wait_recv()
    tot[...] = sx[...] + syr[...]
    for i in range(2):
        for d in range(3):
            out_copy(i, d).wait_recv()
    sent = [tok_copy(i, d) for i in range(3) for d in range(3)]
    sent += [out_copy(i, d) for i in range(2) for d in range(3)]
    for ch in range(NCH):
        sent += [ac(ch, j) for j in range(2)] + [kc(ch, j) for j in range(2)]
        if ch < 2:
            sent += [ax(ch, zz) for zz in range(nz)] + [ay(ch, zz) for zz in range(nz)]
            sent += [az(ch, d) for d in range(nz - 1)] + ([bx(1, 1)] if ch else [])
        else:
            sent += az_all(ch)
            sent += [cy(ch)] if WAY_IN[ch] in "CE" else [by(ch)]
            if WAY_IN[ch] == "C":
                sent += [cx(ch, 0), cx(ch, 1)]
            else:
                sent += [bx(ch, 0)] + ([] if WAY_IN[ch] == "A" else [bx(ch, 1)])
        if WAY_OUT[ch] == "C":
            sent += [zc(ch, d, j) for d in range(nz - 1) for j in range(2)]
            sent += [xc(ch, 0), xc(ch, 1), yc(ch)]
            continue
        sent += [zr(ch, d) for d in range(nz - 1)]
        if WAY_OUT[ch] == "A":
            sent += [ya(ch), xa(ch)]
        else:
            sent += [xb(ch, 0), yb2(ch)]
            sent += [xp1(ch, d) for d in range(nz)] if ch < 2 else [xb(ch, 1)]
    sent += [small_t(d) for d in range(3)] + [small_x()]
    sent += [small_z(d) for d in range(nz - 1)]
    for copy in sent:
        copy.wait_send()
    own_y.wait()
    own_g.wait()


def block_call(nt, nz, slots, *args):
    tok, deep, heads = args[1], args[3].shape[0], args[18].shape[0]
    real = tok.shape[1]
    rows, wide = slots * PAD, heads * PAD
    piece = (nz, 2, deep, CW)
    row = (nt, real, LANES)

    def vm(shape, kind=BF16):
        return pltpu.VMEM(shape, kind)

    def pair(*shape):
        return [DMA(shape), DMA(shape)]

    small = (SROWS, LANES)
    n_c = max(1, WAY_OUT.count("C"))
    return pl.pallas_call(
        functools.partial(block, nt, nz, slots),
        name="block",
        out_shape=(
            jax.ShapeDtypeStruct(row, BF16),
            jax.ShapeDtypeStruct(row, BF16),
            jax.ShapeDtypeStruct((NCH, deep, CW), F32),
            jax.ShapeDtypeStruct(small, F32),
        ),
        in_specs=[SM] + [ANY] * 20,
        out_specs=(ANY, ANY, VM, VM),
        scratch_shapes=[vm(arg.shape, arg.dtype) for arg in args[9:]]
        + [
            vm(row),
            vm(row),
            vm((NCH, nt) + piece),
            vm((nt,) + small, F32),
            vm((nt, PAD, wide), F32),
            vm((NCH, nt) + piece),
            vm((NCH, 2) + piece),
            vm((max(1, WAY_OUT.count("A")),) + piece),
            vm((WAY_OUT.count("B"), 2, nz, deep, CW)),
            vm((NCH, nz, deep, CW)),
            vm((NCH, nz - 1, deep, CW)),
            vm((n_c, nz - 1, 2, 2, deep, CW)),
            vm((n_c, 3, deep, CW)),
            vm((3,) + small, F32),
            vm(small, F32),
            vm(small, F32),
            vm((nz,) + small, F32),
            vm((nt,) + small, F32),
            vm(row),
            vm(row),
            vm((LANES, LANES), F32),
            vm((slots, PAD, wide), F32),
            vm((PAD, TPAD), jnp.int32),
            vm((real, C), F32),
            vm((rows, C), F32),
            vm((rows, C), F32),
            vm((rows, C)),
            vm((C, rows)),
            vm((C, rows)),
            vm((C, rows)),
            vm((nt, rows, LANES)),
            vm((nt, rows, CW)),
            vm((nt, slots, PAD, wide), F32),
            vm((nt, rows, LANES)),
            vm((rows, C), F32),
            vm((rows, C), F32),
            vm((rows, C), F32),
            vm((rows, 1), F32),
            vm((rows, C), F32),
            vm((rows, 1), F32),
            vm((rows, C)),
            vm((rows, C)),
            vm((rows, LANES)),
            vm((rows, LANES)),
            vm((PAD, wide), F32),
            DMA((4,)),
            DMA((20,)),
        ]
        + pair(3, 3)
        + pair(2, 3)
        + pair(NCH, nz - 1, 2)
        + pair(2, nz)
        + pair(2, nz)
        + pair(NCH, 2)
        + pair(NCH, 2)
        + pair(NCH)
        + pair(2, nz)
        + pair(n_c, nz - 1, 2)
        + pair(n_c, 3)
        + pair(NCH, 2)
        + pair(NCH, 2)
        + pair(NCH)
        + pair(NCH, nz - 1)
        + pair(3 + nz),
        compiler_params=pltpu.CompilerParams(
            collective_id=0, has_side_effects=True, vmem_limit_bytes=60 * 2**20
        ),
    )(*args)


def spell(n, *refs):
    ins, outs, refs = refs[:4], refs[4 : 4 + n], refs[4 + n :]
    (y_in, g_in, fin, tot), refs = refs[:4], refs[4:]
    held, (get, put) = refs[:n], refs[n:]
    steps = ins[0].shape[0]
    loads = [pltpu.make_async_copy(ins[2], fin, get.at[0])]
    loads.append(pltpu.make_async_copy(ins[3], tot, get.at[1]))
    for i in range(steps):
        for j, ref in enumerate((y_in, g_in)):
            loads.append(
                pltpu.make_async_copy(ins[j].at[i], ref.at[i], get.at[2 + 2 * i + j])
            )
    for copy in loads:
        copy.start()
    loads[0].wait()
    loads[1].wait()
    spell_rest(fin, tot, *held[2:])
    stores = [pltpu.make_async_copy(held[k], outs[k], put.at[k]) for k in range(2, n)]
    for copy in stores:
        copy.start()
    for i in range(steps):
        for j, ref in enumerate((y_in, g_in)):
            loads[2 + 2 * i + j].wait()
            held[j][i] = ref[i].astype(F32)
            copy = pltpu.make_async_copy(held[j].at[i], outs[j].at[i], put.at[n + 2 * i + j])
            copy.start()
            stores.append(copy)
    for copy in stores:
        copy.wait()


def spell_rest(fin, tot, *outs):
    (
        d_g1, d_s1, d_wq, d_wk, d_wv, d_bq, d_bv, d_wo, d_bo, d_g2, d_s2, d_wh, d_bh,
        d_wd, d_bd, d_tab,
    ) = outs
    d_wq[...] = fin[0, :, :LANES]
    d_wk[...] = fin[1, :, :LANES]
    d_wv[...] = fin[1, :, LANES:]
    d_wo[...] = fin[0, :, LANES:]
    for s in range(2):
        d_wh[:, s * CW : (s + 1) * CW] = fin[2 + s]
        d_wd[:, s * CW : (s + 1) * CW] = fin[4 + s]
    for i, ref in enumerate((d_g1, d_s1, d_bq, d_bv, d_bo, d_g2, d_s2, d_bd)):
        ref[...] = tot[i : i + 1, :]
    d_bh[...] = tot[8:12, :]
    for h in range(d_tab.shape[0]):
        d_tab[h : h + 1, :LANES] = tot[12 + 2 * h : 13 + 2 * h]
        d_tab[h : h + 1, LANES:] = tot[13 + 2 * h : 14 + 2 * h, : TABLE - LANES]


def spell_call(outs, *args):
    n, steps = len(outs), args[0].shape[0]
    held = [pltpu.VMEM(v.shape, v.dtype) for v in args + outs]
    return pl.pallas_call(
        functools.partial(spell, n),
        name="spell",
        out_shape=outs,
        in_specs=[ANY] * 4,
        out_specs=(ANY,) * n,
        scratch_shapes=held + [DMA((2 + 2 * steps,)), DMA((n + 2 * steps,))],
        compiler_params=pltpu.CompilerParams(vmem_limit_bytes=60 * 2**20),
    )(*args)


def per_device(
    nt, na, tokens, gain_one, shift_one, w_query, w_key, w_value, b_query, b_value, w_out, b_out,
    gain_two, shift_two, w_hidden, b_hidden, w_down, b_down, bias_table, rel_index, region,
    win_count, cotangent,
):
    slots = region.shape[0] // nt
    cut = (nt, slots * WT, LANES)
    vectors = [gain_one, shift_one, b_query, b_value, b_out, gain_two, shift_two, b_down]
    parts = block_call(
        nt, na // 2, slots,
        win_count, tokens.reshape(cut), cotangent.reshape(cut),
        w_query, w_key, w_value, w_out.T, w_hidden, w_down.T,
        *[v.reshape(1, LANES) for v in vectors],
        b_hidden.reshape(-1, LANES), bias_table.T, rel_index, region,
    )

    def out(like, shape=None):
        return jax.ShapeDtypeStruct(shape or like.shape, F32)

    one = (1, LANES)
    shapes = (
        out(tokens, cut), out(tokens, cut), out(gain_one, one), out(gain_one, one), out(w_query),
        out(w_key), out(w_value), out(b_query, one), out(b_value, one), out(w_out, w_out.shape[::-1]),
        out(b_out, one), out(gain_two, one), out(shift_two, one), out(w_hidden),
        out(b_hidden, (b_hidden.shape[0] // LANES, LANES)), out(w_down, w_down.shape[::-1]),
        out(b_down, one), out(bias_table, bias_table.shape[::-1]),
    )
    likes = (
        tokens, tokens, gain_one, gain_one, w_query, w_key, w_value, b_query, b_value, w_out,
        b_out, gain_two, shift_two, w_hidden, b_hidden, w_down, b_down, bias_table,
    )
    values = spell_call(shapes, *parts)
    turned = (9, 15, 17)
    return tuple(
        v.T if i in turned else v.reshape(like.shape)
        for i, (v, like) in enumerate(zip(values, likes))
    )


def solution(mesh):
    return jax.shard_map(
        functools.partial(per_device, mesh.shape["ta"], mesh.shape["wa"]),
        mesh=mesh,
        in_specs=(
            P("wa", "ta"),
            P("ta"),
            P("ta"),
            P("wa", "ta"),
            P("wa", "ta"),
            P("wa", "ta"),
            P("ta"),
            P("ta"),
            P("ta", "wa"),
            P("ta"),
            P("ta"),
            P("ta"),
            P("wa", "ta"),
            P("ta"),
            P("ta", "wa"),
            P("ta"),
            P(None, "ta"),
            P(),
            P("wa", None),
            P("wa"),
            P("wa", "ta"),
        ),
        out_specs=(
            P("wa", "ta"),
            P("wa", "ta"),
            P("ta"),
            P("ta"),
            P("wa", "ta"),
            P("wa", "ta"),
            P("wa", "ta"),
            P("ta"),
            P("ta"),
            P("ta", "wa"),
            P("ta"),
            P("ta"),
            P("ta"),
            P("wa", "ta"),
            P("ta"),
            P("ta", "wa"),
            P("ta"),
            P(None, "ta"),
        ),
        check_vma=False,
    )
```

```python
import functools

import jax
import jax.numpy as jnp
from jax import lax
from jax.experimental import pallas as pl
from jax.experimental.pallas import tpu as pltpu
from jax.sharding import PartitionSpec as P

C = 512
HDIM = 32
WT = 49
PAD = 64
TABLE = 169
TPAD = 256
NCH = 6
CW = 256
LANES = 128
SROWS = 24
SCALE = HDIM ** (-0.5)
EPS = 1e-05
F32 = jnp.float32
BF16 = jnp.bfloat16
MESH = pl.DeviceIdType.MESH
ANY = pl.BlockSpec(memory_space=pl.ANY)
VM = pl.BlockSpec(memory_space=pltpu.VMEM)
SM = pl.BlockSpec(memory_space=pltpu.SMEM)
DMA = pltpu.SemaphoreType.DMA


WAY_IN = ("A", "B", "A", "B", "E", "C")
WAY_OUT = ("B", "B", "B", "C", "A", "B")
MLP_ORDER = (0, 1, 3, 2)
PLAN = {
    "h0": ("az2",),
    "h1": ("az4", "yx1",),
    "h2": ("zx2", "ay0",),
    "h3": ("az3",),
    "a0f": ("c11", "cot",),
    "a1f": ("zt4", "az5", "xy2", "zx4",),
    "a1s": ("c02", "zy3", "c10",),
    "a3f": ("zx3",),
    "a3s": ("c04",),
    "m1": ("yx3", "c03",),
    "m2": ("c15",),
    "m3": ("c05",),
    "m4": ("o14", "c13", "ot2", "oo2",),
    "m7": ("o22", "oo3", "oo5",),
    "turn": ("ot3",),
    "b0f": ("ot5", "yout",),
    "b0d": ("o24",),
    "b0s": ("o32",),
    "b1d": ("ot1", "o25", "ot0",),
    "b2d": ("o34",),
    "b3f": ("o21",),
    "b3d": ("oo1", "oo0",),
    "b3s": ("o35",),
    "t1": ("o20", "o23",),
    "t2": ("g",),
    "t3": ("o31", "o30",),
    "t4": ("o33",),
    "m0": ("c12", "c14",),
}


def plan_order(sched):
    out = list(sched.get("h0", ())) + list(sched.get("h1", ()))
    out += list(sched.get("h2", ())) + ["use_a0"]
    out += sched.get("h3", ())
    for i in range(4):
        out += ([f"use_a{i}"] if i else []) + list(sched.get(f"a{i}f", ()))
        out += sched.get(f"a{i}s", ())
    out += list(sched.get("mid", ()))
    for k in range(8):
        out += [f"use_m{k}"] + list(sched.get(f"m{k}", ()))
    out += sched.get("turn", ())
    for i in range(4):
        for part in "fds":
            out += sched.get(f"b{i}{part}", ())
    for i in range(1, 6):
        out += sched.get(f"t{i}", ())
    return out + ["end"]


def flip(bit, by):
    return bit + by - 2 * bit * by


def add(left, right):
    return (left.astype(F32) + right.astype(F32)).astype(BF16)


def nn(left, right):
    return jnp.dot(left, right, preferred_element_type=F32)


def nt_dot(left, right):
    return lax.dot_general(left, right, (((1,), (1,)), ((), ())), preferred_element_type=F32)


def tn_dot(left, right):
    return lax.dot_general(left, right, (((0,), (0,)), ((), ())), preferred_element_type=F32)


def norm(value):
    mean = jnp.mean(value, axis=1, keepdims=True)
    spread = jnp.mean(value * value, axis=1, keepdims=True) - mean * mean
    rstd = lax.rsqrt(spread + EPS)
    return (value - mean) * rstd, rstd


def norm_back(scaled, normed, rstd):
    first = jnp.mean(scaled, axis=1, keepdims=True)
    second = jnp.mean(scaled * normed, axis=1, keepdims=True)
    return rstd * (scaled - first - normed * second)


def gelu_pair(u):
    cdf = 0.5 + 0.5 * lax.erf(u * (0.5**0.5))
    pdf = jnp.exp(-0.5 * u * u) * ((2.0 * jnp.pi) ** -0.5)
    return u * cdf, cdf + u * pdf


def rowsum(value):
    return jnp.sum(value, axis=0, keepdims=True)


def arrival_table(nz):
    keys = [("kc", ch, j) for ch in range(NCH) for j in range(2)]
    keys += [("ac", ch, j) for ch in range(NCH) for j in range(2)]
    keys += [("az", ch, d) for ch in range(2) for d in range(nz - 1)]
    keys += [("tok", i) for i in range(3)] + [("out", i) for i in range(2)]
    keys += [(kind, ch) for kind in ("ax", "ay") for ch in range(2)]
    keys += [("bx", 1, 1), ("st",), ("sz",), ("sx",)]
    for ch in range(2, NCH):
        keys += [("az", ch), ("by", ch)]
        if WAY_IN[ch] == "C":
            keys.append(("cx", ch))
        else:
            keys += [("bx", ch, j) for j in range(1 if WAY_IN[ch] == "A" else 2)]
    for ch in range(NCH):
        if WAY_OUT[ch] == "C":
            keys += [("zc", ch), ("xc", ch), ("yc", ch)]
            continue
        keys += [("zr", ch), ("q", ch), ("p", ch, 0)]
        if WAY_OUT[ch] == "B":
            keys += [("px", ch, d) for d in range(nz)] if ch < 2 else [("p", ch, 1)]
    return {key: i for i, key in enumerate(keys)}


def send_table(nt, nz):
    whole = {("kc", ch, j): 2 * nz for ch in range(NCH) for j in range(2)}
    whole.update({("ac", ch, j): 2 * nz for ch in range(NCH) for j in range(2)})
    sends = {}
    for ch in range(2):
        sends.update({("az", ch, d, 0): 1 for d in range(nz - 1)})
        sends.update({("ax", ch, i): 1 for i in range(nz)})
        sends.update({("ay", ch, i): 2 - ch for i in range(nz)})
        sends.update({("px", ch, d): 1 for d in range(nz)})
    sends["bx", 1, 1] = nz
    for ch in range(2, NCH):
        way = WAY_IN[ch]
        both = 2 if way in "CE" else 1
        size = 2 if way == "C" else 1
        sends.update({("az", ch, d, j): size for d in range(nz - 1) for j in range(both)})
        sends["by", ch] = {"A": 2 * nz, "B": nz, "C": 1, "E": 1}[way]
        sends.update({("bx", ch, j): 1 if way == "C" else nz for j in range(1 + (way != "A"))})
    for ch in range(NCH):
        way = WAY_OUT[ch]
        if way == "C":
            sends.update({("zc", ch, d, j): 2 for d in range(nz - 1) for j in range(2)})
            sends.update({("xc", ch, j): 1 for j in range(3)})
            continue
        sends.update({("zr", ch, d): 1 for d in range(nz - 1)})
        sends["q", ch] = nz
        sends["p", ch, 0] = 2 * nz if way == "A" else nz
        if way == "B" and ch > 1:
            sends["p", ch, 1] = nz
    order = sorted(sends, key=lambda key: -sends[key])
    left = sum(sends.values())
    groups, totals = {key: 0 for key in whole}, [sum(whole.values())]
    for unit, most in ((2 * nz * nt, NCH), (2 * nz, nt), (2, nz), (1, 1)):
        goal = unit * min(most, left // unit)
        if goal:
            total = 0
            while total < goal:
                key = order.pop(0)
                total += sends[key]
                groups[key] = len(totals)
            assert total == goal
            totals.append(total)
            left -= total
    assert not order
    return groups, totals


def block(nt, nz, slots, *refs):
    live, tok, cot, wq, wk, wv, wo, wh, wd = refs[:9]
    outside, refs = refs[9:21], refs[21:]
    inside, refs = refs[4:16], refs[:4] + refs[16:]
    g1, s1, bq, bv, bo, g2, s2, bd, bh, tab, rel, reg = inside
    (
        y_all, g_all, fin, tot,
        xg, cg, gw, vg, rg, dv, rc, ry, rx, r3, rz, rzc, rxc, scr, syr, sx, zb, small, yb, gb, square, mask, inv,
        xs, xp, gy, h1, h1t, h2t, gyt, qs, kvs, probs, att, acc, acc2, n1, r1, n2, r2, low, gkv, gq, gatt,
        pairs,
        loc, ld, rs, ss,
    ) = refs
    heads = LANES // HDIM
    rows = slots * PAD
    half = 2 * PAD
    nhalf = rows // half
    a, t = lax.axis_index("wa"), lax.axis_index("ta")
    x, z, c, y = lax.rem(a, 2), lax.div(a, 2), lax.rem(t, 2), lax.div(t, 2)

    def group(m):
        return 2 * flip(y, m // 2 if isinstance(m, int) else lax.div(m, 2)) + flip(
            c, m % 2 if isinstance(m, int) else lax.rem(m, 2)
        )

    t1, t2, t3 = group(1), group(2), group(3)
    xpeer, ypeer, cpeer = (z * 2 + (1 - x), t), (a, t2), (a, t1)
    zs = [(lax.rem(z + d, nz) * 2 + x, t) for d in range(1, nz)]
    ts = [(a, tt) for tt in (t1, t2, t3)]
    peers = zs + ts + [xpeer]
    barrier = pltpu.get_barrier_semaphore()
    for peer in peers:
        pl.semaphore_signal(barrier, inc=1, device_id=peer, device_id_type=MESH)

    arrival, (group_of, totals) = arrival_table(nz), send_table(nt, nz)

    def coming(*key):
        return rs.at[arrival[key]]

    def going(*key):
        return ss.at[group_of[key]]

    def blocks(n):
        for unit, ref in ((2 * nz * nt, gw), (2 * nz, gw.at[0]), (2, gw.at[0, 0])):
            if n % unit == 0:
                return ref.at[pl.ds(0, n // unit)]
        assert n == 1
        return gw.at[0, 0, 0, 0]

    def await_bytes(ref, sem):
        pltpu.make_async_copy(ref, ref, sem).wait()

    def far(src, dst, send, recv, peer):
        return pltpu.make_async_remote_copy(
            src_ref=src, dst_ref=dst, send_sem=send, recv_sem=recv, device_id=peer,
            device_id_type=MESH,
        )

    def tok_copy(i, d):
        src, dst = ((tok, xg), (cot, cg), (vg, vg))[i]
        peer = ts[d]
        src = src.at[peer[1]] if i < 2 else src.at[t]
        return far(src, dst.at[t], ss.at[len(totals) + i], coming("tok", i), peer)

    def out_copy(i, d):
        src, dst = ((yb, y_all), (gb, g_all))[i]
        peer = ts[d]
        return far(src.at[peer[1]], dst.at[t], ss.at[len(totals) + 3 + i], coming("out", i), peer)

    def az_await(ch):
        n = (nz - 1) * {"A": 1, "B": 1, "C": 4, "E": 2}[WAY_IN[ch]]
        size = n // (nz - 1)
        ref = rz.at[0] if size == 1 else rzc.at[0, :, :, 0] if size == 2 else rzc.at[0]
        await_bytes(ref, coming("az", ch))

    def az_from(ch, zz):
        d = lax.rem(z - zz + nz, nz) - 1
        await_bytes(gw.at[ch, t, z, x], rs.at[arrival["az", ch, 0] + d])

    def far_first(k):
        rising = k + jnp.where(z > k, 0, 1)
        falling = nz - 1 - k - jnp.where(z < nz - 1 - k, 0, 1)
        zz = jnp.where(2 * z < nz, falling, rising)
        return zz, lax.rem(zz - z + nz, nz) - 1

    def az_start(ch):
        for k in range(nz - 1):
            zz, d = far_first(k)
            for j in range(2 if WAY_IN[ch] in "CE" else 1):
                far_t = t2 if j else t
                ref = gw.at[ch, far_t, z] if WAY_IN[ch] == "C" else gw.at[ch, far_t, z, x]
                there = rs.at[arrival["az", ch, 0] + d] if ch < 2 else coming("az", ch)
                far(ref, ref, going("az", ch, k, j), there, (zz * 2 + x, t)).start()

    def zr_start(ch, k):
        zz, d = far_first(k)
        src = dv.at[ch, t, zz, x]
        far(src, rz.at[ch, d], going("zr", ch, k), coming("zr", ch), (zz * 2 + x, t)).start()

    def ax(ch, zz, i):
        ref = gw.at[ch, t, zz, x]
        return far(ref, ref, going("ax", ch, i), coming("ax", ch), xpeer)

    def ay(ch, zz, i):
        ref = gw.at[ch, t, zz] if ch == 0 else gw.at[ch, t, zz, x]
        return far(ref, ref, going("ay", ch, i), coming("ay", ch), ypeer)

    def bx(ch, j):
        ref = gw.at[ch, t2 if j else t, :, x]
        return far(ref, ref, going("bx", ch, j), coming("bx", ch, j), xpeer)

    def by(ch):
        ref = gw.at[ch, t] if WAY_IN[ch] == "A" else gw.at[ch, t, :, x]
        return far(ref, ref, going("by", ch), coming("by", ch), ypeer)

    def cy(ch):
        ref = gw.at[ch, t, z, x]
        return far(ref, ref, going("by", ch), coming("by", ch), ypeer)

    def cx(ch, j):
        ref = gw.at[ch, t2 if j else t, z, x]
        return far(ref, ref, going("bx", ch, j), coming("cx", ch), xpeer)

    def ac(ch, j):
        ref = gw.at[ch, t2 if j else t]
        return far(ref, ref, going("ac", ch, j), coming("ac", ch, j), cpeer)

    def kc(ch, j):
        return far(dv.at[ch, t1 if j else t3], rc.at[ch, j], ss.at[0], rs.at[ch * 2 + j], cpeer)

    a_slot = {ch: i for i, ch in enumerate(c for c in range(NCH) if WAY_OUT[c] == "A")}
    b_slot = {ch: i for i, ch in enumerate(c for c in range(NCH) if WAY_OUT[c] == "B")}
    c_slot = {ch: i for i, ch in enumerate(c for c in range(NCH) if WAY_OUT[c] == "C")}

    def ya(ch):
        return far(dv.at[ch, t2], ry.at[a_slot[ch]], going("p", ch, 0), coming("p", ch, 0), ypeer)

    def xa(ch):
        return far(dv.at[ch, t, :, 1 - x], r3.at[ch], going("q", ch), coming("q", ch), xpeer)

    def piece_of(d):
        return far_first(d)[0] if d < nz - 1 else z

    def xp1(ch, d):
        zz = piece_of(d)
        src, dst = dv.at[ch, t, zz, 1 - x], rx.at[b_slot[ch], 1, zz]
        return far(src, dst, going("px", ch, d), coming("px", ch, d), xpeer)

    def xb(ch, j):
        src = dv.at[ch, t if j else t2, :, 1 - x]
        return far(src, rx.at[b_slot[ch], j], going("p", ch, j), coming("p", ch, j), xpeer)

    def yb2(ch):
        return far(dv.at[ch, t2, :, x], r3.at[ch], going("q", ch), coming("q", ch), ypeer)

    def zc_start(ch, j):
        i = c_slot[ch]
        for k in range(nz - 1):
            zz, d = far_first(k)
            src, peer = dv.at[ch, t if j else t2, zz], (zz * 2 + x, t)
            far(src, rzc.at[i, d, j], going("zc", ch, k, j), coming("zc", ch), peer).start()

    def xc(ch, j):
        src, i = dv.at[ch, t if j else t2, z, 1 - x], c_slot[ch]
        return far(src, rxc.at[i, j], going("xc", ch, j), coming("xc", ch), xpeer)

    def yc(ch):
        i = c_slot[ch]
        return far(dv.at[ch, t2, z, x], rxc.at[i, 2], going("xc", ch, 2), coming("yc", ch), ypeer)

    def small_t(d):
        return far(small.at[ts[d][1]], scr.at[d], ss.at[len(totals) + 5], coming("st"), ts[d])

    def small_z(d):
        return far(zb.at[z], zb.at[z], ss.at[len(totals) + 6], coming("sz"), zs[d])

    def small_x():
        return far(sx, syr, ss.at[len(totals) + 7], coming("sx"), xpeer)

    def lanes(ch, i, size):
        return gw.at[ch, t, z, x, :, pl.ds(i * size, size)]

    loads = [(wq, lanes(0, 0, LANES), 0), (wo, lanes(0, 1, LANES), 0)]
    loads += [(wk, lanes(1, 0, LANES), 0), (wv, lanes(1, 1, LANES), 0)]
    for i in range(2):
        loads += [(wh.at[:, pl.ds(i * CW, CW)], gw.at[2 + i, t, z, x], 1)]
        loads += [(wd.at[:, pl.ds(i * CW, CW)], gw.at[4 + i, t, z, x], 1)]
    loads += [(src, dst, 2 + i) for i, (src, dst) in enumerate(zip(outside, inside))]
    for src, dst, i in loads:
        pltpu.make_async_copy(src, dst, ld.at[i]).start()
    await_bytes(gw.at[0, 0, 0], ld.at[0])
    await_bytes(gw.at[0, 0, pl.ds(0, 2)], ld.at[1])
    for src, dst, i in loads[8:]:
        pltpu.make_async_copy(src, dst, ld.at[i]).wait()
    for i, ref in enumerate((g1, s1, bq, bv, bo, g2, s2, bd)):
        vg[t, i : i + 1, :] = ref[...]
    vg[t, 8:12, :] = bh[...]
    for h in range(heads):
        vg[t, 12 + 2 * h : 13 + 2 * h, :] = tab[h : h + 1, :LANES]
        vg[t, 13 + 2 * h : 14 + 2 * h, : TABLE - LANES] = tab[h : h + 1, LANES:]
        vg[t, 13 + 2 * h : 14 + 2 * h, TABLE - LANES :] = jnp.zeros((1, TPAD - TABLE), F32)
    vg[t, 12 + 2 * heads :, :] = jnp.zeros((SROWS - 12 - 2 * heads, LANES), F32)
    pl.semaphore_wait(barrier, len(peers))
    own_tok = pltpu.make_async_copy(tok.at[t], xg.at[t], loc.at[0])
    own_cot = pltpu.make_async_copy(cot.at[t], cg.at[t], loc.at[1])
    own_tok.start()
    own_cot.start()
    early = [ch for ch in range(2, NCH) if WAY_IN[ch] in "CE"]
    first = [ch for ch in early if f"az{ch}" in PLAN.get("h0", ())]
    for ch in first:
        cy(ch).start()
    for d in range(3):
        tok_copy(2, d).start()
    az_start(1)
    ax(1, z, 0).start()
    ay(1, z, 0).start()
    az_start(0)
    ax(0, z, 0).start()
    for d in range(3):
        tok_copy(0, d).start()
    for ch in early:
        if ch not in first:
            cy(ch).start()
    square[...] = jnp.zeros_like(square)
    square[:WT, :WT] = rel[...].astype(F32)
    rel_t = square[...].T[:PAD, :PAD]
    pick_at = jnp.concatenate([rel_t, rel_t], axis=1).astype(jnp.int32)
    lane = lax.broadcasted_iota(jnp.int32, (PAD, LANES), 1)
    low_at, high_at = jnp.minimum(pick_at, LANES - 1), jnp.maximum(pick_at - LANES, 0)

    def take(value, at):
        return jnp.take_along_axis(value, at, axis=1, mode="promise_in_bounds")

    def entry(tt, h):
        first = jnp.broadcast_to(vg[tt, 12 + 2 * h : 13 + 2 * h, :], (PAD, LANES))
        second = jnp.broadcast_to(vg[tt, 13 + 2 * h : 14 + 2 * h, :], (PAD, LANES))
        return jnp.where(pick_at < LANES, take(first, low_at), take(second, high_at))

    def bias_of(tt):
        for q in range(heads // 2):
            rg[tt, :, q * LANES : (q + 1) * LANES] = jnp.where(
                lane < PAD, entry(tt, 2 * q), entry(tt, 2 * q + 1)
            )

    number = lax.broadcasted_iota(jnp.int32, (PAD, TPAD), 1).astype(F32)
    found = jnp.full((PAD, TPAD), -1.0, F32)
    for i in range(WT):
        found = jnp.where(rel_t[:, i : i + 1] == number, float(i), found)
    inv[...] = found.astype(jnp.int32)
    square[...] = jnp.zeros_like(square)
    mine = reg[pl.ds(pl.multiple_of(t * slots, slots), slots), :]
    square[:slots, :WT] = mine.astype(F32)
    reg_row = square[:slots, :PAD]
    reg_row = jnp.concatenate([reg_row] * heads, axis=1)
    reg_col = square[...].T[:PAD, :slots]
    real = lax.broadcasted_iota(jnp.int32, (PAD, heads * PAD), 0) < WT
    for w in range(slots):
        same = reg_col[:, w : w + 1] == reg_row[w : w + 1, :]
        mask[w] = jnp.where(real, jnp.where(same, 0.0, -100.0), -1e30)
    def cross(ch):
        cy(ch).wait_recv()
        if WAY_IN[ch] == "C":
            for j in range(2):
                cx(ch, j).start()

    for ch in first:
        cross(ch)

    def wide(i):
        return jnp.concatenate([vg[tt, i : i + 1, :] for tt in range(nt)], axis=1)

    def put_small(i, value):
        for tt in range(nt):
            small[tt, i : i + 1, :] = value[:, tt * LANES : (tt + 1) * LANES]

    def spread(source, target):
        for tt in range(nt):
            xs[:, tt * LANES : (tt + 1) * LANES] = source[tt].astype(F32)
        zero = jnp.zeros((PAD - WT, C), F32)
        for w in range(slots):
            target[w * PAD : w * PAD + WT, :] = xs[w * WT : (w + 1) * WT, :]
            target[w * PAD + WT : (w + 1) * PAD, :] = zero

    def gather(source, target):
        for w in range(slots):
            xs[w * WT : (w + 1) * WT, :] = source[w * PAD : w * PAD + WT, :]
        for tt in range(nt):
            target[tt] = xs[:, tt * LANES : (tt + 1) * LANES].astype(BF16)

    def each(body, init=0):
        def step(i, carry):
            return body(i, pl.ds(pl.multiple_of(i * half, half), half), carry)

        return lax.fori_loop(0, nhalf, step, init)

    def weight(ch, tt, start=0, size=CW):
        return gw[ch, tt, :, :, :, start : start + size].reshape(C, size)

    def put_grad(ch, tt, value):
        dv[ch, tt] = value.astype(BF16).reshape(dv.shape[2:])

    def tok_all(i):
        return [tok_copy(i, d) for d in range(3)]

    def await_tok(i):
        await_bytes((xg, cg, vg)[i].at[pl.ds(0, 3)], coming("tok", i))

    def await_name(name):
        kind, ch = name[:-1], int(name[-1])
        if kind == "x":
            await_bytes(r3.at[0], coming("ax", ch))
        elif kind == "ay":
            await_bytes(r3.at[0] if ch else gw.at[0, 0], coming("ay", ch))
        elif kind == "z":
            az_await(ch)
        elif kind in ("xo", "xt"):
            bx(ch, int(kind == "xt")).wait_recv()
        elif kind == "yo":
            by(ch).wait_recv()
        elif kind in ("k0", "k1"):
            ac(ch, int(kind == "k1")).wait_recv()
        elif kind in ("r0", "r1"):
            kc(ch, int(kind == "r1")).wait_recv()
        elif kind == "ya":
            ya(ch).wait_recv()
        elif kind == "xa":
            xa(ch).wait_recv()
        elif kind in ("xbt", "xbo"):
            xb(ch, int(kind == "xbo")).wait_recv()
        elif kind == "yb":
            yb2(ch).wait_recv()
        elif kind == "zc":
            await_bytes(rzc.at[0], coming("zc", ch))
        else:
            assert kind == "xc"
            await_bytes(gw.at[0, 0, 0], coming("xc", ch))

    def own_of(ch):
        return ("z%d" if WAY_IN[ch] == "C" else "xo%d") % ch

    def other_y_of(ch):
        return {"A": "yo%d", "B": "xt%d", "C": "z%d", "E": "xt%d"}[WAY_IN[ch]] % ch

    def waits_of(entry):
        fixed = {
            "use_a0": ("x1", "x0"), "use_a1": ("k01", "k00"), "use_a2": ("xt1", "ay0"),
            "use_a3": ("k11", "k10"), "yx1": ("ay1",), "c11": ("xt1",), "c10": ("ay0",),
            "ay0": ("x0",), "end": (), "cot": (), "yout": (), "g": (),
        }
        if entry in fixed:
            return fixed[entry]
        if entry.startswith("use_m"):
            k = int(entry[-1])
            chs, m = ((2, 4) if k < nt else (3, 5)), MLP_ORDER[k % nt]
            names = {0: own_of, 1: "k0{}".format, 2: other_y_of, 3: "k1{}".format}[m]
            return tuple(names(ch) for ch in chs)
        kind, ch = entry[:-1], int(entry[-1])
        way = WAY_OUT[ch]
        names = {
            "az": (), "zx": ("z",), "zy": ("z",), "zt": ("z",), "yx": ("yo",), "xy": ("xo",),
            "o1": ("r0",), "oo": ("r1",), "ot": ("r0",),
            "o2": {"A": ("ya", "r1"), "B": ("xbt",), "C": ("zc",)}[way],
            "o3": {"A": ("xa",), "B": ("yb",) if ch < 2 else ("xbo", "yb"), "C": ("xc",)}[way],
        }
        if kind == "c0":
            return (own_of(ch),)
        if kind == "c1":
            return (other_y_of(ch),)
        return tuple(f"{n}{ch}" for n in names[kind])

    first_use = {}
    for item in plan_order(PLAN):
        for name in waits_of(item):
            first_use.setdefault(name, item)

    def arrive(entry):
        for name in waits_of(entry):
            if first_use[name] == entry:
                await_name(name)

    def act(entry):
        arrive(entry)
        if entry == "cot":
            for copy in tok_all(1):
                copy.start()
            return
        if entry in ("yout", "g"):
            for d in range(3):
                out_copy(int(entry == "g"), d).start()
            return
        kind, ch = entry[:-1], int(entry[-1])
        way = WAY_OUT[ch]
        if kind == "ay":
            for zz in range(nz):
                ay(ch, zz, zz).start()
        elif kind == "az":
            if WAY_IN[ch] == "C":
                await_bytes(gw.at[0, 0, 0], coming("cx", ch))
            az_start(ch)
        elif kind == "zx":
            bx(ch, 0).start()
        elif kind in ("zt", "yx"):
            bx(ch, 1).start()
        elif kind in ("zy", "xy"):
            by(ch).start()
        elif kind in ("c0", "c1"):
            ac(ch, int(kind == "c1")).start()
        elif kind == "o1":
            dv[ch, t2] = add(dv[ch, t2], rc[ch, 0])
            ya(ch).start()
        elif kind == "ot":
            dv[ch, t2] = add(dv[ch, t2], rc[ch, 0])
            if way == "B":
                xb(ch, 0).start()
            else:
                zc_start(ch, 0)
        elif kind == "oo":
            dv[ch, t] = add(dv[ch, t], rc[ch, 1])
            if way == "C":
                zc_start(ch, 1)
            elif ch < 2:
                for d in range(nz):
                    xp1(ch, d).start()
            else:
                xb(ch, 1).start()
        elif kind == "o2" and way == "A":
            value = dv[ch, t].astype(F32) + rc[ch, 1].astype(F32)
            dv[ch, t] = (value + ry[a_slot[ch]].astype(F32)).astype(BF16)
            xa(ch).start()
        elif kind == "o2" and way == "B":
            dv[ch, t2, :, x] = add(dv[ch, t2, :, x], rx[b_slot[ch], 0])
            yb2(ch).start()
        elif kind == "o2":
            for j, tt in enumerate((t2, t)):
                value = dv[ch, tt, z].astype(F32)
                for d in range(nz - 1):
                    value = value + rzc[c_slot[ch], d, j].astype(F32)
                dv[ch, tt, z] = value.astype(BF16)
                xc(ch, j).start()
        elif kind == "o3" and way == "C":
            for j, tt in enumerate((t2, t)):
                dv[ch, tt, z, x] = add(dv[ch, tt, z, x], rxc[c_slot[ch], j])
            yc(ch).start()
        elif kind == "o3" and ch < 2:
            for d in range(nz):
                zz = piece_of(d)
                xp1(ch, d).wait_recv()
                value = dv[ch, t, zz, x].astype(F32) + rx[b_slot[ch], 1, zz].astype(F32)
                dv[ch, t, zz, x] = (value + r3[ch, zz].astype(F32)).astype(BF16)
                if d < nz - 1:
                    zr_start(ch, d)
        else:
            assert kind == "o3"
            value = dv[ch, t, :, x].astype(F32) + r3[ch].astype(F32)
            if way == "B":
                value = value + rx[b_slot[ch], 1].astype(F32)
            dv[ch, t, :, x] = value.astype(BF16)
            for k in range(nz - 1):
                zr_start(ch, k)

    def last(ch):
        if WAY_OUT[ch] == "C":
            yc(ch).wait_recv()
            fin[ch] = dv[ch, t, z, x].astype(F32) + rxc[c_slot[ch], 2].astype(F32)
            return
        value = dv[ch, t, z, x].astype(F32)
        await_bytes(rz.at[0], coming("zr", ch))
        for d in range(nz - 1):
            value = value + rz[ch, d].astype(F32)
        fin[ch] = value

    def run(slot):
        for entry in PLAN.get(slot, ()):
            act(entry)

    def run_at(index, pattern, count):
        for i in range(count):
            if PLAN.get(pattern % i):

                @pl.when(index == i)
                def _(i=i):
                    run(pattern % i)

    def use_at(index, pattern, count, start=0):
        for i in range(start, count):
            if any(first_use[n] == pattern % i for n in waits_of(pattern % i)):

                @pl.when(index == i)
                def _(i=i):
                    arrive(pattern % i)

    n_live = live[0] - t * slots
    small[...] = jnp.zeros_like(small)
    own_tok.wait()
    run("h0")
    for ch in (1, 0):
        for k in range(nz - 1):
            zz, _ = far_first(nz - 2 - k)
            az_from(ch, zz)
            ax(ch, zz, k + 1).start()
            if ch == 1:
                ay(ch, zz, k + 1).start()
    for ch in early:
        if ch not in first:
            cross(ch)
    run("h1")
    await_tok(2)
    for tt in range(nt):
        bias_of(tt)
    await_tok(0)
    spread(xg, xp)
    gain1, shift1 = wide(0), wide(1)

    def start(i, at, carry):
        normed, rstd = norm(xp[at, :])
        n1[at, :] = normed
        r1[at, :] = rstd
        h = normed * gain1 + shift1
        h1[at, :] = h.astype(BF16)
        h1t[:, at] = h.T.astype(BF16)
        return carry

    each(start)
    run("h2")
    arrive("use_a0")
    ac(1, 0).start()
    ac(0, 0).start()
    run("h3")
    lane_head = lax.broadcasted_iota(jnp.int32, (PAD, LANES), 1) // HDIM
    ones = [(lane_head == h).astype(F32).astype(BF16) for h in range(heads)]

    def stack(value):
        return jnp.concatenate([value * ones[h] for h in range(heads)], axis=0)

    def pick(value):
        out = value[0:PAD]
        for h in range(1, heads):
            out = jnp.where(lane_head == h, value[h * PAD : (h + 1) * PAD], out)
        return out

    acc[...] = jnp.zeros_like(acc)

    def attend(i, carry):
        tt = group(i)

        use_at(i, "use_a%d", nt, 1)
        q = (nn(h1[...], weight(0, tt, 0, LANES)) + vg[tt, 2:3, :]) * SCALE
        qs[tt] = q.astype(BF16)
        kv = nn(h1[...], weight(1, tt))
        kvs[tt, :, :LANES] = kv[:, :LANES].astype(BF16)
        kvs[tt, :, LANES:] = (kv[:, LANES:] + vg[tt, 3:4, :]).astype(BF16)

        def window(w):
            at = pl.ds(pl.multiple_of(w * PAD, PAD), PAD)
            s = nt_dot(kvs[tt, at, :LANES], stack(qs[tt, at, :])) + rg[tt] + mask[w]
            e = jnp.exp(s - jnp.max(s, axis=0, keepdims=True))
            p = e / rowsum(e)
            probs[tt, w] = p
            att[tt, at, :] = pick(tn_dot(p.astype(BF16), kvs[tt, at, LANES:])).astype(BF16)

        def four(hh, carry):
            for j in range(slots // 2):
                window(hh * (slots // 2) + j)

            @pl.when(hh == 0)
            def _():
                run_at(i, "a%df", nt)

            return carry

        lax.fori_loop(0, 2, four, 0)
        acc[...] += nt_dot(att[tt], weight(0, tt, LANES, LANES))
        run_at(i, "a%ds", nt)
        return carry

    lax.fori_loop(0, nt, attend, 0)
    own_cot.wait()
    await_tok(1)
    spread(cg, gy)
    b_out, gain2, shift2 = wide(4), wide(5), wide(6)

    def live_rows(i):
        slot = lax.div(i * half + lax.broadcasted_iota(jnp.int32, (half, 1), 0), PAD)
        return slot < n_live

    def middle(i, at, carry):
        x1 = xp[at, :] + acc[at, :] + b_out
        xp[at, :] = x1
        normed, rstd = norm(x1)
        n2[at, :] = normed
        r2[at, :] = rstd
        h = normed * gain2 + shift2
        low[at, :] = h.astype(BF16)
        h2t[:, at] = h.T.astype(BF16)
        g = jnp.where(live_rows(i), gy[at, :], 0.0)
        gy[at, :] = g
        gkv[at, :] = g.astype(BF16)
        gyt[:, at] = g.T.astype(BF16)
        return carry

    each(middle)
    run("mid")
    acc[...] = jnp.zeros_like(acc)
    acc2[...] = jnp.zeros_like(acc2)
    def mlp(k, carry):
        s, i = lax.div(k, nt), lax.rem(k, nt)
        turn_at = MLP_ORDER[nt - 1]
        for j in range(nt - 1):
            turn_at = jnp.where(i == j, MLP_ORDER[j], turn_at)
        tt = group(turn_at)
        up, down = 2 + s, 4 + s
        use_at(k, "use_m%d", 2 * nt)

        bias = vg[tt, pl.ds(8 + 2 * s, 2), :]
        bias = jnp.concatenate([bias[0:1], bias[1:2]], axis=1)
        hidden = nn(low[...], weight(up, tt)) + bias
        act, slope = gelu_pair(hidden)
        act_low = act.astype(BF16)
        acc[...] += nt_dot(act_low, weight(down, tt))
        put_grad(down, tt, nn(gyt[...], act_low))
        grad = nn(gkv[...], weight(down, tt)) * slope
        total = rowsum(grad)
        small[tt, pl.ds(8 + 2 * s, 1), :] = total[:, :LANES]
        small[tt, pl.ds(9 + 2 * s, 1), :] = total[:, LANES:]
        grad_low = grad.astype(BF16)
        put_grad(up, tt, nn(h2t[...], grad_low))
        acc2[...] += nt_dot(grad_low, weight(up, tt))

        for when, j in ((MLP_ORDER.index(1), 1), (MLP_ORDER.index(3), 0)):

            @pl.when(i == when)
            def _(j=j):
                kc(up, j).start()
                kc(down, j).start()

        run_at(k, "m%d", 2 * nt)
        return carry

    lax.fori_loop(0, 2 * nt, mlp, 0)
    b_down = wide(7)
    zero_row = jnp.zeros((1, C), F32)

    def turn(i, at, carry):
        xp[at, :] = jnp.where(live_rows(i), xp[at, :] + acc[at, :] + b_down, 0.0)
        e, normed, g = acc2[at, :], n2[at, :], gy[at, :]
        gx = norm_back(e * gain2, normed, r2[at, :]) + g
        gy[at, :] = gx
        low[at, :] = gx.astype(BF16)
        h2t[:, at] = gx.T.astype(BF16)
        sums = (rowsum(e * normed), rowsum(e), rowsum(gx), rowsum(g))
        return tuple(p + q for p, q in zip(carry, sums))

    sums = each(turn, (zero_row,) * 4)
    put_small(5, sums[0])
    put_small(6, sums[1])
    put_small(4, sums[2])
    put_small(7, sums[3])
    gather(xp, yb)
    own_y = pltpu.make_async_copy(yb.at[t], y_all.at[t], loc.at[2])
    own_y.start()
    run("turn")
    acc[...] = jnp.zeros_like(acc)

    def back(i, carry):
        tt = group(3 - i)
        gatt[...] = nn(low[...], weight(0, tt, LANES, LANES)).astype(BF16)
        pairs[...] = jnp.zeros_like(pairs)

        def window(w):
            at = pl.ds(pl.multiple_of(w * PAD, PAD), PAD)
            q4, g4 = stack(qs[tt, at, :]), stack(gatt[at, :])
            p = probs[tt, w]
            dp = nt_dot(kvs[tt, at, LANES:], g4)
            ds = p * (dp - rowsum(p * dp))
            ds_low = ds.astype(BF16)
            gkv[at, :LANES] = nn(ds_low, q4).astype(BF16)
            gkv[at, LANES:CW] = nn(p.astype(BF16), g4).astype(BF16)
            gq[at, :] = pick(tn_dot(ds_low, kvs[tt, at, :LANES])).astype(BF16)
            return ds_low.astype(F32)

        def four(hh, carry):
            total = window(hh * (slots // 2))
            for j in range(1, slots // 2):
                total = total + window(hh * (slots // 2) + j)
            pairs[...] += total

            @pl.when(hh == 0)
            def _():
                run_at(i, "b%df", nt)

            return carry

        lax.fori_loop(0, 2, four, 0)
        gk_gv = gkv[:, :CW]
        put_grad(1, tt, nn(h1t[...], gk_gv))

        left = nn(h1t[...], gq[...]) * SCALE
        put_grad(0, tt, jnp.concatenate([left, nn(h2t[...], att[tt])], axis=1))

        @pl.when(i == 0)
        def _():
            kc(1, 0).start()
            kc(0, 0).start()

        @pl.when(i == 2)
        def _():
            kc(1, 1).start()
            kc(0, 1).start()

        run_at(i, "b%dd", nt)
        small[tt, 2:3, :] = rowsum(gq[...].astype(F32)) * SCALE
        small[tt, 3:4, :] = rowsum(gkv[:, LANES:CW].astype(F32))
        grad_q = nt_dot(gq[...], weight(0, tt, 0, LANES)) * SCALE
        acc[...] += grad_q + nt_dot(gk_gv, weight(1, tt))
        for h in range(heads):
            lanes = h // 2 * LANES
            source = pairs[:, lanes : lanes + LANES]
            for q in range(TPAD // LANES):
                where = inv[:, q * LANES : (q + 1) * LANES]
                value = take(source, jnp.maximum(where, 0) + h % 2 * PAD)
                value = jnp.where(where >= 0, value, 0.0)
                small[tt, pl.ds(12 + 2 * h + q, 1), :] = rowsum(value)

        run_at(i, "b%ds", nt)
        return carry

    lax.fori_loop(0, nt, back, 0)

    def finish(i, at, carry):
        e, normed = acc[at, :], n1[at, :]
        xp[at, :] = norm_back(e * gain1, normed, r1[at, :]) + gy[at, :]
        sums = (rowsum(e * normed), rowsum(e))
        return tuple(p + q for p, q in zip(carry, sums))

    sums = each(finish, (zero_row,) * 2)
    put_small(0, sums[0])
    put_small(1, sums[1])
    for d in range(3):
        small_t(d).start()
    gather(xp, gb)
    own_g = pltpu.make_async_copy(gb.at[t], g_all.at[t], loc.at[3])
    own_g.start()
    run("t1")
    run("t2")
    await_bytes(scr, coming("st"))
    zb[z] = small[t] + scr[0] + (scr[1] + scr[2])
    for d in range(nz - 1):
        small_z(d).start()
    run("t3")
    await_bytes(zb.at[pl.ds(0, nz - 1)], coming("sz"))
    value = zb[0]
    for zz in range(1, nz):
        value = value + zb[zz]
    sx[...] = value
    small_x().start()
    run("t4")
    run("t5")
    for ch in (2, 4, 3, 5, 1, 0):
        last(ch)
    small_x().wait_recv()
    tot[...] = sx[...] + syr[...]
    for i in range(2):
        await_bytes((yb, gb)[i].at[pl.ds(0, 3)], coming("out", i))
    for i, n in enumerate(totals):
        await_bytes(blocks(n), ss.at[i])
    three = (xg, cg, vg, yb, gb, small)
    for i, ref in enumerate(three):
        await_bytes(ref.at[pl.ds(0, 3)], ss.at[len(totals) + i])
    await_bytes(zb.at[pl.ds(0, nz - 1)], ss.at[len(totals) + 6])
    await_bytes(sx, ss.at[len(totals) + 7])
    own_y.wait()
    own_g.wait()


def block_call(nt, nz, slots, *args):
    tok, deep, heads = args[1], args[3].shape[0], args[18].shape[0]
    real = tok.shape[1]
    rows, wide = slots * PAD, heads * PAD
    piece = (nz, 2, deep, CW)
    row = (nt, real, LANES)

    def vm(shape, kind=BF16):
        return pltpu.VMEM(shape, kind)

    small = (SROWS, LANES)
    n_c = max(1, WAY_OUT.count("C"))
    return pl.pallas_call(
        functools.partial(block, nt, nz, slots),
        name="block",
        out_shape=(
            jax.ShapeDtypeStruct(row, BF16),
            jax.ShapeDtypeStruct(row, BF16),
            jax.ShapeDtypeStruct((NCH, deep, CW), F32),
            jax.ShapeDtypeStruct(small, F32),
        ),
        in_specs=[SM] + [ANY] * 20,
        out_specs=(ANY, ANY, VM, VM),
        scratch_shapes=[vm(arg.shape, arg.dtype) for arg in args[9:]]
        + [
            vm(row),
            vm(row),
            vm((NCH, nt) + piece),
            vm((nt,) + small, F32),
            vm((nt, PAD, wide), F32),
            vm((NCH, nt) + piece),
            vm((NCH, 2) + piece),
            vm((max(1, WAY_OUT.count("A")),) + piece),
            vm((WAY_OUT.count("B"), 2, nz, deep, CW)),
            vm((NCH, nz, deep, CW)),
            vm((NCH, nz - 1, deep, CW)),
            vm((n_c, nz - 1, 2, 2, deep, CW)),
            vm((n_c, 3, deep, CW)),
            vm((3,) + small, F32),
            vm(small, F32),
            vm(small, F32),
            vm((nz,) + small, F32),
            vm((nt,) + small, F32),
            vm(row),
            vm(row),
            vm((LANES, LANES), F32),
            vm((slots, PAD, wide), F32),
            vm((PAD, TPAD), jnp.int32),
            vm((real, C), F32),
            vm((rows, C), F32),
            vm((rows, C), F32),
            vm((rows, C)),
            vm((C, rows)),
            vm((C, rows)),
            vm((C, rows)),
            vm((nt, rows, LANES)),
            vm((nt, rows, CW)),
            vm((nt, slots, PAD, wide), F32),
            vm((nt, rows, LANES)),
            vm((rows, C), F32),
            vm((rows, C), F32),
            vm((rows, C), F32),
            vm((rows, 1), F32),
            vm((rows, C), F32),
            vm((rows, 1), F32),
            vm((rows, C)),
            vm((rows, C)),
            vm((rows, LANES)),
            vm((rows, LANES)),
            vm((PAD, wide), F32),
            DMA((4,)),
            DMA((14,)),
            DMA((len(arrival_table(nz)),)),
            DMA((len(send_table(nt, nz)[1]) + 8,)),
        ],
        compiler_params=pltpu.CompilerParams(
            collective_id=0, has_side_effects=True, vmem_limit_bytes=60 * 2**20
        ),
    )(*args)


def spell(n, *refs):
    ins, outs, refs = refs[:4], refs[4 : 4 + n], refs[4 + n :]
    (y_in, g_in, fin, tot), refs = refs[:4], refs[4:]
    held, (get, put) = refs[:n], refs[n:]
    steps = ins[0].shape[0]
    loads = [pltpu.make_async_copy(ins[2], fin, get.at[0])]
    loads.append(pltpu.make_async_copy(ins[3], tot, get.at[1]))
    for i in range(steps):
        for j, ref in enumerate((y_in, g_in)):
            loads.append(
                pltpu.make_async_copy(ins[j].at[i], ref.at[i], get.at[2 + 2 * i + j])
            )
    for copy in loads:
        copy.start()
    loads[0].wait()
    loads[1].wait()
    spell_rest(fin, tot, *held[2:])
    like = {}
    for k in range(2, n):
        slot = 2 + list(like).index(held[k].shape) if held[k].shape in like else 2 + len(like)
        like.setdefault(held[k].shape, []).append(k)
        pltpu.make_async_copy(held[k], outs[k], put.at[slot]).start()
    for i in range(steps):
        for j, ref in enumerate((y_in, g_in)):
            loads[2 + 2 * i + j].wait()
            held[j][i] = ref[i].astype(F32)
            pltpu.make_async_copy(held[j].at[i], outs[j].at[i], put.at[j]).start()
    for j in range(2):
        pltpu.make_async_copy(held[j], outs[j], put.at[j]).wait()
    for slot, (shape, ks) in enumerate(like.items()):
        size = len(ks) * shape[0] * shape[1]
        if len(ks) == 1:
            ref = held[ks[0]]
        elif shape[0] == 1:
            ref = tot.at[pl.ds(0, len(ks))]
        else:
            ref = fin.at[pl.ds(0, size // (fin.shape[1] * fin.shape[2]))]
        pltpu.make_async_copy(ref, ref, put.at[2 + slot]).wait()


def spell_rest(fin, tot, *outs):
    (
        d_g1, d_s1, d_wq, d_wk, d_wv, d_bq, d_bv, d_wo, d_bo, d_g2, d_s2, d_wh, d_bh,
        d_wd, d_bd, d_tab,
    ) = outs
    d_wq[...] = fin[0, :, :LANES]
    d_wk[...] = fin[1, :, :LANES]
    d_wv[...] = fin[1, :, LANES:]
    d_wo[...] = fin[0, :, LANES:]
    for s in range(2):
        d_wh[:, s * CW : (s + 1) * CW] = fin[2 + s]
        d_wd[:, s * CW : (s + 1) * CW] = fin[4 + s]
    for i, ref in enumerate((d_g1, d_s1, d_bq, d_bv, d_bo, d_g2, d_s2, d_bd)):
        ref[...] = tot[i : i + 1, :]
    d_bh[...] = tot[8:12, :]
    for h in range(d_tab.shape[0]):
        d_tab[h : h + 1, :LANES] = tot[12 + 2 * h : 13 + 2 * h]
        d_tab[h : h + 1, LANES:] = tot[13 + 2 * h : 14 + 2 * h, : TABLE - LANES]


def spell_call(outs, *args):
    n, steps = len(outs), args[0].shape[0]
    held = [pltpu.VMEM(v.shape, v.dtype) for v in args + outs]
    return pl.pallas_call(
        functools.partial(spell, n),
        name="spell",
        out_shape=outs,
        in_specs=[ANY] * 4,
        out_specs=(ANY,) * n,
        scratch_shapes=held + [DMA((2 + 2 * steps,)), DMA((2 + len({v.shape for v in outs[2:]}),))],
        compiler_params=pltpu.CompilerParams(vmem_limit_bytes=60 * 2**20),
    )(*args)


def per_device(
    nt, na, tokens, gain_one, shift_one, w_query, w_key, w_value, b_query, b_value, w_out, b_out,
    gain_two, shift_two, w_hidden, b_hidden, w_down, b_down, bias_table, rel_index, region,
    win_count, cotangent,
):
    slots = region.shape[0] // nt
    cut = (nt, slots * WT, LANES)
    vectors = [gain_one, shift_one, b_query, b_value, b_out, gain_two, shift_two, b_down]
    parts = block_call(
        nt, na // 2, slots,
        win_count, tokens.reshape(cut), cotangent.reshape(cut),
        w_query, w_key, w_value, w_out.T, w_hidden, w_down.T,
        *[v.reshape(1, LANES) for v in vectors],
        b_hidden.reshape(-1, LANES), bias_table.T, rel_index, region,
    )

    def out(like, shape=None):
        return jax.ShapeDtypeStruct(shape or like.shape, F32)

    one = (1, LANES)
    shapes = (
        out(tokens, cut), out(tokens, cut), out(gain_one, one), out(gain_one, one), out(w_query),
        out(w_key), out(w_value), out(b_query, one), out(b_value, one), out(w_out, w_out.shape[::-1]),
        out(b_out, one), out(gain_two, one), out(shift_two, one), out(w_hidden),
        out(b_hidden, (b_hidden.shape[0] // LANES, LANES)), out(w_down, w_down.shape[::-1]),
        out(b_down, one), out(bias_table, bias_table.shape[::-1]),
    )
    likes = (
        tokens, tokens, gain_one, gain_one, w_query, w_key, w_value, b_query, b_value, w_out,
        b_out, gain_two, shift_two, w_hidden, b_hidden, w_down, b_down, bias_table,
    )
    values = spell_call(shapes, *parts)
    turned = (9, 15, 17)
    return tuple(
        v.T if i in turned else v.reshape(like.shape)
        for i, (v, like) in enumerate(zip(values, likes))
    )


def solution(mesh):
    return jax.shard_map(
        functools.partial(per_device, mesh.shape["ta"], mesh.shape["wa"]),
        mesh=mesh,
        in_specs=(
            P("wa", "ta"),
            P("ta"),
            P("ta"),
            P("wa", "ta"),
            P("wa", "ta"),
            P("wa", "ta"),
            P("ta"),
            P("ta"),
            P("ta", "wa"),
            P("ta"),
            P("ta"),
            P("ta"),
            P("wa", "ta"),
            P("ta"),
            P("ta", "wa"),
            P("ta"),
            P(None, "ta"),
            P(),
            P("wa", None),
            P("wa"),
            P("wa", "ta"),
        ),
        out_specs=(
            P("wa", "ta"),
            P("wa", "ta"),
            P("ta"),
            P("ta"),
            P("wa", "ta"),
            P("wa", "ta"),
            P("wa", "ta"),
            P("ta"),
            P("ta"),
            P("ta", "wa"),
            P("ta"),
            P("ta"),
            P("ta"),
            P("wa", "ta"),
            P("ta"),
            P("ta", "wa"),
            P("ta"),
            P(None, "ta"),
        ),
        check_vma=False,
    )
```

```python
import functools

import jax
import jax.numpy as jnp
from jax import lax
from jax.experimental import pallas as pl
from jax.experimental.pallas import tpu as pltpu
from jax.sharding import PartitionSpec as P

C = 512
HDIM = 32
WT = 49
PAD = 64
TABLE = 169
TPAD = 256
NCH = 6
CW = 256
LANES = 128
SROWS = 24
SCALE = HDIM ** (-0.5)
EPS = 1e-05
F32 = jnp.float32
BF16 = jnp.bfloat16
MESH = pl.DeviceIdType.MESH
ANY = pl.BlockSpec(memory_space=pl.ANY)
VM = pl.BlockSpec(memory_space=pltpu.VMEM)
SM = pl.BlockSpec(memory_space=pltpu.SMEM)
DMA = pltpu.SemaphoreType.DMA


WAY_IN = ("A", "B", "A", "B", "E", "C")
WAY_OUT = ("B", "B", "B", "C", "A", "B")
MLP_ORDER = (0, 1, 3, 2)
PLAN = {
    "h0": ("az2",),
    "h1": ("az4", "yx1",),
    "h2": ("zx2", "ay0",),
    "h3": ("az3",),
    "a0f": ("c11", "cot",),
    "a1f": ("zt4", "az5", "xy2", "zx4",),
    "a1s": ("c02", "zy3",),
    "a3f": ("zx3",),
    "a3s": ("c04",),
    "m1": ("yx3", "c03",),
    "m2": ("c15",),
    "m3": ("c05",),
    "m4": ("o14", "c13", "ot2", "oo2",),
    "m7": ("o22", "oo3", "oo5",),
    "turn": ("ot3",),
    "b0f": ("ot5", "yout",),
    "b0d": ("o24",),
    "b0s": ("o32",),
    "b1d": ("ot1", "o25", "ot0",),
    "b2d": ("o34",),
    "b3f": ("o21",),
    "b3d": ("oo0",),
    "b3s": ("o35",),
    "t1": ("o20", "o23",),
    "t2": ("g", "o31",),
    "t3": ("o33", "o30",),
    "m0": ("c12", "c14",),
    "b3e": ("oo1",),
    "a2f": ("c10",),
}


def plan_order(sched):
    out = list(sched.get("h0", ())) + list(sched.get("h1", ()))
    out += list(sched.get("h2", ())) + ["use_a0"]
    out += sched.get("h3", ())
    for i in range(4):
        out += ([f"use_a{i}"] if i else []) + list(sched.get(f"a{i}f", ()))
        out += sched.get(f"a{i}s", ())
    out += list(sched.get("mid", ()))
    for k in range(8):
        out += [f"use_m{k}"] + list(sched.get(f"m{k}", ()))
    out += sched.get("turn", ())
    for i in range(4):
        for part in "feds":
            out += sched.get(f"b{i}{part}", ())
    for i in range(1, 6):
        out += sched.get(f"t{i}", ())
    return out + ["end"]


def flip(bit, by):
    return bit + by - 2 * bit * by


def add(left, right):
    return (left.astype(F32) + right.astype(F32)).astype(BF16)


def nn(left, right):
    return jnp.dot(left, right, preferred_element_type=F32)


def nt_dot(left, right):
    return lax.dot_general(left, right, (((1,), (1,)), ((), ())), preferred_element_type=F32)


def tn_dot(left, right):
    return lax.dot_general(left, right, (((0,), (0,)), ((), ())), preferred_element_type=F32)


def norm(value):
    mean = jnp.mean(value, axis=1, keepdims=True)
    spread = jnp.mean(value * value, axis=1, keepdims=True) - mean * mean
    rstd = lax.rsqrt(spread + EPS)
    return (value - mean) * rstd, rstd


def norm_back(scaled, normed, rstd):
    first = jnp.mean(scaled, axis=1, keepdims=True)
    second = jnp.mean(scaled * normed, axis=1, keepdims=True)
    return rstd * (scaled - first - normed * second)


def gelu_pair(u):
    cdf = 0.5 + 0.5 * lax.erf(u * (0.5**0.5))
    pdf = jnp.exp(-0.5 * u * u) * ((2.0 * jnp.pi) ** -0.5)
    return u * cdf, cdf + u * pdf


def rowsum(value):
    return jnp.sum(value, axis=0, keepdims=True)


def arrival_table(nz):
    keys = [("kc", ch, j) for ch in range(NCH) for j in range(2)]
    keys += [("ac", ch, j) for ch in range(NCH) for j in range(2)]
    keys += [("az", ch, d) for ch in range(2) for d in range(nz - 1)]
    keys += [("tok", i) for i in range(3)] + [("out", i) for i in range(2)]
    keys += [(kind, ch) for kind in ("ax", "ay") for ch in range(2)]
    keys += [("bx", 1, 1), ("st",), ("sz",), ("sx",)]
    for ch in range(2, NCH):
        keys += [("az", ch), ("by", ch)]
        if WAY_IN[ch] == "C":
            keys.append(("cx", ch))
        else:
            keys += [("bx", ch, j) for j in range(1 if WAY_IN[ch] == "A" else 2)]
    for ch in range(NCH):
        if WAY_OUT[ch] == "C":
            keys += [("zc", ch), ("xc", ch), ("yc", ch)]
            continue
        keys += [("zr", ch), ("q", ch), ("p", ch, 0)]
        if WAY_OUT[ch] == "B":
            keys += [("px", ch, d) for d in range(nz)] if ch < 2 else [("p", ch, 1)]
    return {key: i for i, key in enumerate(keys)}


def send_table(nt, nz):
    whole = {("kc", ch, j): 2 * nz for ch in range(NCH) for j in range(2)}
    whole.update({("ac", ch, j): 2 * nz for ch in range(NCH) for j in range(2)})
    sends = {}
    for ch in range(2):
        sends.update({("az", ch, d, 0): 1 for d in range(nz - 1)})
        sends.update({("ax", ch, i): 1 for i in range(nz)})
        sends.update({("ay", ch, i): 2 - ch for i in range(nz)})
        sends.update({("px", ch, d): 1 for d in range(nz)})
    sends["bx", 1, 1] = nz
    for ch in range(2, NCH):
        way = WAY_IN[ch]
        both = 2 if way in "CE" else 1
        size = 2 if way == "C" else 1
        sends.update({("az", ch, d, j): size for d in range(nz - 1) for j in range(both)})
        sends["by", ch] = {"A": 2 * nz, "B": nz, "C": 1, "E": 1}[way]
        sends.update({("bx", ch, j): 1 if way == "C" else nz for j in range(1 + (way != "A"))})
    for ch in range(NCH):
        way = WAY_OUT[ch]
        if way == "C":
            sends.update({("zc", ch, d, j): 2 for d in range(nz - 1) for j in range(2)})
            sends.update({("xc", ch, j): 1 for j in range(3)})
            continue
        sends.update({("zr", ch, d): 1 for d in range(nz - 1)})
        sends["q", ch] = nz
        sends["p", ch, 0] = 2 * nz if way == "A" else nz
        if way == "B" and ch > 1:
            sends["p", ch, 1] = nz
    order = sorted(sends, key=lambda key: -sends[key])
    left = sum(sends.values())
    groups, totals = {key: 0 for key in whole}, [sum(whole.values())]
    for unit, most in ((2 * nz * nt, NCH), (2 * nz, nt), (2, nz), (1, 1)):
        goal = unit * min(most, left // unit)
        if goal:
            total = 0
            while total < goal:
                key = order.pop(0)
                total += sends[key]
                groups[key] = len(totals)
            assert total == goal
            totals.append(total)
            left -= total
    assert not order
    return groups, totals


def block(nt, nz, slots, *refs):
    live, tok, cot, wq, wk, wv, wo, wh, wd = refs[:9]
    outside, refs = refs[9:21], refs[21:]
    inside, refs = refs[4:16], refs[:4] + refs[16:]
    g1, s1, bq, bv, bo, g2, s2, bd, bh, tab, rel, reg = inside
    (
        y_all, g_all, fin, tot,
        xg, cg, gw, vg, rg, dv, rc, ry, rx, r3, rz, rzc, rxc, scr, syr, sx, zb, small, yb, gb, square, mask, inv,
        xs, xp, gy, h1, h1t, h2t, gyt, qs, kvs, probs, att, acc, acc2, n1, r1, n2, r2, low, gkv, gq, gatt,
        pairs,
        loc, ld, rs, ss,
    ) = refs
    heads = LANES // HDIM
    rows = slots * PAD
    half = 2 * PAD
    nhalf = rows // half
    a, t = lax.axis_index("wa"), lax.axis_index("ta")
    x, z, c, y = lax.rem(a, 2), lax.div(a, 2), lax.rem(t, 2), lax.div(t, 2)

    def group(m):
        return 2 * flip(y, m // 2 if isinstance(m, int) else lax.div(m, 2)) + flip(
            c, m % 2 if isinstance(m, int) else lax.rem(m, 2)
        )

    t1, t2, t3 = group(1), group(2), group(3)
    xpeer, ypeer, cpeer = (z * 2 + (1 - x), t), (a, t2), (a, t1)
    zs = [(lax.rem(z + d, nz) * 2 + x, t) for d in range(1, nz)]
    ts = [(a, tt) for tt in (t1, t2, t3)]
    peers = zs + ts + [xpeer]
    barrier = pltpu.get_barrier_semaphore()
    for peer in peers:
        pl.semaphore_signal(barrier, inc=1, device_id=peer, device_id_type=MESH)

    arrival, (group_of, totals) = arrival_table(nz), send_table(nt, nz)

    def coming(*key):
        return rs.at[arrival[key]]

    def going(*key):
        return ss.at[group_of[key]]

    def blocks(n):
        for unit, ref in ((2 * nz * nt, gw), (2 * nz, gw.at[0]), (2, gw.at[0, 0])):
            if n % unit == 0:
                return ref.at[pl.ds(0, n // unit)]
        assert n == 1
        return gw.at[0, 0, 0, 0]

    def await_bytes(ref, sem):
        pltpu.make_async_copy(ref, ref, sem).wait()

    def far(src, dst, send, recv, peer):
        return pltpu.make_async_remote_copy(
            src_ref=src, dst_ref=dst, send_sem=send, recv_sem=recv, device_id=peer,
            device_id_type=MESH,
        )

    def tok_copy(i, d):
        src, dst = ((tok, xg), (cot, cg), (vg, vg))[i]
        peer = ts[d]
        src = src.at[peer[1]] if i < 2 else src.at[t]
        return far(src, dst.at[t], ss.at[len(totals) + i], coming("tok", i), peer)

    def out_copy(i, d):
        src, dst = ((yb, y_all), (gb, g_all))[i]
        peer = ts[d]
        return far(src.at[peer[1]], dst.at[t], ss.at[len(totals) + 3 + i], coming("out", i), peer)

    def az_await(ch):
        n = (nz - 1) * {"A": 1, "B": 1, "C": 4, "E": 2}[WAY_IN[ch]]
        size = n // (nz - 1)
        ref = rz.at[0] if size == 1 else rzc.at[0, :, :, 0] if size == 2 else rzc.at[0]
        await_bytes(ref, coming("az", ch))

    def az_from(ch, zz):
        d = lax.rem(z - zz + nz, nz) - 1
        await_bytes(gw.at[ch, t, z, x], rs.at[arrival["az", ch, 0] + d])

    def far_first(k):
        rising = k + jnp.where(z > k, 0, 1)
        falling = nz - 1 - k - jnp.where(z < nz - 1 - k, 0, 1)
        zz = jnp.where(2 * z < nz, falling, rising)
        return zz, lax.rem(zz - z + nz, nz) - 1

    def az_start(ch):
        for k in range(nz - 1):
            zz, d = far_first(k)
            for j in range(2 if WAY_IN[ch] in "CE" else 1):
                far_t = t2 if j else t
                ref = gw.at[ch, far_t, z] if WAY_IN[ch] == "C" else gw.at[ch, far_t, z, x]
                there = rs.at[arrival["az", ch, 0] + d] if ch < 2 else coming("az", ch)
                far(ref, ref, going("az", ch, k, j), there, (zz * 2 + x, t)).start()

    def zr_start(ch, k):
        zz, d = far_first(k)
        src = dv.at[ch, t, zz, x]
        far(src, rz.at[ch, d], going("zr", ch, k), coming("zr", ch), (zz * 2 + x, t)).start()

    def ax(ch, zz, i):
        ref = gw.at[ch, t, zz, x]
        return far(ref, ref, going("ax", ch, i), coming("ax", ch), xpeer)

    def ay(ch, zz, i):
        ref = gw.at[ch, t, zz] if ch == 0 else gw.at[ch, t, zz, x]
        return far(ref, ref, going("ay", ch, i), coming("ay", ch), ypeer)

    def bx(ch, j):
        ref = gw.at[ch, t2 if j else t, :, x]
        return far(ref, ref, going("bx", ch, j), coming("bx", ch, j), xpeer)

    def by(ch):
        ref = gw.at[ch, t] if WAY_IN[ch] == "A" else gw.at[ch, t, :, x]
        return far(ref, ref, going("by", ch), coming("by", ch), ypeer)

    def cy(ch):
        ref = gw.at[ch, t, z, x]
        return far(ref, ref, going("by", ch), coming("by", ch), ypeer)

    def cx(ch, j):
        ref = gw.at[ch, t2 if j else t, z, x]
        return far(ref, ref, going("bx", ch, j), coming("cx", ch), xpeer)

    def ac(ch, j):
        ref = gw.at[ch, t2 if j else t]
        return far(ref, ref, going("ac", ch, j), coming("ac", ch, j), cpeer)

    def kc(ch, j):
        return far(dv.at[ch, t1 if j else t3], rc.at[ch, j], ss.at[0], rs.at[ch * 2 + j], cpeer)

    a_slot = {ch: i for i, ch in enumerate(c for c in range(NCH) if WAY_OUT[c] == "A")}
    b_slot = {ch: i for i, ch in enumerate(c for c in range(NCH) if WAY_OUT[c] == "B")}
    c_slot = {ch: i for i, ch in enumerate(c for c in range(NCH) if WAY_OUT[c] == "C")}

    def ya(ch):
        return far(dv.at[ch, t2], ry.at[a_slot[ch]], going("p", ch, 0), coming("p", ch, 0), ypeer)

    def xa(ch):
        return far(dv.at[ch, t, :, 1 - x], r3.at[ch], going("q", ch), coming("q", ch), xpeer)

    def piece_of(d):
        return far_first(d)[0] if d < nz - 1 else z

    def xp1(ch, d):
        zz = piece_of(d)
        src, dst = dv.at[ch, t, zz, 1 - x], rx.at[b_slot[ch], 1, zz]
        return far(src, dst, going("px", ch, d), coming("px", ch, d), xpeer)

    def xb(ch, j):
        src = dv.at[ch, t if j else t2, :, 1 - x]
        return far(src, rx.at[b_slot[ch], j], going("p", ch, j), coming("p", ch, j), xpeer)

    def yb2(ch):
        return far(dv.at[ch, t2, :, x], r3.at[ch], going("q", ch), coming("q", ch), ypeer)

    def zc_start(ch, j):
        i = c_slot[ch]
        for k in range(nz - 1):
            zz, d = far_first(k)
            src, peer = dv.at[ch, t if j else t2, zz], (zz * 2 + x, t)
            far(src, rzc.at[i, d, j], going("zc", ch, k, j), coming("zc", ch), peer).start()

    def xc(ch, j):
        src, i = dv.at[ch, t if j else t2, z, 1 - x], c_slot[ch]
        return far(src, rxc.at[i, j], going("xc", ch, j), coming("xc", ch), xpeer)

    def yc(ch):
        i = c_slot[ch]
        return far(dv.at[ch, t2, z, x], rxc.at[i, 2], going("xc", ch, 2), coming("yc", ch), ypeer)

    def small_t(d):
        return far(small.at[ts[d][1]], scr.at[d], ss.at[len(totals) + 5], coming("st"), ts[d])

    def small_z(d):
        return far(zb.at[z], zb.at[z], ss.at[len(totals) + 6], coming("sz"), zs[d])

    def small_x():
        return far(sx, syr, ss.at[len(totals) + 7], coming("sx"), xpeer)

    def lanes(ch, i, size):
        return gw.at[ch, t, z, x, :, pl.ds(i * size, size)]

    loads = [(wq, lanes(0, 0, LANES), 0), (wo, lanes(0, 1, LANES), 0)]
    loads += [(wk, lanes(1, 0, LANES), 0), (wv, lanes(1, 1, LANES), 0)]
    for i in range(2):
        loads += [(wh.at[:, pl.ds(i * CW, CW)], gw.at[2 + i, t, z, x], 1)]
        loads += [(wd.at[:, pl.ds(i * CW, CW)], gw.at[4 + i, t, z, x], 1)]
    loads += [(src, dst, 2 + i) for i, (src, dst) in enumerate(zip(outside, inside))]
    for src, dst, i in loads:
        pltpu.make_async_copy(src, dst, ld.at[i]).start()
    await_bytes(gw.at[0, 0, 0], ld.at[0])
    await_bytes(gw.at[0, 0, pl.ds(0, 2)], ld.at[1])
    for src, dst, i in loads[8:]:
        pltpu.make_async_copy(src, dst, ld.at[i]).wait()
    for i, ref in enumerate((g1, s1, bq, bv, bo, g2, s2, bd)):
        vg[t, i : i + 1, :] = ref[...]
    vg[t, 8:12, :] = bh[...]
    for h in range(heads):
        vg[t, 12 + 2 * h : 13 + 2 * h, :] = tab[h : h + 1, :LANES]
        vg[t, 13 + 2 * h : 14 + 2 * h, : TABLE - LANES] = tab[h : h + 1, LANES:]
        vg[t, 13 + 2 * h : 14 + 2 * h, TABLE - LANES :] = jnp.zeros((1, TPAD - TABLE), F32)
    vg[t, 12 + 2 * heads :, :] = jnp.zeros((SROWS - 12 - 2 * heads, LANES), F32)
    pl.semaphore_wait(barrier, len(peers))
    own_tok = pltpu.make_async_copy(tok.at[t], xg.at[t], loc.at[0])
    own_cot = pltpu.make_async_copy(cot.at[t], cg.at[t], loc.at[1])
    own_tok.start()
    own_cot.start()
    early = [ch for ch in range(2, NCH) if WAY_IN[ch] in "CE"]
    first = [ch for ch in early if f"az{ch}" in PLAN.get("h0", ())]
    for ch in first:
        cy(ch).start()
    for d in range(3):
        tok_copy(2, d).start()
    az_start(1)
    ax(1, z, 0).start()
    ay(1, z, 0).start()
    az_start(0)
    ax(0, z, 0).start()
    for d in range(3):
        tok_copy(0, d).start()
    for ch in early:
        if ch not in first:
            cy(ch).start()
    square[...] = jnp.zeros_like(square)
    square[:WT, :WT] = rel[...].astype(F32)
    rel_t = square[...].T[:PAD, :PAD]
    pick_at = jnp.concatenate([rel_t, rel_t], axis=1).astype(jnp.int32)
    lane = lax.broadcasted_iota(jnp.int32, (PAD, LANES), 1)
    low_at, high_at = jnp.minimum(pick_at, LANES - 1), jnp.maximum(pick_at - LANES, 0)

    def take(value, at):
        return jnp.take_along_axis(value, at, axis=1, mode="promise_in_bounds")

    def entry(tt, h):
        first = jnp.broadcast_to(vg[tt, 12 + 2 * h : 13 + 2 * h, :], (PAD, LANES))
        second = jnp.broadcast_to(vg[tt, 13 + 2 * h : 14 + 2 * h, :], (PAD, LANES))
        return jnp.where(pick_at < LANES, take(first, low_at), take(second, high_at))

    def bias_of(tt):
        for q in range(heads // 2):
            rg[tt, :, q * LANES : (q + 1) * LANES] = jnp.where(
                lane < PAD, entry(tt, 2 * q), entry(tt, 2 * q + 1)
            )

    number = lax.broadcasted_iota(jnp.int32, (PAD, TPAD), 1).astype(F32)
    found = jnp.full((PAD, TPAD), -1.0, F32)
    for i in range(WT):
        found = jnp.where(rel_t[:, i : i + 1] == number, float(i), found)
    inv[...] = found.astype(jnp.int32)
    square[...] = jnp.zeros_like(square)
    mine = reg[pl.ds(pl.multiple_of(t * slots, slots), slots), :]
    square[:slots, :WT] = mine.astype(F32)
    reg_row = square[:slots, :PAD]
    reg_row = jnp.concatenate([reg_row] * heads, axis=1)
    reg_col = square[...].T[:PAD, :slots]
    real = lax.broadcasted_iota(jnp.int32, (PAD, heads * PAD), 0) < WT
    for w in range(slots):
        same = reg_col[:, w : w + 1] == reg_row[w : w + 1, :]
        mask[w] = jnp.where(real, jnp.where(same, 0.0, -100.0), -1e30)
    def cross(ch):
        cy(ch).wait_recv()
        if WAY_IN[ch] == "C":
            for j in range(2):
                cx(ch, j).start()

    for ch in first:
        cross(ch)

    def wide(i):
        return jnp.concatenate([vg[tt, i : i + 1, :] for tt in range(nt)], axis=1)

    def put_small(i, value):
        for tt in range(nt):
            small[tt, i : i + 1, :] = value[:, tt * LANES : (tt + 1) * LANES]

    def spread(source, target):
        for tt in range(nt):
            xs[:, tt * LANES : (tt + 1) * LANES] = source[tt].astype(F32)
        zero = jnp.zeros((PAD - WT, C), F32)
        for w in range(slots):
            target[w * PAD : w * PAD + WT, :] = xs[w * WT : (w + 1) * WT, :]
            target[w * PAD + WT : (w + 1) * PAD, :] = zero

    def gather(source, target):
        for w in range(slots):
            xs[w * WT : (w + 1) * WT, :] = source[w * PAD : w * PAD + WT, :]
        for tt in range(nt):
            target[tt] = xs[:, tt * LANES : (tt + 1) * LANES].astype(BF16)

    def each(body, init=0):
        def step(i, carry):
            return body(i, pl.ds(pl.multiple_of(i * half, half), half), carry)

        return lax.fori_loop(0, nhalf, step, init)

    def weight(ch, tt, start=0, size=CW):
        return gw[ch, tt, :, :, :, start : start + size].reshape(C, size)

    def put_grad(ch, tt, value):
        dv[ch, tt] = value.astype(BF16).reshape(dv.shape[2:])

    def tok_all(i):
        return [tok_copy(i, d) for d in range(3)]

    def await_tok(i):
        await_bytes((xg, cg, vg)[i].at[pl.ds(0, 3)], coming("tok", i))

    def await_name(name):
        kind, ch = name[:-1], int(name[-1])
        if kind == "x":
            await_bytes(r3.at[0], coming("ax", ch))
        elif kind == "ay":
            await_bytes(r3.at[0] if ch else gw.at[0, 0], coming("ay", ch))
        elif kind == "z":
            az_await(ch)
        elif kind in ("xo", "xt"):
            bx(ch, int(kind == "xt")).wait_recv()
        elif kind == "yo":
            by(ch).wait_recv()
        elif kind in ("k0", "k1"):
            ac(ch, int(kind == "k1")).wait_recv()
        elif kind in ("r0", "r1"):
            kc(ch, int(kind == "r1")).wait_recv()
        elif kind == "ya":
            ya(ch).wait_recv()
        elif kind == "xa":
            xa(ch).wait_recv()
        elif kind in ("xbt", "xbo"):
            xb(ch, int(kind == "xbo")).wait_recv()
        elif kind == "yb":
            yb2(ch).wait_recv()
        elif kind == "zc":
            await_bytes(rzc.at[0], coming("zc", ch))
        else:
            assert kind == "xc"
            await_bytes(gw.at[0, 0, 0], coming("xc", ch))

    def own_of(ch):
        return ("z%d" if WAY_IN[ch] == "C" else "xo%d") % ch

    def other_y_of(ch):
        return {"A": "yo%d", "B": "xt%d", "C": "z%d", "E": "xt%d"}[WAY_IN[ch]] % ch

    def waits_of(entry):
        fixed = {
            "use_a0": ("x1", "x0"), "use_a1": ("k01", "k00"), "use_a2": ("xt1", "ay0"),
            "use_a3": ("k11", "k10"), "yx1": ("ay1",), "c11": ("xt1",), "c10": ("ay0",),
            "ay0": ("x0",), "end": (), "cot": (), "yout": (), "g": (),
        }
        if entry in fixed:
            return fixed[entry]
        if entry.startswith("use_m"):
            k = int(entry[-1])
            chs, m = ((2, 4) if k < nt else (3, 5)), MLP_ORDER[k % nt]
            names = {0: own_of, 1: "k0{}".format, 2: other_y_of, 3: "k1{}".format}[m]
            return tuple(names(ch) for ch in chs)
        kind, ch = entry[:-1], int(entry[-1])
        way = WAY_OUT[ch]
        names = {
            "az": (), "zx": ("z",), "zy": ("z",), "zt": ("z",), "yx": ("yo",), "xy": ("xo",),
            "o1": ("r0",), "oo": ("r1",), "ot": ("r0",),
            "o2": {"A": ("ya", "r1"), "B": ("xbt",), "C": ("zc",)}[way],
            "o3": {"A": ("xa",), "B": ("yb",) if ch < 2 else ("xbo", "yb"), "C": ("xc",)}[way],
        }
        if kind == "c0":
            return (own_of(ch),)
        if kind == "c1":
            return (other_y_of(ch),)
        return tuple(f"{n}{ch}" for n in names[kind])

    first_use = {}
    for item in plan_order(PLAN):
        for name in waits_of(item):
            first_use.setdefault(name, item)

    def arrive(entry):
        for name in waits_of(entry):
            if first_use[name] == entry:
                await_name(name)

    def act(entry):
        arrive(entry)
        if entry == "cot":
            for copy in tok_all(1):
                copy.start()
            return
        if entry in ("yout", "g"):
            for d in range(3):
                out_copy(int(entry == "g"), d).start()
            return
        kind, ch = entry[:-1], int(entry[-1])
        way = WAY_OUT[ch]
        if kind == "ay":
            for zz in range(nz):
                ay(ch, zz, zz).start()
        elif kind == "az":
            if WAY_IN[ch] == "C":
                await_bytes(gw.at[0, 0, 0], coming("cx", ch))
            az_start(ch)
        elif kind == "zx":
            bx(ch, 0).start()
        elif kind in ("zt", "yx"):
            bx(ch, 1).start()
        elif kind in ("zy", "xy"):
            by(ch).start()
        elif kind in ("c0", "c1"):
            ac(ch, int(kind == "c1")).start()
        elif kind == "o1":
            dv[ch, t2] = add(dv[ch, t2], rc[ch, 0])
            ya(ch).start()
        elif kind == "ot":
            dv[ch, t2] = add(dv[ch, t2], rc[ch, 0])
            if way == "B":
                xb(ch, 0).start()
            else:
                zc_start(ch, 0)
        elif kind == "oo":
            dv[ch, t] = add(dv[ch, t], rc[ch, 1])
            if way == "C":
                zc_start(ch, 1)
            elif ch < 2:
                for d in range(nz):
                    xp1(ch, d).start()
            else:
                xb(ch, 1).start()
        elif kind == "o2" and way == "A":
            value = dv[ch, t].astype(F32) + rc[ch, 1].astype(F32)
            dv[ch, t] = (value + ry[a_slot[ch]].astype(F32)).astype(BF16)
            xa(ch).start()
        elif kind == "o2" and way == "B":
            dv[ch, t2, :, x] = add(dv[ch, t2, :, x], rx[b_slot[ch], 0])
            yb2(ch).start()
        elif kind == "o2":
            for j, tt in enumerate((t2, t)):
                value = dv[ch, tt, z].astype(F32)
                for d in range(nz - 1):
                    value = value + rzc[c_slot[ch], d, j].astype(F32)
                dv[ch, tt, z] = value.astype(BF16)
                xc(ch, j).start()
        elif kind == "o3" and way == "C":
            for j, tt in enumerate((t2, t)):
                dv[ch, tt, z, x] = add(dv[ch, tt, z, x], rxc[c_slot[ch], j])
            yc(ch).start()
        elif kind == "o3" and ch < 2:
            for d in range(nz):
                zz = piece_of(d)
                xp1(ch, d).wait_recv()
                value = dv[ch, t, zz, x].astype(F32) + rx[b_slot[ch], 1, zz].astype(F32)
                dv[ch, t, zz, x] = (value + r3[ch, zz].astype(F32)).astype(BF16)
                if d < nz - 1:
                    zr_start(ch, d)
        else:
            assert kind == "o3"
            value = dv[ch, t, :, x].astype(F32) + r3[ch].astype(F32)
            if way == "B":
                value = value + rx[b_slot[ch], 1].astype(F32)
            dv[ch, t, :, x] = value.astype(BF16)
            for k in range(nz - 1):
                zr_start(ch, k)

    def last(ch):
        if WAY_OUT[ch] == "C":
            yc(ch).wait_recv()
            fin[ch] = dv[ch, t, z, x].astype(F32) + rxc[c_slot[ch], 2].astype(F32)
            return
        value = dv[ch, t, z, x].astype(F32)
        await_bytes(rz.at[0], coming("zr", ch))
        for d in range(nz - 1):
            value = value + rz[ch, d].astype(F32)
        fin[ch] = value

    def run(slot):
        for entry in PLAN.get(slot, ()):
            act(entry)

    def run_at(index, pattern, count):
        for i in range(count):
            if PLAN.get(pattern % i):

                @pl.when(index == i)
                def _(i=i):
                    run(pattern % i)

    def use_at(index, pattern, count, start=0):
        for i in range(start, count):
            if any(first_use[n] == pattern % i for n in waits_of(pattern % i)):

                @pl.when(index == i)
                def _(i=i):
                    arrive(pattern % i)

    n_live = live[0] - t * slots
    small[...] = jnp.zeros_like(small)
    own_tok.wait()
    run("h0")
    for ch in (1, 0):
        for k in range(nz - 1):
            zz, _ = far_first(nz - 2 - k)
            az_from(ch, zz)
            ax(ch, zz, k + 1).start()
            if ch == 1:
                ay(ch, zz, k + 1).start()
    for ch in early:
        if ch not in first:
            cross(ch)
    run("h1")
    await_tok(2)
    for tt in range(nt):
        bias_of(tt)
    await_tok(0)
    spread(xg, xp)
    gain1, shift1 = wide(0), wide(1)

    def start(i, at, carry):
        normed, rstd = norm(xp[at, :])
        n1[at, :] = normed
        r1[at, :] = rstd
        h = normed * gain1 + shift1
        h1[at, :] = h.astype(BF16)
        h1t[:, at] = h.T.astype(BF16)
        return carry

    each(start)
    run("h2")
    arrive("use_a0")
    ac(1, 0).start()
    ac(0, 0).start()
    run("h3")
    lane_head = lax.broadcasted_iota(jnp.int32, (PAD, LANES), 1) // HDIM
    ones = [(lane_head == h).astype(F32).astype(BF16) for h in range(heads)]

    def stack(value):
        return jnp.concatenate([value * ones[h] for h in range(heads)], axis=0)

    def pick(value):
        out = value[0:PAD]
        for h in range(1, heads):
            out = jnp.where(lane_head == h, value[h * PAD : (h + 1) * PAD], out)
        return out

    acc[...] = jnp.zeros_like(acc)

    def attend(i, carry):
        tt = group(i)

        use_at(i, "use_a%d", nt, 1)
        q = (nn(h1[...], weight(0, tt, 0, LANES)) + vg[tt, 2:3, :]) * SCALE
        qs[tt] = q.astype(BF16)
        kv = nn(h1[...], weight(1, tt))
        kvs[tt, :, :LANES] = kv[:, :LANES].astype(BF16)
        kvs[tt, :, LANES:] = (kv[:, LANES:] + vg[tt, 3:4, :]).astype(BF16)

        def window(w):
            at = pl.ds(pl.multiple_of(w * PAD, PAD), PAD)
            s = nt_dot(kvs[tt, at, :LANES], stack(qs[tt, at, :])) + rg[tt] + mask[w]
            e = jnp.exp(s - jnp.max(s, axis=0, keepdims=True))
            p = e / rowsum(e)
            probs[tt, w] = p
            att[tt, at, :] = pick(tn_dot(p.astype(BF16), kvs[tt, at, LANES:])).astype(BF16)

        def four(hh, carry):
            for j in range(slots // 2):
                window(hh * (slots // 2) + j)

            @pl.when(hh == 0)
            def _():
                run_at(i, "a%df", nt)

            return carry

        lax.fori_loop(0, 2, four, 0)
        acc[...] += nt_dot(att[tt], weight(0, tt, LANES, LANES))
        run_at(i, "a%ds", nt)
        return carry

    lax.fori_loop(0, nt, attend, 0)
    own_cot.wait()
    await_tok(1)
    spread(cg, gy)
    b_out, gain2, shift2 = wide(4), wide(5), wide(6)

    def live_rows(i):
        slot = lax.div(i * half + lax.broadcasted_iota(jnp.int32, (half, 1), 0), PAD)
        return slot < n_live

    def middle(i, at, carry):
        x1 = xp[at, :] + acc[at, :] + b_out
        xp[at, :] = x1
        normed, rstd = norm(x1)
        n2[at, :] = normed
        r2[at, :] = rstd
        h = normed * gain2 + shift2
        low[at, :] = h.astype(BF16)
        h2t[:, at] = h.T.astype(BF16)
        g = jnp.where(live_rows(i), gy[at, :], 0.0)
        gy[at, :] = g
        gkv[at, :] = g.astype(BF16)
        gyt[:, at] = g.T.astype(BF16)
        return carry

    each(middle)
    run("mid")
    acc[...] = jnp.zeros_like(acc)
    acc2[...] = jnp.zeros_like(acc2)
    def mlp(k, carry):
        s, i = lax.div(k, nt), lax.rem(k, nt)
        turn_at = MLP_ORDER[nt - 1]
        for j in range(nt - 1):
            turn_at = jnp.where(i == j, MLP_ORDER[j], turn_at)
        tt = group(turn_at)
        up, down = 2 + s, 4 + s
        use_at(k, "use_m%d", 2 * nt)

        bias = vg[tt, pl.ds(8 + 2 * s, 2), :]
        bias = jnp.concatenate([bias[0:1], bias[1:2]], axis=1)
        hidden = nn(low[...], weight(up, tt)) + bias
        act, slope = gelu_pair(hidden)
        act_low = act.astype(BF16)
        acc[...] += nt_dot(act_low, weight(down, tt))
        put_grad(down, tt, nn(gyt[...], act_low))
        grad = nn(gkv[...], weight(down, tt)) * slope
        total = rowsum(grad)
        small[tt, pl.ds(8 + 2 * s, 1), :] = total[:, :LANES]
        small[tt, pl.ds(9 + 2 * s, 1), :] = total[:, LANES:]
        grad_low = grad.astype(BF16)
        put_grad(up, tt, nn(h2t[...], grad_low))
        acc2[...] += nt_dot(grad_low, weight(up, tt))

        for when, j in ((MLP_ORDER.index(1), 1), (MLP_ORDER.index(3), 0)):

            @pl.when(i == when)
            def _(j=j):
                kc(up, j).start()
                kc(down, j).start()

        run_at(k, "m%d", 2 * nt)
        return carry

    lax.fori_loop(0, 2 * nt, mlp, 0)
    b_down = wide(7)
    zero_row = jnp.zeros((1, C), F32)

    def turn(i, at, carry):
        xp[at, :] = jnp.where(live_rows(i), xp[at, :] + acc[at, :] + b_down, 0.0)
        e, normed, g = acc2[at, :], n2[at, :], gy[at, :]
        gx = norm_back(e * gain2, normed, r2[at, :]) + g
        gy[at, :] = gx
        low[at, :] = gx.astype(BF16)
        h2t[:, at] = gx.T.astype(BF16)
        sums = (rowsum(e * normed), rowsum(e), rowsum(gx), rowsum(g))
        return tuple(p + q for p, q in zip(carry, sums))

    sums = each(turn, (zero_row,) * 4)
    put_small(5, sums[0])
    put_small(6, sums[1])
    put_small(4, sums[2])
    put_small(7, sums[3])
    gather(xp, yb)
    own_y = pltpu.make_async_copy(yb.at[t], y_all.at[t], loc.at[2])
    own_y.start()
    run("turn")
    acc[...] = jnp.zeros_like(acc)

    def back(i, carry):
        tt = group(3 - i)
        gatt[...] = nn(low[...], weight(0, tt, LANES, LANES)).astype(BF16)
        pairs[...] = jnp.zeros_like(pairs)

        def window(w):
            at = pl.ds(pl.multiple_of(w * PAD, PAD), PAD)
            q4, g4 = stack(qs[tt, at, :]), stack(gatt[at, :])
            p = probs[tt, w]
            dp = nt_dot(kvs[tt, at, LANES:], g4)
            ds = p * (dp - rowsum(p * dp))
            ds_low = ds.astype(BF16)
            gkv[at, :LANES] = nn(ds_low, q4).astype(BF16)
            gkv[at, LANES:CW] = nn(p.astype(BF16), g4).astype(BF16)
            gq[at, :] = pick(tn_dot(ds_low, kvs[tt, at, :LANES])).astype(BF16)
            return ds_low.astype(F32)

        def four(hh, carry):
            total = window(hh * (slots // 2))
            for j in range(1, slots // 2):
                total = total + window(hh * (slots // 2) + j)
            pairs[...] += total

            @pl.when(hh == 0)
            def _():
                run_at(i, "b%df", nt)

            return carry

        lax.fori_loop(0, 2, four, 0)
        gk_gv = gkv[:, :CW]
        put_grad(1, tt, nn(h1t[...], gk_gv))
        run_at(i, "b%de", nt)

        left = nn(h1t[...], gq[...]) * SCALE
        put_grad(0, tt, jnp.concatenate([left, nn(h2t[...], att[tt])], axis=1))

        @pl.when(i == 0)
        def _():
            kc(1, 0).start()
            kc(0, 0).start()

        @pl.when(i == 2)
        def _():
            kc(1, 1).start()
            kc(0, 1).start()

        run_at(i, "b%dd", nt)
        small[tt, 2:3, :] = rowsum(gq[...].astype(F32)) * SCALE
        small[tt, 3:4, :] = rowsum(gkv[:, LANES:CW].astype(F32))
        grad_q = nt_dot(gq[...], weight(0, tt, 0, LANES)) * SCALE
        acc[...] += grad_q + nt_dot(gk_gv, weight(1, tt))
        for h in range(heads):
            lanes = h // 2 * LANES
            source = pairs[:, lanes : lanes + LANES]
            for q in range(TPAD // LANES):
                where = inv[:, q * LANES : (q + 1) * LANES]
                value = take(source, jnp.maximum(where, 0) + h % 2 * PAD)
                value = jnp.where(where >= 0, value, 0.0)
                small[tt, pl.ds(12 + 2 * h + q, 1), :] = rowsum(value)

        run_at(i, "b%ds", nt)
        return carry

    lax.fori_loop(0, nt, back, 0)

    def finish(i, at, carry):
        e, normed = acc[at, :], n1[at, :]
        xp[at, :] = norm_back(e * gain1, normed, r1[at, :]) + gy[at, :]
        sums = (rowsum(e * normed), rowsum(e))
        return tuple(p + q for p, q in zip(carry, sums))

    sums = each(finish, (zero_row,) * 2)
    put_small(0, sums[0])
    put_small(1, sums[1])
    for d in range(3):
        small_t(d).start()
    gather(xp, gb)
    own_g = pltpu.make_async_copy(gb.at[t], g_all.at[t], loc.at[3])
    own_g.start()
    run("t1")
    run("t2")
    await_bytes(scr, coming("st"))
    zb[z] = small[t] + scr[0] + (scr[1] + scr[2])
    for d in range(nz - 1):
        small_z(d).start()
    run("t3")
    await_bytes(zb.at[pl.ds(0, nz - 1)], coming("sz"))
    value = zb[0]
    for zz in range(1, nz):
        value = value + zb[zz]
    sx[...] = value
    small_x().start()
    run("t4")
    run("t5")
    for ch in (2, 4, 3, 5, 1, 0):
        last(ch)
    small_x().wait_recv()
    tot[...] = sx[...] + syr[...]
    for i in range(2):
        await_bytes((yb, gb)[i].at[pl.ds(0, 3)], coming("out", i))
    for i, n in enumerate(totals):
        await_bytes(blocks(n), ss.at[i])
    three = (xg, cg, vg, yb, gb, small)
    for i, ref in enumerate(three):
        await_bytes(ref.at[pl.ds(0, 3)], ss.at[len(totals) + i])
    await_bytes(zb.at[pl.ds(0, nz - 1)], ss.at[len(totals) + 6])
    await_bytes(sx, ss.at[len(totals) + 7])
    own_y.wait()
    own_g.wait()


def block_call(nt, nz, slots, *args):
    tok, deep, heads = args[1], args[3].shape[0], args[18].shape[0]
    real = tok.shape[1]
    rows, wide = slots * PAD, heads * PAD
    piece = (nz, 2, deep, CW)
    row = (nt, real, LANES)

    def vm(shape, kind=BF16):
        return pltpu.VMEM(shape, kind)

    small = (SROWS, LANES)
    n_c = max(1, WAY_OUT.count("C"))
    return pl.pallas_call(
        functools.partial(block, nt, nz, slots),
        name="block",
        out_shape=(
            jax.ShapeDtypeStruct(row, BF16),
            jax.ShapeDtypeStruct(row, BF16),
            jax.ShapeDtypeStruct((NCH, deep, CW), F32),
            jax.ShapeDtypeStruct(small, F32),
        ),
        in_specs=[SM] + [ANY] * 20,
        out_specs=(ANY, ANY, VM, VM),
        scratch_shapes=[vm(arg.shape, arg.dtype) for arg in args[9:]]
        + [
            vm(row),
            vm(row),
            vm((NCH, nt) + piece),
            vm((nt,) + small, F32),
            vm((nt, PAD, wide), F32),
            vm((NCH, nt) + piece),
            vm((NCH, 2) + piece),
            vm((max(1, WAY_OUT.count("A")),) + piece),
            vm((WAY_OUT.count("B"), 2, nz, deep, CW)),
            vm((NCH, nz, deep, CW)),
            vm((NCH, nz - 1, deep, CW)),
            vm((n_c, nz - 1, 2, 2, deep, CW)),
            vm((n_c, 3, deep, CW)),
            vm((3,) + small, F32),
            vm(small, F32),
            vm(small, F32),
            vm((nz,) + small, F32),
            vm((nt,) + small, F32),
            vm(row),
            vm(row),
            vm((LANES, LANES), F32),
            vm((slots, PAD, wide), F32),
            vm((PAD, TPAD), jnp.int32),
            vm((real, C), F32),
            vm((rows, C), F32),
            vm((rows, C), F32),
            vm((rows, C)),
            vm((C, rows)),
            vm((C, rows)),
            vm((C, rows)),
            vm((nt, rows, LANES)),
            vm((nt, rows, CW)),
            vm((nt, slots, PAD, wide), F32),
            vm((nt, rows, LANES)),
            vm((rows, C), F32),
            vm((rows, C), F32),
            vm((rows, C), F32),
            vm((rows, 1), F32),
            vm((rows, C), F32),
            vm((rows, 1), F32),
            vm((rows, C)),
            vm((rows, C)),
            vm((rows, LANES)),
            vm((rows, LANES)),
            vm((PAD, wide), F32),
            DMA((4,)),
            DMA((14,)),
            DMA((len(arrival_table(nz)),)),
            DMA((len(send_table(nt, nz)[1]) + 8,)),
        ],
        compiler_params=pltpu.CompilerParams(
            collective_id=0, has_side_effects=True, vmem_limit_bytes=60 * 2**20
        ),
    )(*args)


def spell(n, *refs):
    ins, outs, refs = refs[:4], refs[4 : 4 + n], refs[4 + n :]
    (y_in, g_in, fin, tot), refs = refs[:4], refs[4:]
    held, (get, put) = refs[:n], refs[n:]
    steps = ins[0].shape[0]
    loads = [pltpu.make_async_copy(ins[2], fin, get.at[0])]
    loads.append(pltpu.make_async_copy(ins[3], tot, get.at[1]))
    for i in range(steps):
        for j, ref in enumerate((y_in, g_in)):
            loads.append(
                pltpu.make_async_copy(ins[j].at[i], ref.at[i], get.at[2 + 2 * i + j])
            )
    for copy in loads:
        copy.start()
    loads[0].wait()
    loads[1].wait()
    spell_rest(fin, tot, *held[2:])
    like = {}
    for k in range(2, n):
        slot = 2 + list(like).index(held[k].shape) if held[k].shape in like else 2 + len(like)
        like.setdefault(held[k].shape, []).append(k)
        pltpu.make_async_copy(held[k], outs[k], put.at[slot]).start()
    for i in range(steps):
        for j, ref in enumerate((y_in, g_in)):
            loads[2 + 2 * i + j].wait()
            held[j][i] = ref[i].astype(F32)
            pltpu.make_async_copy(held[j].at[i], outs[j].at[i], put.at[j]).start()
    for j in range(2):
        pltpu.make_async_copy(held[j], outs[j], put.at[j]).wait()
    for slot, (shape, ks) in enumerate(like.items()):
        size = len(ks) * shape[0] * shape[1]
        if len(ks) == 1:
            ref = held[ks[0]]
        elif shape[0] == 1:
            ref = tot.at[pl.ds(0, len(ks))]
        else:
            ref = fin.at[pl.ds(0, size // (fin.shape[1] * fin.shape[2]))]
        pltpu.make_async_copy(ref, ref, put.at[2 + slot]).wait()


def spell_rest(fin, tot, *outs):
    (
        d_g1, d_s1, d_wq, d_wk, d_wv, d_bq, d_bv, d_wo, d_bo, d_g2, d_s2, d_wh, d_bh,
        d_wd, d_bd, d_tab,
    ) = outs
    d_wq[...] = fin[0, :, :LANES]
    d_wk[...] = fin[1, :, :LANES]
    d_wv[...] = fin[1, :, LANES:]
    d_wo[...] = fin[0, :, LANES:]
    for s in range(2):
        d_wh[:, s * CW : (s + 1) * CW] = fin[2 + s]
        d_wd[:, s * CW : (s + 1) * CW] = fin[4 + s]
    for i, ref in enumerate((d_g1, d_s1, d_bq, d_bv, d_bo, d_g2, d_s2, d_bd)):
        ref[...] = tot[i : i + 1, :]
    d_bh[...] = tot[8:12, :]
    for h in range(d_tab.shape[0]):
        d_tab[h : h + 1, :LANES] = tot[12 + 2 * h : 13 + 2 * h]
        d_tab[h : h + 1, LANES:] = tot[13 + 2 * h : 14 + 2 * h, : TABLE - LANES]


def spell_call(outs, *args):
    n, steps = len(outs), args[0].shape[0]
    held = [pltpu.VMEM(v.shape, v.dtype) for v in args + outs]
    return pl.pallas_call(
        functools.partial(spell, n),
        name="spell",
        out_shape=outs,
        in_specs=[ANY] * 4,
        out_specs=(ANY,) * n,
        scratch_shapes=held + [DMA((2 + 2 * steps,)), DMA((2 + len({v.shape for v in outs[2:]}),))],
        compiler_params=pltpu.CompilerParams(vmem_limit_bytes=60 * 2**20),
    )(*args)


def per_device(
    nt, na, tokens, gain_one, shift_one, w_query, w_key, w_value, b_query, b_value, w_out, b_out,
    gain_two, shift_two, w_hidden, b_hidden, w_down, b_down, bias_table, rel_index, region,
    win_count, cotangent,
):
    slots = region.shape[0] // nt
    cut = (nt, slots * WT, LANES)
    vectors = [gain_one, shift_one, b_query, b_value, b_out, gain_two, shift_two, b_down]
    parts = block_call(
        nt, na // 2, slots,
        win_count, tokens.reshape(cut), cotangent.reshape(cut),
        w_query, w_key, w_value, w_out.T, w_hidden, w_down.T,
        *[v.reshape(1, LANES) for v in vectors],
        b_hidden.reshape(-1, LANES), bias_table.T, rel_index, region,
    )

    def out(like, shape=None):
        return jax.ShapeDtypeStruct(shape or like.shape, F32)

    one = (1, LANES)
    shapes = (
        out(tokens, cut), out(tokens, cut), out(gain_one, one), out(gain_one, one), out(w_query),
        out(w_key), out(w_value), out(b_query, one), out(b_value, one), out(w_out, w_out.shape[::-1]),
        out(b_out, one), out(gain_two, one), out(shift_two, one), out(w_hidden),
        out(b_hidden, (b_hidden.shape[0] // LANES, LANES)), out(w_down, w_down.shape[::-1]),
        out(b_down, one), out(bias_table, bias_table.shape[::-1]),
    )
    likes = (
        tokens, tokens, gain_one, gain_one, w_query, w_key, w_value, b_query, b_value, w_out,
        b_out, gain_two, shift_two, w_hidden, b_hidden, w_down, b_down, bias_table,
    )
    values = spell_call(shapes, *parts)
    turned = (9, 15, 17)
    return tuple(
        v.T if i in turned else v.reshape(like.shape)
        for i, (v, like) in enumerate(zip(values, likes))
    )


def solution(mesh):
    return jax.shard_map(
        functools.partial(per_device, mesh.shape["ta"], mesh.shape["wa"]),
        mesh=mesh,
        in_specs=(
            P("wa", "ta"),
            P("ta"),
            P("ta"),
            P("wa", "ta"),
            P("wa", "ta"),
            P("wa", "ta"),
            P("ta"),
            P("ta"),
            P("ta", "wa"),
            P("ta"),
            P("ta"),
            P("ta"),
            P("wa", "ta"),
            P("ta"),
            P("ta", "wa"),
            P("ta"),
            P(None, "ta"),
            P(),
            P("wa", None),
            P("wa"),
            P("wa", "ta"),
        ),
        out_specs=(
            P("wa", "ta"),
            P("wa", "ta"),
            P("ta"),
            P("ta"),
            P("wa", "ta"),
            P("wa", "ta"),
            P("wa", "ta"),
            P("ta"),
            P("ta"),
            P("ta", "wa"),
            P("ta"),
            P("ta"),
            P("ta"),
            P("wa", "ta"),
            P("ta"),
            P("ta", "wa"),
            P("ta"),
            P(None, "ta"),
        ),
        check_vma=False,
    )
```

```python
import functools

import jax
import jax.numpy as jnp
from jax import lax
from jax.experimental import pallas as pl
from jax.experimental.pallas import tpu as pltpu
from jax.sharding import PartitionSpec as P

C = 512
HDIM = 32
WT = 49
PAD = 64
TABLE = 169
TPAD = 256
NCH = 6
CW = 256
LANES = 128
SROWS = 24
SCALE = HDIM ** (-0.5)
EPS = 1e-05
F32 = jnp.float32
BF16 = jnp.bfloat16
MESH = pl.DeviceIdType.MESH
ANY = pl.BlockSpec(memory_space=pl.ANY)
VM = pl.BlockSpec(memory_space=pltpu.VMEM)
SM = pl.BlockSpec(memory_space=pltpu.SMEM)
DMA = pltpu.SemaphoreType.DMA


WAY_IN = ("A", "B", "A", "B", "E", "C")
WAY_OUT = ("B", "B", "B", "C", "A", "B")
MLP_ORDER = (0, 1, 3, 2)
PLAN = {
    "h0": ("az2",),
    "h1": ("az4", "yx1",),
    "h2": ("zx2", "ay0",),
    "h3": ("az3",),
    "a0f": ("c11", "cot",),
    "a1f": ("zt4", "az5", "xy2", "zx4",),
    "a1s": ("c02", "zy3",),
    "a3f": ("zx3",),
    "a3s": ("c04",),
    "m1": ("yx3", "c03",),
    "m2": ("c15",),
    "m3": ("c05",),
    "m4": ("o14", "c13", "ot2", "oo2",),
    "m7": ("o22", "oo3", "oo5",),
    "turn": ("ot3",),
    "b0f": ("ot5",),
    "b0d": ("o24",),
    "b0s": ("o32",),
    "b1d": ("ot1", "o25", "ot0",),
    "b2d": ("o34",),
    "b3f": ("o21",),
    "b3d": ("oo0",),
    "b3s": ("o35",),
    "t1": ("o20", "o23",),
    "t2": ("g", "o31",),
    "t3": ("o33", "o30",),
    "m0": ("c12", "c14",),
    "b3e": ("oo1",),
    "a2f": ("c10",),
    "b1f": ("yout",),
}


def plan_order(sched):
    out = list(sched.get("h0", ())) + list(sched.get("h1", ()))
    out += list(sched.get("h2", ())) + ["use_a0"]
    out += sched.get("h3", ())
    for i in range(4):
        out += ([f"use_a{i}"] if i else []) + list(sched.get(f"a{i}f", ()))
        out += sched.get(f"a{i}s", ())
    out += list(sched.get("mid", ()))
    for k in range(8):
        out += [f"use_m{k}"] + list(sched.get(f"m{k}", ()))
    out += sched.get("turn", ())
    for i in range(4):
        for part in "feds":
            out += sched.get(f"b{i}{part}", ())
    for i in range(1, 6):
        out += sched.get(f"t{i}", ())
    return out + ["end"]


def flip(bit, by):
    return bit + by - 2 * bit * by


def add(left, right):
    return (left.astype(F32) + right.astype(F32)).astype(BF16)


def nn(left, right):
    return jnp.dot(left, right, preferred_element_type=F32)


def nt_dot(left, right):
    return lax.dot_general(left, right, (((1,), (1,)), ((), ())), preferred_element_type=F32)


def tn_dot(left, right):
    return lax.dot_general(left, right, (((0,), (0,)), ((), ())), preferred_element_type=F32)


def norm(value):
    mean = jnp.mean(value, axis=1, keepdims=True)
    spread = jnp.mean(value * value, axis=1, keepdims=True) - mean * mean
    rstd = lax.rsqrt(spread + EPS)
    return (value - mean) * rstd, rstd


def norm_back(scaled, normed, rstd):
    first = jnp.mean(scaled, axis=1, keepdims=True)
    second = jnp.mean(scaled * normed, axis=1, keepdims=True)
    return rstd * (scaled - first - normed * second)


def gelu_pair(u):
    cdf = 0.5 + 0.5 * lax.erf(u * (0.5**0.5))
    pdf = jnp.exp(-0.5 * u * u) * ((2.0 * jnp.pi) ** -0.5)
    return u * cdf, cdf + u * pdf


def rowsum(value):
    return jnp.sum(value, axis=0, keepdims=True)


def arrival_table(nz):
    keys = [("kc", ch, j) for ch in range(NCH) for j in range(2)]
    keys += [("ac", ch, j) for ch in range(NCH) for j in range(2)]
    keys += [("az", ch, d) for ch in range(2) for d in range(nz - 1)]
    keys += [("tok", i) for i in range(3)] + [("out", i) for i in range(2)]
    keys += [(kind, ch) for kind in ("ax", "ay") for ch in range(2)]
    keys += [("bx", 1, 1), ("st",), ("sz",), ("sx",)]
    for ch in range(2, NCH):
        keys += [("az", ch), ("by", ch)]
        if WAY_IN[ch] == "C":
            keys.append(("cx", ch))
        else:
            keys += [("bx", ch, j) for j in range(1 if WAY_IN[ch] == "A" else 2)]
    for ch in range(NCH):
        if WAY_OUT[ch] == "C":
            keys += [("zc", ch), ("xc", ch), ("yc", ch)]
            continue
        keys += [("zr", ch), ("q", ch), ("p", ch, 0)]
        if WAY_OUT[ch] == "B":
            keys += [("px", ch, d) for d in range(nz)] if ch < 2 else [("p", ch, 1)]
    return {key: i for i, key in enumerate(keys)}


def send_table(nt, nz):
    whole = {("kc", ch, j): 2 * nz for ch in range(NCH) for j in range(2)}
    whole.update({("ac", ch, j): 2 * nz for ch in range(NCH) for j in range(2)})
    sends = {}
    for ch in range(2):
        sends.update({("az", ch, d, 0): 1 for d in range(nz - 1)})
        sends.update({("ax", ch, i): 1 for i in range(nz)})
        sends.update({("ay", ch, i): 2 - ch for i in range(nz)})
        sends.update({("px", ch, d): 1 for d in range(nz)})
    sends["bx", 1, 1] = nz
    for ch in range(2, NCH):
        way = WAY_IN[ch]
        both = 2 if way in "CE" else 1
        size = 2 if way == "C" else 1
        sends.update({("az", ch, d, j): size for d in range(nz - 1) for j in range(both)})
        sends["by", ch] = {"A": 2 * nz, "B": nz, "C": 1, "E": 1}[way]
        sends.update({("bx", ch, j): 1 if way == "C" else nz for j in range(1 + (way != "A"))})
    for ch in range(NCH):
        way = WAY_OUT[ch]
        if way == "C":
            sends.update({("zc", ch, d, j): 2 for d in range(nz - 1) for j in range(2)})
            sends.update({("xc", ch, j): 1 for j in range(3)})
            continue
        sends.update({("zr", ch, d): 1 for d in range(nz - 1)})
        sends["q", ch] = nz
        sends["p", ch, 0] = 2 * nz if way == "A" else nz
        if way == "B" and ch > 1:
            sends["p", ch, 1] = nz
    order = sorted(sends, key=lambda key: -sends[key])
    left = sum(sends.values())
    groups, totals = {key: 0 for key in whole}, [sum(whole.values())]
    for unit, most in ((2 * nz * nt, NCH), (2 * nz, nt), (2, nz), (1, 1)):
        goal = unit * min(most, left // unit)
        if goal:
            total = 0
            while total < goal:
                key = order.pop(0)
                total += sends[key]
                groups[key] = len(totals)
            assert total == goal
            totals.append(total)
            left -= total
    assert not order
    return groups, totals


def block(nt, nz, slots, *refs):
    live, tok, cot, wq, wk, wv, wo, wh, wd = refs[:9]
    outside, refs = refs[9:21], refs[21:]
    inside, refs = refs[4:16], refs[:4] + refs[16:]
    g1, s1, bq, bv, bo, g2, s2, bd, bh, tab, rel, reg = inside
    (
        y_all, g_all, fin, tot,
        xg, cg, gw, vg, rg, dv, rc, ry, rx, r3, rz, rzc, rxc, scr, syr, sx, zb, small, yb, gb, square, mask, inv,
        xs, xp, gy, h1, h1t, h2t, gyt, qs, kvs, probs, att, acc, acc2, n1, r1, n2, r2, low, gkv, gq, gatt,
        pairs,
        loc, ld, rs, ss,
    ) = refs
    heads = LANES // HDIM
    rows = slots * PAD
    half = 2 * PAD
    nhalf = rows // half
    a, t = lax.axis_index("wa"), lax.axis_index("ta")
    x, z, c, y = lax.rem(a, 2), lax.div(a, 2), lax.rem(t, 2), lax.div(t, 2)

    def group(m):
        return 2 * flip(y, m // 2 if isinstance(m, int) else lax.div(m, 2)) + flip(
            c, m % 2 if isinstance(m, int) else lax.rem(m, 2)
        )

    t1, t2, t3 = group(1), group(2), group(3)
    xpeer, ypeer, cpeer = (z * 2 + (1 - x), t), (a, t2), (a, t1)
    zs = [(lax.rem(z + d, nz) * 2 + x, t) for d in range(1, nz)]
    ts = [(a, tt) for tt in (t1, t2, t3)]
    peers = zs + ts + [xpeer]
    barrier = pltpu.get_barrier_semaphore()
    for peer in peers:
        pl.semaphore_signal(barrier, inc=1, device_id=peer, device_id_type=MESH)

    arrival, (group_of, totals) = arrival_table(nz), send_table(nt, nz)

    def coming(*key):
        return rs.at[arrival[key]]

    def going(*key):
        return ss.at[group_of[key]]

    def blocks(n):
        for unit, ref in ((2 * nz * nt, gw), (2 * nz, gw.at[0]), (2, gw.at[0, 0])):
            if n % unit == 0:
                return ref.at[pl.ds(0, n // unit)]
        assert n == 1
        return gw.at[0, 0, 0, 0]

    def await_bytes(ref, sem):
        pltpu.make_async_copy(ref, ref, sem).wait()

    def far(src, dst, send, recv, peer):
        return pltpu.make_async_remote_copy(
            src_ref=src, dst_ref=dst, send_sem=send, recv_sem=recv, device_id=peer,
            device_id_type=MESH,
        )

    def tok_copy(i, d):
        src, dst = ((tok, xg), (cot, cg), (vg, vg))[i]
        peer = ts[d]
        src = src.at[peer[1]] if i < 2 else src.at[t]
        return far(src, dst.at[t], ss.at[len(totals) + i], coming("tok", i), peer)

    def out_copy(i, d):
        src, dst = ((yb, y_all), (gb, g_all))[i]
        peer = ts[d]
        return far(src.at[peer[1]], dst.at[t], ss.at[len(totals) + 3 + i], coming("out", i), peer)

    def az_await(ch):
        n = (nz - 1) * {"A": 1, "B": 1, "C": 4, "E": 2}[WAY_IN[ch]]
        size = n // (nz - 1)
        ref = rz.at[0] if size == 1 else rzc.at[0, :, :, 0] if size == 2 else rzc.at[0]
        await_bytes(ref, coming("az", ch))

    def az_from(ch, zz):
        d = lax.rem(z - zz + nz, nz) - 1
        await_bytes(gw.at[ch, t, z, x], rs.at[arrival["az", ch, 0] + d])

    def far_first(k):
        rising = k + jnp.where(z > k, 0, 1)
        falling = nz - 1 - k - jnp.where(z < nz - 1 - k, 0, 1)
        zz = jnp.where(2 * z < nz, falling, rising)
        return zz, lax.rem(zz - z + nz, nz) - 1

    def az_start(ch):
        for k in range(nz - 1):
            zz, d = far_first(k)
            for j in range(2 if WAY_IN[ch] in "CE" else 1):
                far_t = t2 if j else t
                ref = gw.at[ch, far_t, z] if WAY_IN[ch] == "C" else gw.at[ch, far_t, z, x]
                there = rs.at[arrival["az", ch, 0] + d] if ch < 2 else coming("az", ch)
                far(ref, ref, going("az", ch, k, j), there, (zz * 2 + x, t)).start()

    def zr_start(ch, k):
        zz, d = far_first(k)
        src = dv.at[ch, t, zz, x]
        far(src, rz.at[ch, d], going("zr", ch, k), coming("zr", ch), (zz * 2 + x, t)).start()

    def ax(ch, zz, i):
        ref = gw.at[ch, t, zz, x]
        return far(ref, ref, going("ax", ch, i), coming("ax", ch), xpeer)

    def ay(ch, zz, i):
        ref = gw.at[ch, t, zz] if ch == 0 else gw.at[ch, t, zz, x]
        return far(ref, ref, going("ay", ch, i), coming("ay", ch), ypeer)

    def bx(ch, j):
        ref = gw.at[ch, t2 if j else t, :, x]
        return far(ref, ref, going("bx", ch, j), coming("bx", ch, j), xpeer)

    def by(ch):
        ref = gw.at[ch, t] if WAY_IN[ch] == "A" else gw.at[ch, t, :, x]
        return far(ref, ref, going("by", ch), coming("by", ch), ypeer)

    def cy(ch):
        ref = gw.at[ch, t, z, x]
        return far(ref, ref, going("by", ch), coming("by", ch), ypeer)

    def cx(ch, j):
        ref = gw.at[ch, t2 if j else t, z, x]
        return far(ref, ref, going("bx", ch, j), coming("cx", ch), xpeer)

    def ac(ch, j):
        ref = gw.at[ch, t2 if j else t]
        return far(ref, ref, going("ac", ch, j), coming("ac", ch, j), cpeer)

    def kc(ch, j):
        return far(dv.at[ch, t1 if j else t3], rc.at[ch, j], ss.at[0], rs.at[ch * 2 + j], cpeer)

    a_slot = {ch: i for i, ch in enumerate(c for c in range(NCH) if WAY_OUT[c] == "A")}
    b_slot = {ch: i for i, ch in enumerate(c for c in range(NCH) if WAY_OUT[c] == "B")}
    c_slot = {ch: i for i, ch in enumerate(c for c in range(NCH) if WAY_OUT[c] == "C")}

    def ya(ch):
        return far(dv.at[ch, t2], ry.at[a_slot[ch]], going("p", ch, 0), coming("p", ch, 0), ypeer)

    def xa(ch):
        return far(dv.at[ch, t, :, 1 - x], r3.at[ch], going("q", ch), coming("q", ch), xpeer)

    def piece_of(d):
        return far_first(d)[0] if d < nz - 1 else z

    def xp1(ch, d):
        zz = piece_of(d)
        src, dst = dv.at[ch, t, zz, 1 - x], rx.at[b_slot[ch], 1, zz]
        return far(src, dst, going("px", ch, d), coming("px", ch, d), xpeer)

    def xb(ch, j):
        src = dv.at[ch, t if j else t2, :, 1 - x]
        return far(src, rx.at[b_slot[ch], j], going("p", ch, j), coming("p", ch, j), xpeer)

    def yb2(ch):
        return far(dv.at[ch, t2, :, x], r3.at[ch], going("q", ch), coming("q", ch), ypeer)

    def zc_start(ch, j):
        i = c_slot[ch]
        for k in range(nz - 1):
            zz, d = far_first(k)
            src, peer = dv.at[ch, t if j else t2, zz], (zz * 2 + x, t)
            far(src, rzc.at[i, d, j], going("zc", ch, k, j), coming("zc", ch), peer).start()

    def xc(ch, j):
        src, i = dv.at[ch, t if j else t2, z, 1 - x], c_slot[ch]
        return far(src, rxc.at[i, j], going("xc", ch, j), coming("xc", ch), xpeer)

    def yc(ch):
        i = c_slot[ch]
        return far(dv.at[ch, t2, z, x], rxc.at[i, 2], going("xc", ch, 2), coming("yc", ch), ypeer)

    def small_t(d):
        return far(small.at[ts[d][1]], scr.at[d], ss.at[len(totals) + 5], coming("st"), ts[d])

    def small_z(d):
        return far(zb.at[z], zb.at[z], ss.at[len(totals) + 6], coming("sz"), zs[d])

    def small_x():
        return far(sx, syr, ss.at[len(totals) + 7], coming("sx"), xpeer)

    def lanes(ch, i, size):
        return gw.at[ch, t, z, x, :, pl.ds(i * size, size)]

    loads = [(wq, lanes(0, 0, LANES), 0), (wo, lanes(0, 1, LANES), 0)]
    loads += [(wk, lanes(1, 0, LANES), 0), (wv, lanes(1, 1, LANES), 0)]
    for i in range(2):
        loads += [(wh.at[:, pl.ds(i * CW, CW)], gw.at[2 + i, t, z, x], 1)]
        loads += [(wd.at[:, pl.ds(i * CW, CW)], gw.at[4 + i, t, z, x], 1)]
    loads += [(src, dst, 2 + i) for i, (src, dst) in enumerate(zip(outside, inside))]
    for src, dst, i in loads:
        pltpu.make_async_copy(src, dst, ld.at[i]).start()
    await_bytes(gw.at[0, 0, 0], ld.at[0])
    await_bytes(gw.at[0, 0, pl.ds(0, 2)], ld.at[1])
    for src, dst, i in loads[8:]:
        pltpu.make_async_copy(src, dst, ld.at[i]).wait()
    for i, ref in enumerate((g1, s1, bq, bv, bo, g2, s2, bd)):
        vg[t, i : i + 1, :] = ref[...]
    vg[t, 8:12, :] = bh[...]
    for h in range(heads):
        vg[t, 12 + 2 * h : 13 + 2 * h, :] = tab[h : h + 1, :LANES]
        vg[t, 13 + 2 * h : 14 + 2 * h, : TABLE - LANES] = tab[h : h + 1, LANES:]
        vg[t, 13 + 2 * h : 14 + 2 * h, TABLE - LANES :] = jnp.zeros((1, TPAD - TABLE), F32)
    vg[t, 12 + 2 * heads :, :] = jnp.zeros((SROWS - 12 - 2 * heads, LANES), F32)
    pl.semaphore_wait(barrier, len(peers))
    own_tok = pltpu.make_async_copy(tok.at[t], xg.at[t], loc.at[0])
    own_cot = pltpu.make_async_copy(cot.at[t], cg.at[t], loc.at[1])
    own_tok.start()
    own_cot.start()
    early = [ch for ch in range(2, NCH) if WAY_IN[ch] in "CE"]
    first = [ch for ch in early if f"az{ch}" in PLAN.get("h0", ())]
    for ch in first:
        cy(ch).start()
    for d in range(3):
        tok_copy(2, d).start()
    az_start(1)
    ax(1, z, 0).start()
    ay(1, z, 0).start()
    az_start(0)
    ax(0, z, 0).start()
    for d in range(3):
        tok_copy(0, d).start()
    for ch in early:
        if ch not in first:
            cy(ch).start()
    square[...] = jnp.zeros_like(square)
    square[:WT, :WT] = rel[...].astype(F32)
    rel_t = square[...].T[:PAD, :PAD]
    pick_at = jnp.concatenate([rel_t, rel_t], axis=1).astype(jnp.int32)
    lane = lax.broadcasted_iota(jnp.int32, (PAD, LANES), 1)
    low_at, high_at = jnp.minimum(pick_at, LANES - 1), jnp.maximum(pick_at - LANES, 0)

    def take(value, at):
        return jnp.take_along_axis(value, at, axis=1, mode="promise_in_bounds")

    def entry(tt, h):
        first = jnp.broadcast_to(vg[tt, 12 + 2 * h : 13 + 2 * h, :], (PAD, LANES))
        second = jnp.broadcast_to(vg[tt, 13 + 2 * h : 14 + 2 * h, :], (PAD, LANES))
        return jnp.where(pick_at < LANES, take(first, low_at), take(second, high_at))

    def bias_of(tt):
        for q in range(heads // 2):
            rg[tt, :, q * LANES : (q + 1) * LANES] = jnp.where(
                lane < PAD, entry(tt, 2 * q), entry(tt, 2 * q + 1)
            )

    number = lax.broadcasted_iota(jnp.int32, (PAD, TPAD), 1).astype(F32)
    found = jnp.full((PAD, TPAD), -1.0, F32)
    for i in range(WT):
        found = jnp.where(rel_t[:, i : i + 1] == number, float(i), found)
    inv[...] = found.astype(jnp.int32)
    square[...] = jnp.zeros_like(square)
    mine = reg[pl.ds(pl.multiple_of(t * slots, slots), slots), :]
    square[:slots, :WT] = mine.astype(F32)
    reg_row = square[:slots, :PAD]
    reg_row = jnp.concatenate([reg_row] * heads, axis=1)
    reg_col = square[...].T[:PAD, :slots]
    real = lax.broadcasted_iota(jnp.int32, (PAD, heads * PAD), 0) < WT
    for w in range(slots):
        same = reg_col[:, w : w + 1] == reg_row[w : w + 1, :]
        mask[w] = jnp.where(real, jnp.where(same, 0.0, -100.0), -1e30)
    def cross(ch):
        cy(ch).wait_recv()
        if WAY_IN[ch] == "C":
            for j in range(2):
                cx(ch, j).start()

    for ch in first:
        cross(ch)

    def wide(i):
        return jnp.concatenate([vg[tt, i : i + 1, :] for tt in range(nt)], axis=1)

    def put_small(i, value):
        for tt in range(nt):
            small[tt, i : i + 1, :] = value[:, tt * LANES : (tt + 1) * LANES]

    def spread(source, target):
        for tt in range(nt):
            xs[:, tt * LANES : (tt + 1) * LANES] = source[tt].astype(F32)
        zero = jnp.zeros((PAD - WT, C), F32)
        for w in range(slots):
            target[w * PAD : w * PAD + WT, :] = xs[w * WT : (w + 1) * WT, :]
            target[w * PAD + WT : (w + 1) * PAD, :] = zero

    def gather(source, target):
        for w in range(slots):
            xs[w * WT : (w + 1) * WT, :] = source[w * PAD : w * PAD + WT, :]
        for tt in range(nt):
            target[tt] = xs[:, tt * LANES : (tt + 1) * LANES].astype(BF16)

    def each(body, init=0):
        def step(i, carry):
            return body(i, pl.ds(pl.multiple_of(i * half, half), half), carry)

        return lax.fori_loop(0, nhalf, step, init)

    def weight(ch, tt, start=0, size=CW):
        return gw[ch, tt, :, :, :, start : start + size].reshape(C, size)

    def put_grad(ch, tt, value):
        dv[ch, tt] = value.astype(BF16).reshape(dv.shape[2:])

    def tok_all(i):
        return [tok_copy(i, d) for d in range(3)]

    def await_tok(i):
        await_bytes((xg, cg, vg)[i].at[pl.ds(0, 3)], coming("tok", i))

    def await_name(name):
        kind, ch = name[:-1], int(name[-1])
        if kind == "x":
            await_bytes(r3.at[0], coming("ax", ch))
        elif kind == "ay":
            await_bytes(r3.at[0] if ch else gw.at[0, 0], coming("ay", ch))
        elif kind == "z":
            az_await(ch)
        elif kind in ("xo", "xt"):
            bx(ch, int(kind == "xt")).wait_recv()
        elif kind == "yo":
            by(ch).wait_recv()
        elif kind in ("k0", "k1"):
            ac(ch, int(kind == "k1")).wait_recv()
        elif kind in ("r0", "r1"):
            kc(ch, int(kind == "r1")).wait_recv()
        elif kind == "ya":
            ya(ch).wait_recv()
        elif kind == "xa":
            xa(ch).wait_recv()
        elif kind in ("xbt", "xbo"):
            xb(ch, int(kind == "xbo")).wait_recv()
        elif kind == "yb":
            yb2(ch).wait_recv()
        elif kind == "zc":
            await_bytes(rzc.at[0], coming("zc", ch))
        else:
            assert kind == "xc"
            await_bytes(gw.at[0, 0, 0], coming("xc", ch))

    def own_of(ch):
        return ("z%d" if WAY_IN[ch] == "C" else "xo%d") % ch

    def other_y_of(ch):
        return {"A": "yo%d", "B": "xt%d", "C": "z%d", "E": "xt%d"}[WAY_IN[ch]] % ch

    def waits_of(entry):
        fixed = {
            "use_a0": ("x1", "x0"), "use_a1": ("k01", "k00"), "use_a2": ("xt1", "ay0"),
            "use_a3": ("k11", "k10"), "yx1": ("ay1",), "c11": ("xt1",), "c10": ("ay0",),
            "ay0": ("x0",), "end": (), "cot": (), "yout": (), "g": (),
        }
        if entry in fixed:
            return fixed[entry]
        if entry.startswith("use_m"):
            k = int(entry[-1])
            chs, m = ((2, 4) if k < nt else (3, 5)), MLP_ORDER[k % nt]
            names = {0: own_of, 1: "k0{}".format, 2: other_y_of, 3: "k1{}".format}[m]
            return tuple(names(ch) for ch in chs)
        kind, ch = entry[:-1], int(entry[-1])
        way = WAY_OUT[ch]
        names = {
            "az": (), "zx": ("z",), "zy": ("z",), "zt": ("z",), "yx": ("yo",), "xy": ("xo",),
            "o1": ("r0",), "oo": ("r1",), "ot": ("r0",),
            "o2": {"A": ("ya", "r1"), "B": ("xbt",), "C": ("zc",)}[way],
            "o3": {"A": ("xa",), "B": ("yb",) if ch < 2 else ("xbo", "yb"), "C": ("xc",)}[way],
        }
        if kind == "c0":
            return (own_of(ch),)
        if kind == "c1":
            return (other_y_of(ch),)
        return tuple(f"{n}{ch}" for n in names[kind])

    first_use = {}
    for item in plan_order(PLAN):
        for name in waits_of(item):
            first_use.setdefault(name, item)

    def arrive(entry):
        for name in waits_of(entry):
            if first_use[name] == entry:
                await_name(name)

    def act(entry):
        arrive(entry)
        if entry == "cot":
            for copy in tok_all(1):
                copy.start()
            return
        if entry in ("yout", "g"):
            for d in range(3):
                out_copy(int(entry == "g"), d).start()
            return
        kind, ch = entry[:-1], int(entry[-1])
        way = WAY_OUT[ch]
        if kind == "ay":
            for zz in range(nz):
                ay(ch, zz, zz).start()
        elif kind == "az":
            if WAY_IN[ch] == "C":
                await_bytes(gw.at[0, 0, 0], coming("cx", ch))
            az_start(ch)
        elif kind == "zx":
            bx(ch, 0).start()
        elif kind in ("zt", "yx"):
            bx(ch, 1).start()
        elif kind in ("zy", "xy"):
            by(ch).start()
        elif kind in ("c0", "c1"):
            ac(ch, int(kind == "c1")).start()
        elif kind == "o1":
            dv[ch, t2] = add(dv[ch, t2], rc[ch, 0])
            ya(ch).start()
        elif kind == "ot":
            dv[ch, t2] = add(dv[ch, t2], rc[ch, 0])
            if way == "B":
                xb(ch, 0).start()
            else:
                zc_start(ch, 0)
        elif kind == "oo":
            dv[ch, t] = add(dv[ch, t], rc[ch, 1])
            if way == "C":
                zc_start(ch, 1)
            elif ch < 2:
                for d in range(nz):
                    xp1(ch, d).start()
            else:
                xb(ch, 1).start()
        elif kind == "o2" and way == "A":
            value = dv[ch, t].astype(F32) + rc[ch, 1].astype(F32)
            dv[ch, t] = (value + ry[a_slot[ch]].astype(F32)).astype(BF16)
            xa(ch).start()
        elif kind == "o2" and way == "B":
            dv[ch, t2, :, x] = add(dv[ch, t2, :, x], rx[b_slot[ch], 0])
            yb2(ch).start()
        elif kind == "o2":
            for j, tt in enumerate((t2, t)):
                value = dv[ch, tt, z].astype(F32)
                for d in range(nz - 1):
                    value = value + rzc[c_slot[ch], d, j].astype(F32)
                dv[ch, tt, z] = value.astype(BF16)
                xc(ch, j).start()
        elif kind == "o3" and way == "C":
            for j, tt in enumerate((t2, t)):
                dv[ch, tt, z, x] = add(dv[ch, tt, z, x], rxc[c_slot[ch], j])
            yc(ch).start()
        elif kind == "o3" and ch < 2:
            for d in range(nz):
                zz = piece_of(d)
                xp1(ch, d).wait_recv()
                value = dv[ch, t, zz, x].astype(F32) + rx[b_slot[ch], 1, zz].astype(F32)
                dv[ch, t, zz, x] = (value + r3[ch, zz].astype(F32)).astype(BF16)
                if d < nz - 1:
                    zr_start(ch, d)
        else:
            assert kind == "o3"
            value = dv[ch, t, :, x].astype(F32) + r3[ch].astype(F32)
            if way == "B":
                value = value + rx[b_slot[ch], 1].astype(F32)
            dv[ch, t, :, x] = value.astype(BF16)
            for k in range(nz - 1):
                zr_start(ch, k)

    def last(ch):
        if WAY_OUT[ch] == "C":
            yc(ch).wait_recv()
            fin[ch] = dv[ch, t, z, x].astype(F32) + rxc[c_slot[ch], 2].astype(F32)
            return
        value = dv[ch, t, z, x].astype(F32)
        await_bytes(rz.at[0], coming("zr", ch))
        for d in range(nz - 1):
            value = value + rz[ch, d].astype(F32)
        fin[ch] = value

    def run(slot):
        for entry in PLAN.get(slot, ()):
            act(entry)

    def run_at(index, pattern, count):
        for i in range(count):
            if PLAN.get(pattern % i):

                @pl.when(index == i)
                def _(i=i):
                    run(pattern % i)

    def use_at(index, pattern, count, start=0):
        for i in range(start, count):
            if any(first_use[n] == pattern % i for n in waits_of(pattern % i)):

                @pl.when(index == i)
                def _(i=i):
                    arrive(pattern % i)

    n_live = live[0] - t * slots
    small[...] = jnp.zeros_like(small)
    own_tok.wait()
    run("h0")
    for ch in (1, 0):
        for k in range(nz - 1):
            zz, _ = far_first(nz - 2 - k)
            az_from(ch, zz)
            ax(ch, zz, k + 1).start()
            if ch == 1:
                ay(ch, zz, k + 1).start()
    for ch in early:
        if ch not in first:
            cross(ch)
    run("h1")
    await_tok(2)
    for tt in range(nt):
        bias_of(tt)
    await_tok(0)
    spread(xg, xp)
    gain1, shift1 = wide(0), wide(1)

    def start(i, at, carry):
        normed, rstd = norm(xp[at, :])
        n1[at, :] = normed
        r1[at, :] = rstd
        h = normed * gain1 + shift1
        h1[at, :] = h.astype(BF16)
        h1t[:, at] = h.T.astype(BF16)
        return carry

    each(start)
    run("h2")
    arrive("use_a0")
    ac(1, 0).start()
    ac(0, 0).start()
    run("h3")
    lane_head = lax.broadcasted_iota(jnp.int32, (PAD, LANES), 1) // HDIM
    ones = [(lane_head == h).astype(F32).astype(BF16) for h in range(heads)]

    def stack(value):
        return jnp.concatenate([value * ones[h] for h in range(heads)], axis=0)

    def pick(value):
        out = value[0:PAD]
        for h in range(1, heads):
            out = jnp.where(lane_head == h, value[h * PAD : (h + 1) * PAD], out)
        return out

    acc[...] = jnp.zeros_like(acc)

    def attend(i, carry):
        tt = group(i)

        use_at(i, "use_a%d", nt, 1)
        q = (nn(h1[...], weight(0, tt, 0, LANES)) + vg[tt, 2:3, :]) * SCALE
        qs[tt] = q.astype(BF16)
        kv = nn(h1[...], weight(1, tt))
        kvs[tt, :, :LANES] = kv[:, :LANES].astype(BF16)
        kvs[tt, :, LANES:] = (kv[:, LANES:] + vg[tt, 3:4, :]).astype(BF16)

        def window(w):
            at = pl.ds(pl.multiple_of(w * PAD, PAD), PAD)
            s = nt_dot(kvs[tt, at, :LANES], stack(qs[tt, at, :])) + rg[tt] + mask[w]
            e = jnp.exp(s - jnp.max(s, axis=0, keepdims=True))
            p = e / rowsum(e)
            probs[tt, w] = p
            att[tt, at, :] = pick(tn_dot(p.astype(BF16), kvs[tt, at, LANES:])).astype(BF16)

        def four(hh, carry):
            for j in range(slots // 2):
                window(hh * (slots // 2) + j)

            @pl.when(hh == 0)
            def _():
                run_at(i, "a%df", nt)

            return carry

        lax.fori_loop(0, 2, four, 0)
        acc[...] += nt_dot(att[tt], weight(0, tt, LANES, LANES))
        run_at(i, "a%ds", nt)
        return carry

    lax.fori_loop(0, nt, attend, 0)
    own_cot.wait()
    await_tok(1)
    spread(cg, gy)
    b_out, gain2, shift2 = wide(4), wide(5), wide(6)

    def live_rows(i):
        slot = lax.div(i * half + lax.broadcasted_iota(jnp.int32, (half, 1), 0), PAD)
        return slot < n_live

    def middle(i, at, carry):
        x1 = xp[at, :] + acc[at, :] + b_out
        xp[at, :] = x1
        normed, rstd = norm(x1)
        n2[at, :] = normed
        r2[at, :] = rstd
        h = normed * gain2 + shift2
        low[at, :] = h.astype(BF16)
        h2t[:, at] = h.T.astype(BF16)
        g = jnp.where(live_rows(i), gy[at, :], 0.0)
        gy[at, :] = g
        gkv[at, :] = g.astype(BF16)
        gyt[:, at] = g.T.astype(BF16)
        return carry

    each(middle)
    run("mid")
    acc[...] = jnp.zeros_like(acc)
    acc2[...] = jnp.zeros_like(acc2)
    def mlp(k, carry):
        s, i = lax.div(k, nt), lax.rem(k, nt)
        turn_at = MLP_ORDER[nt - 1]
        for j in range(nt - 1):
            turn_at = jnp.where(i == j, MLP_ORDER[j], turn_at)
        tt = group(turn_at)
        up, down = 2 + s, 4 + s
        use_at(k, "use_m%d", 2 * nt)

        bias = vg[tt, pl.ds(8 + 2 * s, 2), :]
        bias = jnp.concatenate([bias[0:1], bias[1:2]], axis=1)
        hidden = nn(low[...], weight(up, tt)) + bias
        act, slope = gelu_pair(hidden)
        act_low = act.astype(BF16)
        acc[...] += nt_dot(act_low, weight(down, tt))
        put_grad(down, tt, nn(gyt[...], act_low))
        grad = nn(gkv[...], weight(down, tt)) * slope
        total = rowsum(grad)
        small[tt, pl.ds(8 + 2 * s, 1), :] = total[:, :LANES]
        small[tt, pl.ds(9 + 2 * s, 1), :] = total[:, LANES:]
        grad_low = grad.astype(BF16)
        put_grad(up, tt, nn(h2t[...], grad_low))
        acc2[...] += nt_dot(grad_low, weight(up, tt))

        for when, j in ((MLP_ORDER.index(1), 1), (MLP_ORDER.index(3), 0)):

            @pl.when(i == when)
            def _(j=j):
                kc(up, j).start()
                kc(down, j).start()

        run_at(k, "m%d", 2 * nt)
        return carry

    lax.fori_loop(0, 2 * nt, mlp, 0)
    b_down = wide(7)
    zero_row = jnp.zeros((1, C), F32)

    def turn(i, at, carry):
        xp[at, :] = jnp.where(live_rows(i), xp[at, :] + acc[at, :] + b_down, 0.0)
        e, normed, g = acc2[at, :], n2[at, :], gy[at, :]
        gx = norm_back(e * gain2, normed, r2[at, :]) + g
        gy[at, :] = gx
        low[at, :] = gx.astype(BF16)
        h2t[:, at] = gx.T.astype(BF16)
        sums = (rowsum(e * normed), rowsum(e), rowsum(gx), rowsum(g))
        return tuple(p + q for p, q in zip(carry, sums))

    sums = each(turn, (zero_row,) * 4)
    put_small(5, sums[0])
    put_small(6, sums[1])
    put_small(4, sums[2])
    put_small(7, sums[3])
    gather(xp, yb)
    own_y = pltpu.make_async_copy(yb.at[t], y_all.at[t], loc.at[2])
    own_y.start()
    run("turn")
    acc[...] = jnp.zeros_like(acc)

    def back(i, carry):
        tt = group(3 - i)
        gatt[...] = nn(low[...], weight(0, tt, LANES, LANES)).astype(BF16)
        pairs[...] = jnp.zeros_like(pairs)

        def window(w):
            at = pl.ds(pl.multiple_of(w * PAD, PAD), PAD)
            q4, g4 = stack(qs[tt, at, :]), stack(gatt[at, :])
            p = probs[tt, w]
            dp = nt_dot(kvs[tt, at, LANES:], g4)
            ds = p * (dp - rowsum(p * dp))
            ds_low = ds.astype(BF16)
            gkv[at, :LANES] = nn(ds_low, q4).astype(BF16)
            gkv[at, LANES:CW] = nn(p.astype(BF16), g4).astype(BF16)
            gq[at, :] = pick(tn_dot(ds_low, kvs[tt, at, :LANES])).astype(BF16)
            return ds_low.astype(F32)

        def four(hh, carry):
            total = window(hh * (slots // 2))
            for j in range(1, slots // 2):
                total = total + window(hh * (slots // 2) + j)
            pairs[...] += total

            @pl.when(hh == 0)
            def _():
                run_at(i, "b%df", nt)

            return carry

        lax.fori_loop(0, 2, four, 0)
        gk_gv = gkv[:, :CW]
        put_grad(1, tt, nn(h1t[...], gk_gv))
        run_at(i, "b%de", nt)

        left = nn(h1t[...], gq[...]) * SCALE
        put_grad(0, tt, jnp.concatenate([left, nn(h2t[...], att[tt])], axis=1))

        @pl.when(i == 0)
        def _():
            kc(1, 0).start()
            kc(0, 0).start()

        @pl.when(i == 2)
        def _():
            kc(1, 1).start()
            kc(0, 1).start()

        run_at(i, "b%dd", nt)
        small[tt, 2:3, :] = rowsum(gq[...].astype(F32)) * SCALE
        small[tt, 3:4, :] = rowsum(gkv[:, LANES:CW].astype(F32))
        grad_q = nt_dot(gq[...], weight(0, tt, 0, LANES)) * SCALE
        acc[...] += grad_q + nt_dot(gk_gv, weight(1, tt))
        for h in range(heads):
            lanes = h // 2 * LANES
            source = pairs[:, lanes : lanes + LANES]
            for q in range(TPAD // LANES):
                where = inv[:, q * LANES : (q + 1) * LANES]
                value = take(source, jnp.maximum(where, 0) + h % 2 * PAD)
                value = jnp.where(where >= 0, value, 0.0)
                small[tt, pl.ds(12 + 2 * h + q, 1), :] = rowsum(value)

        run_at(i, "b%ds", nt)
        return carry

    lax.fori_loop(0, nt, back, 0)

    def finish(i, at, carry):
        e, normed = acc[at, :], n1[at, :]
        xp[at, :] = norm_back(e * gain1, normed, r1[at, :]) + gy[at, :]
        sums = (rowsum(e * normed), rowsum(e))
        return tuple(p + q for p, q in zip(carry, sums))

    sums = each(finish, (zero_row,) * 2)
    put_small(0, sums[0])
    put_small(1, sums[1])
    for d in range(3):
        small_t(d).start()
    gather(xp, gb)
    own_g = pltpu.make_async_copy(gb.at[t], g_all.at[t], loc.at[3])
    own_g.start()
    run("t1")
    run("t2")
    await_bytes(scr, coming("st"))
    zb[z] = small[t] + scr[0] + (scr[1] + scr[2])
    for d in range(nz - 1):
        small_z(d).start()
    run("t3")
    await_bytes(zb.at[pl.ds(0, nz - 1)], coming("sz"))
    value = zb[0]
    for zz in range(1, nz):
        value = value + zb[zz]
    sx[...] = value
    small_x().start()
    run("t4")
    run("t5")
    for ch in (2, 4, 3, 5, 1, 0):
        last(ch)
    small_x().wait_recv()
    tot[...] = sx[...] + syr[...]
    for i in range(2):
        await_bytes((yb, gb)[i].at[pl.ds(0, 3)], coming("out", i))
    for i, n in enumerate(totals):
        await_bytes(blocks(n), ss.at[i])
    three = (xg, cg, vg, yb, gb, small)
    for i, ref in enumerate(three):
        await_bytes(ref.at[pl.ds(0, 3)], ss.at[len(totals) + i])
    await_bytes(zb.at[pl.ds(0, nz - 1)], ss.at[len(totals) + 6])
    await_bytes(sx, ss.at[len(totals) + 7])
    own_y.wait()
    own_g.wait()


def block_call(nt, nz, slots, *args):
    tok, deep, heads = args[1], args[3].shape[0], args[18].shape[0]
    real = tok.shape[1]
    rows, wide = slots * PAD, heads * PAD
    piece = (nz, 2, deep, CW)
    row = (nt, real, LANES)

    def vm(shape, kind=BF16):
        return pltpu.VMEM(shape, kind)

    small = (SROWS, LANES)
    n_c = max(1, WAY_OUT.count("C"))
    return pl.pallas_call(
        functools.partial(block, nt, nz, slots),
        name="block",
        out_shape=(
            jax.ShapeDtypeStruct(row, BF16),
            jax.ShapeDtypeStruct(row, BF16),
            jax.ShapeDtypeStruct((NCH, deep, CW), F32),
            jax.ShapeDtypeStruct(small, F32),
        ),
        in_specs=[SM] + [ANY] * 20,
        out_specs=(ANY, ANY, VM, VM),
        scratch_shapes=[vm(arg.shape, arg.dtype) for arg in args[9:]]
        + [
            vm(row),
            vm(row),
            vm((NCH, nt) + piece),
            vm((nt,) + small, F32),
            vm((nt, PAD, wide), F32),
            vm((NCH, nt) + piece),
            vm((NCH, 2) + piece),
            vm((max(1, WAY_OUT.count("A")),) + piece),
            vm((WAY_OUT.count("B"), 2, nz, deep, CW)),
            vm((NCH, nz, deep, CW)),
            vm((NCH, nz - 1, deep, CW)),
            vm((n_c, nz - 1, 2, 2, deep, CW)),
            vm((n_c, 3, deep, CW)),
            vm((3,) + small, F32),
            vm(small, F32),
            vm(small, F32),
            vm((nz,) + small, F32),
            vm((nt,) + small, F32),
            vm(row),
            vm(row),
            vm((LANES, LANES), F32),
            vm((slots, PAD, wide), F32),
            vm((PAD, TPAD), jnp.int32),
            vm((real, C), F32),
            vm((rows, C), F32),
            vm((rows, C), F32),
            vm((rows, C)),
            vm((C, rows)),
            vm((C, rows)),
            vm((C, rows)),
            vm((nt, rows, LANES)),
            vm((nt, rows, CW)),
            vm((nt, slots, PAD, wide), F32),
            vm((nt, rows, LANES)),
            vm((rows, C), F32),
            vm((rows, C), F32),
            vm((rows, C), F32),
            vm((rows, 1), F32),
            vm((rows, C), F32),
            vm((rows, 1), F32),
            vm((rows, C)),
            vm((rows, C)),
            vm((rows, LANES)),
            vm((rows, LANES)),
            vm((PAD, wide), F32),
            DMA((4,)),
            DMA((14,)),
            DMA((len(arrival_table(nz)),)),
            DMA((len(send_table(nt, nz)[1]) + 8,)),
        ],
        compiler_params=pltpu.CompilerParams(
            collective_id=0, has_side_effects=True, vmem_limit_bytes=60 * 2**20
        ),
    )(*args)


def spell(n, *refs):
    ins, outs, refs = refs[:4], refs[4 : 4 + n], refs[4 + n :]
    (y_in, g_in, fin, tot), refs = refs[:4], refs[4:]
    held, (get, put) = refs[:n], refs[n:]
    steps = ins[0].shape[0]
    loads = [pltpu.make_async_copy(ins[2], fin, get.at[0])]
    loads.append(pltpu.make_async_copy(ins[3], tot, get.at[1]))
    for i in range(steps):
        for j, ref in enumerate((y_in, g_in)):
            loads.append(
                pltpu.make_async_copy(ins[j].at[i], ref.at[i], get.at[2 + 2 * i + j])
            )
    for copy in loads:
        copy.start()
    loads[0].wait()
    loads[1].wait()
    spell_rest(fin, tot, *held[2:])
    like = {}
    for k in range(2, n):
        slot = 2 + list(like).index(held[k].shape) if held[k].shape in like else 2 + len(like)
        like.setdefault(held[k].shape, []).append(k)
        pltpu.make_async_copy(held[k], outs[k], put.at[slot]).start()
    for i in range(steps):
        for j, ref in enumerate((y_in, g_in)):
            loads[2 + 2 * i + j].wait()
            held[j][i] = ref[i].astype(F32)
            pltpu.make_async_copy(held[j].at[i], outs[j].at[i], put.at[j]).start()
    for j in range(2):
        pltpu.make_async_copy(held[j], outs[j], put.at[j]).wait()
    for slot, (shape, ks) in enumerate(like.items()):
        size = len(ks) * shape[0] * shape[1]
        if len(ks) == 1:
            ref = held[ks[0]]
        elif shape[0] == 1:
            ref = tot.at[pl.ds(0, len(ks))]
        else:
            ref = fin.at[pl.ds(0, size // (fin.shape[1] * fin.shape[2]))]
        pltpu.make_async_copy(ref, ref, put.at[2 + slot]).wait()


def spell_rest(fin, tot, *outs):
    (
        d_g1, d_s1, d_wq, d_wk, d_wv, d_bq, d_bv, d_wo, d_bo, d_g2, d_s2, d_wh, d_bh,
        d_wd, d_bd, d_tab,
    ) = outs
    d_wq[...] = fin[0, :, :LANES]
    d_wk[...] = fin[1, :, :LANES]
    d_wv[...] = fin[1, :, LANES:]
    d_wo[...] = fin[0, :, LANES:]
    for s in range(2):
        d_wh[:, s * CW : (s + 1) * CW] = fin[2 + s]
        d_wd[:, s * CW : (s + 1) * CW] = fin[4 + s]
    for i, ref in enumerate((d_g1, d_s1, d_bq, d_bv, d_bo, d_g2, d_s2, d_bd)):
        ref[...] = tot[i : i + 1, :]
    d_bh[...] = tot[8:12, :]
    for h in range(d_tab.shape[0]):
        d_tab[h : h + 1, :LANES] = tot[12 + 2 * h : 13 + 2 * h]
        d_tab[h : h + 1, LANES:] = tot[13 + 2 * h : 14 + 2 * h, : TABLE - LANES]


def spell_call(outs, *args):
    n, steps = len(outs), args[0].shape[0]
    held = [pltpu.VMEM(v.shape, v.dtype) for v in args + outs]
    return pl.pallas_call(
        functools.partial(spell, n),
        name="spell",
        out_shape=outs,
        in_specs=[ANY] * 4,
        out_specs=(ANY,) * n,
        scratch_shapes=held + [DMA((2 + 2 * steps,)), DMA((2 + len({v.shape for v in outs[2:]}),))],
        compiler_params=pltpu.CompilerParams(vmem_limit_bytes=60 * 2**20),
    )(*args)


def per_device(
    nt, na, tokens, gain_one, shift_one, w_query, w_key, w_value, b_query, b_value, w_out, b_out,
    gain_two, shift_two, w_hidden, b_hidden, w_down, b_down, bias_table, rel_index, region,
    win_count, cotangent,
):
    slots = region.shape[0] // nt
    cut = (nt, slots * WT, LANES)
    vectors = [gain_one, shift_one, b_query, b_value, b_out, gain_two, shift_two, b_down]
    parts = block_call(
        nt, na // 2, slots,
        win_count, tokens.reshape(cut), cotangent.reshape(cut),
        w_query, w_key, w_value, w_out.T, w_hidden, w_down.T,
        *[v.reshape(1, LANES) for v in vectors],
        b_hidden.reshape(-1, LANES), bias_table.T, rel_index, region,
    )

    def out(like, shape=None):
        return jax.ShapeDtypeStruct(shape or like.shape, F32)

    one = (1, LANES)
    shapes = (
        out(tokens, cut), out(tokens, cut), out(gain_one, one), out(gain_one, one), out(w_query),
        out(w_key), out(w_value), out(b_query, one), out(b_value, one), out(w_out, w_out.shape[::-1]),
        out(b_out, one), out(gain_two, one), out(shift_two, one), out(w_hidden),
        out(b_hidden, (b_hidden.shape[0] // LANES, LANES)), out(w_down, w_down.shape[::-1]),
        out(b_down, one), out(bias_table, bias_table.shape[::-1]),
    )
    likes = (
        tokens, tokens, gain_one, gain_one, w_query, w_key, w_value, b_query, b_value, w_out,
        b_out, gain_two, shift_two, w_hidden, b_hidden, w_down, b_down, bias_table,
    )
    values = spell_call(shapes, *parts)
    turned = (9, 15, 17)
    return tuple(
        v.T if i in turned else v.reshape(like.shape)
        for i, (v, like) in enumerate(zip(values, likes))
    )


def solution(mesh):
    return jax.shard_map(
        functools.partial(per_device, mesh.shape["ta"], mesh.shape["wa"]),
        mesh=mesh,
        in_specs=(
            P("wa", "ta"),
            P("ta"),
            P("ta"),
            P("wa", "ta"),
            P("wa", "ta"),
            P("wa", "ta"),
            P("ta"),
            P("ta"),
            P("ta", "wa"),
            P("ta"),
            P("ta"),
            P("ta"),
            P("wa", "ta"),
            P("ta"),
            P("ta", "wa"),
            P("ta"),
            P(None, "ta"),
            P(),
            P("wa", None),
            P("wa"),
            P("wa", "ta"),
        ),
        out_specs=(
            P("wa", "ta"),
            P("wa", "ta"),
            P("ta"),
            P("ta"),
            P("wa", "ta"),
            P("wa", "ta"),
            P("wa", "ta"),
            P("ta"),
            P("ta"),
            P("ta", "wa"),
            P("ta"),
            P("ta"),
            P("ta"),
            P("wa", "ta"),
            P("ta"),
            P("ta", "wa"),
            P("ta"),
            P(None, "ta"),
        ),
        check_vma=False,
    )
```
